32 devices in a mesh: dp: 16 (over z, y, x), mp: 2 (over core).
Axes of the slice: x: 2, y: 2, z: 4, core: 2. Of those that a mesh axis runs over, the one named last changes fastest.
Arguments:
- hidden_in: bfloat16 [2048, 4096], P('dp', 'mp'), may hold values from -6 to 6
- lengths: int32 [16], P('dp'), may hold values from 1 to 128
- norm_attn: float32 [4096], replicated, may hold values from 0.25 to 1.75
- q_weight: bfloat16 [4096, 4096], P('dp', 'mp'), may hold values from -0.01171875 to 0.01171875
- k_weight: bfloat16 [4096, 4096], P('dp', 'mp'), may hold values from -0.09375 to 0.09375
- v_weight: bfloat16 [4096, 4096], P('dp', 'mp'), may hold values from -0.09375 to 0.09375
- out_weight_t: bfloat16 [4096, 4096], P('dp', 'mp'), may hold values from -0.09375 to 0.09375
- norm_ffn: float32 [4096], replicated, may hold values from 0.25 to 1.75
- gate_weight: bfloat16 [4096, 10240], P('dp', 'mp'), may hold values from -0.09375 to 0.09375
- up_weight: bfloat16 [4096, 10240], P('dp', 'mp'), may hold values from -0.09375 to 0.09375
- down_weight_t: bfloat16 [4096, 10240], P('dp', 'mp'), may hold values from -0.0625 to 0.0625
- scale_key: float32 [4096], P('mp'), may hold values from 0.25 to 4
- scale_value: float32 [4096], P('mp'), may hold values from 0.1 to 1.9
- scale_ffn: float32 [10240], P('mp'), may hold values from 0.1 to 1.9
- out_grad: bfloat16 [2048, 4096], P('dp'), may hold values from -6 to 6
- position_bias: float32 [64, 128, 128], P('mp'), may hold values from -6 to 256
Outputs:
- block_out: bfloat16 [2048, 4096], P('dp', 'mp')
- input_grad: bfloat16 [2048, 4096], P('dp', 'mp')
- grad_key: float32 [4096], P('mp')
- grad_value: float32 [4096], P('mp')
- grad_ffn: float32 [10240], P('mp')
The draws below stay inside these ranges and needn't reach their ends.
Inputs may be any that keep to these rules, and one draw needn't show every extreme that they name: Keys of sequence b at positions lengths[b] and beyond are padding.
All inputs are finite; a program needn't handle non-finite values.
Results may differ from the reference program's by a relative error of at most 0.03.
Values may be sent and summed in bfloat16 or wider, within the bound.
A program may use at most 320 MiB of HBM per device.

```python
import math
import jax
import jax.numpy as jnp
from jax import lax

D = 4096
FF = 10240
HEADS = 64
HEAD_DIM = 64
SEQ = 128
HD = 4096
BATCH = 16
TOKENS = 2048
N_MP = 2


def draw_position_bias(key, part):
    first_key = jax.random.fold_in(key, 0)
    return jnp.clip(jax.random.normal(first_key, (HEADS, SEQ, SEQ), jnp.float32), -6.0, 6.0)


def with_ends(array, own_key, smallest, largest):
    longest = array.shape.index(max(array.shape))
    spots = []
    for shift in (0, 1):
        where = [jax.random.randint(jax.random.fold_in(own_key, axis), (), 0, length) for axis, length in enumerate(array.shape)]
        where[longest] = (where[longest] + shift) % array.shape[longest]
        spots.append(tuple(where))
    return array.at[spots[0]].set(smallest).at[spots[1]].set(largest)


def block_scale(rng, shape, shards, smallest, top_value):
    factor_of, own = 1.0, jax.random.fold_in(rng, 6)
    for dim, blocks in shards:
        draws = jnp.exp(jax.random.uniform(jax.random.fold_in(own, dim), (blocks,), jnp.float32, smallest / len(shards), top_value / len(shards)))
        factor_of = factor_of * jnp.repeat(draws, shape[dim] // blocks).reshape([-1 if axis == dim else 1 for axis in range(len(shape))])
    return factor_of


def gaussian(stream_key, extent, spread, most, cuts=(), held_as=jnp.bfloat16):
    values = jax.random.normal(stream_key, extent, jnp.float32) * spread
    if len(cuts) > 0:
        values = block_scale(stream_key, extent, cuts, -0.22, 0.18) * values
    return jnp.clip(values, min=-most, max=most).astype(held_as)


def setup_inputs(seed: int = 0) -> dict:
    keys = jax.random.split(jax.random.key(seed), 17)
    return {
        "hidden_in": gaussian(keys[0], (TOKENS, D), 1.0, 6.0, ((0, 16), (1, 2))),
        "lengths": with_ends(jax.random.randint(keys[1], (BATCH,), 1, SEQ + 1), jax.random.fold_in(keys[1], 1), 1, SEQ).astype(jnp.int32),
        "norm_attn": jnp.clip(1.0 + 0.15 * jax.random.normal(keys[2], (D,), jnp.float32), 0.25, 1.75),
        "q_weight": gaussian(keys[3], (D, HD), (D * HEAD_DIM) ** -0.5, 0.01171875, ((0, 16), (1, 2))),
        "k_weight": gaussian(keys[4], (D, HD), D ** -0.5, 0.09375, ((0, 16), (1, 2))),
        "v_weight": gaussian(keys[5], (D, HD), D ** -0.5, 0.09375, ((0, 16), (1, 2))),
        "out_weight_t": gaussian(keys[6], (D, HD), HD ** -0.5, 0.09375, ((0, 16), (1, 2))),
        "norm_ffn": jnp.clip(1.0 + 0.15 * jax.random.normal(keys[7], (D,), jnp.float32), 0.25, 1.75),
        "gate_weight": gaussian(keys[8], (D, FF), D ** -0.5, 0.09375, ((0, 16), (1, 2))),
        "up_weight": gaussian(keys[9], (D, FF), D ** -0.5, 0.09375, ((0, 16), (1, 2))),
        "down_weight_t": gaussian(keys[10], (D, FF), FF ** -0.5, 0.0625, ((0, 16), (1, 2))),
        "scale_key": jnp.clip(jnp.exp(math.log(4.0) - 2.7725887 * jax.random.uniform(keys[11], (HD,), jnp.float32) ** block_scale(keys[11], (HD,), ((0, 2),), -0.2, 0.2)), 0.25, 4.0),
        "scale_value": jnp.clip(1.0 + 0.18 * jax.random.normal(keys[12], (HD,), jnp.float32), 0.1, 1.9),
        "scale_ffn": jnp.clip(1.0 + 0.18 * jax.random.normal(keys[13], (FF,), jnp.float32), 0.1, 1.9),
        "out_grad": gaussian(keys[14], (TOKENS, D), 1.0, 6.0, ((0, 16),)),
        "position_bias": draw_position_bias(jax.random.fold_in(keys[16], 71), 0),
    }


EPSILON = 1e-06
NEGATIVE = -1e+30

def inverse_rms(values):
    return lax.rsqrt(lax.optimization_barrier(jnp.mean(values * values, axis=-1, keepdims=True)) + EPSILON)

def lowered(values):
    return lax.optimization_barrier(values.astype(jnp.bfloat16))

def widen(values):
    return values.astype(jnp.float32)

def gelu_tanh(values):
    return jax.nn.gelu(values, approximate=True)

def contract_last(left_side, right_side):
    return lax.dot_general(left_side, right_side, (((1,), (1,)), ((), ())), preferred_element_type=jnp.float32)

def block_split(matrix, block_count):
    return jnp.transpose(matrix.reshape(matrix.shape[0], block_count, -1), (1, 0, 2))

def rounded_blocks(operands, block_count):
    row_count = operands[0][0].shape[0]
    out_width = operands[0][1].shape[0]
    stacked = tuple((block_split(member, block_count) for couple in operands for member in couple))

    def accumulate(running, pieces):
        partial_term = jnp.zeros((row_count, out_width), jnp.float32)
        for position in range(len(operands)):
            partial_term = partial_term + contract_last(pieces[2 * position], pieces[2 * position + 1])
        rounded = lax.optimization_barrier(partial_term.astype(jnp.bfloat16))
        return (running + rounded.astype(jnp.float32), None)
    result, unused = lax.scan(accumulate, jnp.zeros((row_count, out_width), jnp.float32), stacked)
    return result

def norm_back(grad_in, values, inverse, gain_vec):
    scaled = grad_in * gain_vec
    correction = values * inverse * inverse * inverse * lax.optimization_barrier(jnp.mean(scaled * values, axis=-1, keepdims=True))
    return inverse * scaled - correction

def reference(hidden_in, lengths, norm_attn, q_weight, k_weight, v_weight, out_weight_t, norm_ffn, gate_weight, up_weight, down_weight_t, scale_key, scale_value, scale_ffn, out_grad, position_bias):
    shaped = (BATCH, SEQ, HEADS, HEAD_DIM)
    inputs32 = hidden_in.astype(jnp.float32)
    inv_first = inverse_rms(inputs32)
    normed_first = (inputs32 * inv_first * norm_attn).astype(jnp.bfloat16)
    queries = lowered(jnp.dot(normed_first, q_weight, preferred_element_type=jnp.float32))
    key_pre = jnp.dot(normed_first, k_weight, preferred_element_type=jnp.float32)
    value_pre = jnp.dot(normed_first, v_weight, preferred_element_type=jnp.float32)
    key_rows = lowered(key_pre * scale_key)
    value_rows = lowered(value_pre * scale_value)
    q_heads = widen(queries).reshape(shaped)
    k_heads = widen(key_rows).reshape(shaped)
    v_heads = widen(value_rows).reshape(shaped)
    scores = jnp.einsum('bihe,bjhe->bhij', q_heads, k_heads) + position_bias.astype(jnp.float32)[None]
    positions = jnp.arange(SEQ, dtype=jnp.int32)
    valid_keys = positions[None, :] < lengths[:, None]
    scores = jnp.where(valid_keys[:, None, None, :], scores, NEGATIVE)
    attn_probs = jax.nn.softmax(scores, axis=-1)
    probs_low = widen(lowered(attn_probs))
    context = jnp.einsum('bhij,bjhe->bihe', probs_low, v_heads).reshape(TOKENS, HEADS * HEAD_DIM).astype(jnp.bfloat16)
    first_sum = inputs32 + rounded_blocks(((context, out_weight_t),), N_MP)
    inv_second = inverse_rms(first_sum)
    normed_second = (first_sum * inv_second * norm_ffn).astype(jnp.bfloat16)
    gate_proj = jnp.dot(normed_second, gate_weight, preferred_element_type=jnp.float32)
    upward = jnp.dot(normed_second, up_weight, preferred_element_type=jnp.float32)
    activated, gelu_back = jax.vjp(gelu_tanh, gate_proj)
    product = activated * upward
    hidden = (product * scale_ffn).astype(jnp.bfloat16)
    block_out = (first_sum + rounded_blocks(((hidden, down_weight_t),), N_MP)).astype(jnp.bfloat16)
    d_hidden = jnp.dot(out_grad, down_weight_t, preferred_element_type=jnp.float32)
    grad_ffn = lax.optimization_barrier(jnp.sum(d_hidden * product, axis=0))
    d_product = d_hidden * scale_ffn
    d_gate = gelu_back(d_product * upward)[0].astype(jnp.bfloat16)
    d_up = (d_product * activated).astype(jnp.bfloat16)
    d_second = rounded_blocks(((d_gate, gate_weight), (d_up, up_weight)), N_MP)
    d_first = out_grad.astype(jnp.float32) + norm_back(d_second, first_sum, inv_second, norm_ffn)
    d_context = lowered(jnp.dot(d_first.astype(jnp.bfloat16), out_weight_t, preferred_element_type=jnp.float32))
    dc_heads = widen(d_context).reshape(shaped)
    d_probs = jnp.einsum('bihe,bjhe->bhij', dc_heads, v_heads)
    d_scores = widen(lowered(attn_probs * (d_probs - lax.optimization_barrier(jnp.sum(attn_probs * d_probs, axis=-1, keepdims=True)))))
    d_values = jnp.einsum('bhij,bihe->bjhe', probs_low, dc_heads).reshape(TOKENS, HEADS * HEAD_DIM)
    d_keys = jnp.einsum('bhij,bihe->bjhe', d_scores, q_heads).reshape(TOKENS, HEADS * HEAD_DIM)
    d_queries = jnp.einsum('bhij,bjhe->bihe', d_scores, k_heads).reshape(TOKENS, HEADS * HEAD_DIM).astype(jnp.bfloat16)
    grad_key = lax.optimization_barrier(jnp.sum(d_keys * key_pre, axis=0))
    grad_value = lax.optimization_barrier(jnp.sum(d_values * value_pre, axis=0))
    d_key_pre = (d_keys * scale_key).astype(jnp.bfloat16)
    d_value_pre = (d_values * scale_value).astype(jnp.bfloat16)
    d_normed = rounded_blocks(((d_queries, q_weight), (d_key_pre, k_weight), (d_value_pre, v_weight)), N_MP)
    input_grad = (d_first + norm_back(d_normed, inputs32, inv_first, norm_attn)).astype(jnp.bfloat16)
    return (block_out, input_grad, grad_key, grad_value, grad_ffn)
```

```python
import functools

import jax
import jax.numpy as jnp
from jax import lax
from jax.experimental import pallas as pl
from jax.experimental.pallas import tpu as pltpu
from jax.sharding import PartitionSpec as P

HEAD_DIM = 64
MESH = pl.DeviceIdType.MESH


EPSILON = 1e-06
NEGATIVE = -1e30


def inverse_rms(values):
    return lax.rsqrt(jnp.mean(values * values, axis=-1, keepdims=True) + EPSILON)


def gelu_tanh(values):
    return jax.nn.gelu(values, approximate=True)


def contract_last(left_side, right_side):
    return lax.dot_general(
        left_side, right_side, (((1,), (1,)), ((), ())), preferred_element_type=jnp.float32
    )


def norm_back(grad_in, values, inverse, gain_vec):
    scaled = grad_in * gain_vec
    correction = (
        values * inverse * inverse * inverse * jnp.mean(scaled * values, axis=-1, keepdims=True)
    )
    return inverse * scaled - correction


WEIGHT_AXIS = "lo"


def on_device_general(
    hidden_in, lengths, norm_attn, q_weight, k_weight, v_weight, out_weight_t, norm_ffn,
    gate_weight, up_weight, down_weight_t, scale_key, scale_value, scale_ffn, out_grad,
    position_bias,
):
    f32, bf16 = jnp.float32, jnp.bfloat16
    wa = WEIGHT_AXIS
    ta = "lo" if wa == "hi" else "hi"
    n_hi, n_lo = lax.axis_size("hi"), lax.axis_size("lo")
    n_t = lax.axis_size(ta)

    def swap(x, bit):
        return lax.ppermute(x, "lo", [(i, i ^ bit) for i in range(n_lo)])

    def own_first(parts):
        if n_lo != 4:
            return parts
        index = lax.axis_index("lo")
        rows, width = parts.shape[0], parts.shape[-1]
        parts = parts.reshape(rows, n_hi, 2, 2, width)
        parts = jnp.where((index & 2) > 0, parts[:, :, ::-1], parts)
        parts = jnp.where((index & 1) > 0, parts[:, :, :, ::-1], parts)
        return parts.reshape(rows, n_hi, n_lo, width)

    def sum_mp(x):
        x = x.astype(bf16)
        if lax.axis_size("mp") != 2:
            return lax.psum(x, "mp").astype(f32)
        return x.astype(f32) + lax.ppermute(x, "mp", [(0, 1), (1, 0)]).astype(f32)

    def split_features(x):
        rows = x.shape[0]
        parts = own_first(x.reshape(rows, n_hi, n_lo, -1))
        order = (1, 0, 2, 3) if ta == "hi" else (2, 0, 1, 3)
        return parts.transpose(order).reshape(n_t, rows, -1)

    def join_features(x):
        rows = x.shape[1]
        if ta == "hi":
            parts = x.transpose(1, 0, 2).reshape(rows, n_hi, n_lo, -1)
            return own_first(parts).reshape(rows, -1)
        return x.reshape(n_lo, rows, n_hi, -1).transpose(1, 2, 0, 3).reshape(rows, -1)

    def exchange(x):
        return lax.all_to_all(x, ta, split_axis=0, concat_axis=0, tiled=True)

    def gather_rows(w):
        if n_lo != 4:
            return lax.all_gather(w, wa, axis=0, tiled=True)
        half = w.shape[0] // 2
        first, second = swap(w, 1), swap(w, 2)
        third = swap(second[:half], 1), swap(first[half:], 2)
        return jnp.concatenate([w, first, second, *third], axis=0)

    def gather_tokens(x):
        return lax.all_gather(x, ta, axis=0, tiled=True)

    def scatter_tokens(x):
        return lax.psum_scatter(x.astype(bf16), ta, scatter_dimension=0, tiled=True)

    def dot(a, b):
        return jnp.dot(a, b, preferred_element_type=f32)

    d_model = norm_attn.shape[0]
    tokens_local = hidden_in.shape[0]
    seq_local = lengths.shape[0]
    seq_len = tokens_local // seq_local
    t_index = lax.axis_index(ta)
    gain_attn = split_features(norm_attn[None])
    gain_attn = lax.dynamic_index_in_dim(gain_attn, t_index, 0, False)
    gain_ffn = split_features(norm_ffn[None])
    gain_ffn = lax.dynamic_index_in_dim(gain_ffn, t_index, 0, False)

    full_inputs = lax.all_gather(hidden_in, "mp", axis=1, tiled=True)
    both = jnp.concatenate([split_features(full_inputs), split_features(out_grad)], axis=2)
    both = exchange(both).reshape(n_t * tokens_local, -1)
    inputs_blk, out_grad_blk = jnp.split(both, 2, axis=1)
    inputs32 = inputs_blk.astype(f32)

    def token_mean(x):
        return lax.psum(jnp.sum(x, axis=-1, keepdims=True), ta) / d_model

    q_full, k_full, v_full = gather_rows(q_weight), gather_rows(k_weight), gather_rows(v_weight)
    o_full = gather_rows(out_weight_t)
    gate_full, up_full = gather_rows(gate_weight), gather_rows(up_weight)
    down_full = gather_rows(down_weight_t)

    inv_first = lax.rsqrt(token_mean(inputs32 * inputs32) + EPSILON)
    normed_first = (inputs32 * inv_first * gain_attn).astype(bf16)
    queries = scatter_tokens(dot(normed_first, q_full))
    key_pre = scatter_tokens(dot(normed_first, k_full)).astype(f32)
    value_pre = scatter_tokens(dot(normed_first, v_full)).astype(f32)
    heads_local = queries.shape[1] // HEAD_DIM
    shaped = (seq_local, seq_len, heads_local, HEAD_DIM)
    key_rows = (key_pre * scale_key).astype(bf16)
    value_rows = (value_pre * scale_value).astype(bf16)
    q_heads = queries.reshape(shaped)
    k_heads = key_rows.reshape(shaped)
    v_heads = value_rows.reshape(shaped)
    scores = (
        jnp.einsum("bihe,bjhe->bhij", q_heads, k_heads, preferred_element_type=f32)
        + position_bias[None]
    )
    positions = lax.broadcasted_iota(jnp.int32, (seq_local, seq_len), 1)
    valid_keys = positions < lengths[:, None]
    scores = jnp.where(valid_keys[:, None, None, :], scores, NEGATIVE)
    largest = jnp.max(scores, axis=-1, keepdims=True)
    exponent = jnp.exp(scores - largest)
    attn_probs = exponent / jnp.sum(exponent, axis=-1, keepdims=True)
    probs_low = attn_probs.astype(bf16)
    context = (
        jnp.einsum("bhij,bjhe->bihe", probs_low, v_heads, preferred_element_type=f32)
        .reshape(tokens_local, -1)
        .astype(bf16)
    )
    first_sum = inputs32 + sum_mp(contract_last(gather_tokens(context), o_full))
    inv_second = lax.rsqrt(token_mean(first_sum * first_sum) + EPSILON)
    normed_second = (first_sum * inv_second * gain_ffn).astype(bf16)
    gate_proj = scatter_tokens(dot(normed_second, gate_full)).astype(f32)
    upward = scatter_tokens(dot(normed_second, up_full)).astype(f32)
    d_hidden = scatter_tokens(dot(out_grad_blk, down_full)).astype(f32)
    activated, gelu_back = jax.vjp(gelu_tanh, gate_proj)
    product = activated * upward
    hidden = (product * scale_ffn).astype(bf16)
    grad_ffn_part = jnp.sum(d_hidden * product, axis=0)
    d_product = d_hidden * scale_ffn
    d_gate = gelu_back(d_product * upward)[0].astype(bf16)
    d_up = (d_product * activated).astype(bf16)
    d_second = sum_mp(
        contract_last(gather_tokens(d_gate), gate_full)
        + contract_last(gather_tokens(d_up), up_full)
    )
    scaled = d_second * gain_ffn
    d_first = (
        out_grad_blk.astype(f32)
        + inv_second * scaled
        - first_sum * inv_second * inv_second * inv_second * token_mean(scaled * first_sum)
    )
    d_context = scatter_tokens(dot(d_first.astype(bf16), o_full))
    dc_heads = d_context.reshape(shaped)
    d_probs = jnp.einsum("bihe,bjhe->bhij", dc_heads, v_heads, preferred_element_type=f32)
    d_scores = (
        attn_probs * (d_probs - jnp.sum(attn_probs * d_probs, axis=-1, keepdims=True))
    ).astype(bf16)
    d_values = jnp.einsum(
        "bhij,bihe->bjhe", probs_low, dc_heads, preferred_element_type=f32
    ).reshape(tokens_local, -1)
    d_keys = jnp.einsum(
        "bhij,bihe->bjhe", d_scores, q_heads, preferred_element_type=f32
    ).reshape(tokens_local, -1)
    d_queries = (
        jnp.einsum("bhij,bjhe->bihe", d_scores, k_heads, preferred_element_type=f32)
        .reshape(tokens_local, -1)
        .astype(bf16)
    )
    grad_key_part = jnp.sum(d_keys * key_pre, axis=0)
    grad_value_part = jnp.sum(d_values * value_pre, axis=0)
    d_key_pre = (d_keys * scale_key).astype(bf16)
    d_value_pre = (d_values * scale_value).astype(bf16)
    d_normed = sum_mp(
        contract_last(gather_tokens(d_queries), q_full)
        + contract_last(gather_tokens(d_key_pre), k_full)
        + contract_last(gather_tokens(d_value_pre), v_full)
    )
    scaled_in = d_normed * gain_attn
    mean_dot = token_mean(scaled_in * inputs32)
    input_grad = (
        d_first
        + inv_first * scaled_in
        - inputs32 * inv_first * inv_first * inv_first * mean_dot
    ).astype(bf16)

    ffn_out = sum_mp(contract_last(gather_tokens(hidden), down_full))
    block_out = (first_sum + ffn_out).astype(bf16)

    share_width = hidden_in.shape[1]
    offset = lax.axis_index("mp") * share_width

    def own_share(x):
        joined = join_features(exchange(x.reshape(n_t, tokens_local, -1)))
        return lax.dynamic_slice_in_dim(joined, offset, share_width, 1)

    parts = jnp.concatenate([grad_key_part, grad_value_part, grad_ffn_part])
    totals = lax.psum(lax.psum(parts, "lo"), "hi")
    width = grad_key_part.shape[0]
    return (
        own_share(block_out),
        own_share(input_grad),
        totals[:width],
        totals[width : 2 * width],
        totals[2 * width :],
    )


def stream_body(n_w, n_x, *refs):
    w_refs, x_refs = refs[:n_w], refs[n_w:n_w + n_x]
    outs = refs[n_w + n_x:2 * n_w + n_x]
    x_outs = refs[2 * n_w + n_x:2 * (n_w + n_x)]
    own_sem, a_send, a_recv, b_send, b_recv, c_send, c_recv, x_own, x_send, x_recv = refs[
        2 * (n_w + n_x):2 * (n_w + n_x) + 10
    ]
    holds = refs[2 * (n_w + n_x) + 10:]
    n_hi, n_lo = lax.axis_size("hi"), lax.axis_size("lo")
    hi, lo = lax.axis_index("hi"), lax.axis_index("lo")

    def to_hi(index):
        return {"hi": index}

    def to_lo(bit):
        return {"lo": lo ^ bit}

    barrier = pltpu.get_barrier_semaphore()
    for s in range(1, n_hi):
        pl.semaphore_signal(
            barrier, inc=1, device_id=to_hi(lax.rem(hi + s, n_hi)), device_id_type=MESH
        )
    for bit in (1, 2):
        pl.semaphore_signal(barrier, inc=1, device_id=to_lo(bit), device_id_type=MESH)
    pl.semaphore_wait(barrier, n_hi + 1)

    def rows_of(out, hi_index, lo_index, start, size):
        block = out.shape[0] // (n_hi * n_lo)
        return out.at[pl.ds((hi_index * n_lo + lo_index) * block + start, size)]

    def columns_of(w, index):
        width = w.shape[1] // n_hi
        return w.at[:, pl.ds(pl.multiple_of(index * width, 128), width)]

    def remote(src, dst, send, recv, where):
        return pltpu.make_async_remote_copy(
            src_ref=src, dst_ref=dst, send_sem=send, recv_sem=recv,
            device_id=where, device_id_type=MESH,
        )

    block = w_refs[0].shape[0]
    half = block // 2

    def a_copy(w, s):
        there = lax.rem(hi + s, n_hi)
        return remote(
            columns_of(w_refs[w], there), rows_of(outs[w], hi, lo, 0, block),
            a_send.at[w, s - 1], a_recv.at[w, s - 1], to_hi(there),
        )

    def b_copy(w, k, bit):
        from_hi = lax.rem(hi + n_hi - k, n_hi)
        dst = rows_of(outs[w], from_hi, lo, 0, block)
        src = columns_of(w_refs[w], hi) if k == 0 else dst
        return remote(src, dst, b_send.at[w, k, bit - 1], b_recv.at[w, k, bit - 1], to_lo(bit))

    def c_copy(w, k, bit):
        from_hi = lax.rem(hi + n_hi - k, n_hi)
        part = rows_of(outs[w], from_hi, lo ^ bit, (bit - 1) * half, half)
        return remote(
            part, part, c_send.at[w, k, bit - 1], c_recv.at[w, k, bit - 1], to_lo(3 - bit)
        )

    def x_copy(x, s):
        there = lax.rem(hi + s, n_hi)
        rows = x_refs[x].shape[0]
        return remote(
            x_refs[x], x_outs[x].at[pl.ds(hi * rows, rows)],
            x_send.at[x, s - 1], x_recv.at[x, s - 1], to_hi(there),
        )

    def own_in(w):
        return pltpu.make_async_copy(columns_of(w_refs[w], hi), holds[w], own_sem.at[w])

    def own_out(w):
        return pltpu.make_async_copy(
            holds[w], rows_of(outs[w], hi, lo, 0, block), own_sem.at[w]
        )

    def x_in(x):
        return pltpu.make_async_copy(x_refs[x], holds[n_w + x], x_own.at[x])

    def x_out(x):
        rows = x_refs[x].shape[0]
        return pltpu.make_async_copy(
            holds[n_w + x], x_outs[x].at[pl.ds(hi * rows, rows)], x_own.at[x]
        )

    for w in range(n_w):
        own_in(w).start()
    for x in range(n_x):
        x_in(x).start()
    for s in range(1, n_hi):
        a_copy(0, s).start()
    for bit in (1, 2):
        b_copy(0, 0, bit).start()
    for x in range(n_x):
        for s in range(1, n_hi):
            x_copy(x, s).start()
    for w in range(1, min(2, n_w)):
        for s in range(1, n_hi):
            a_copy(w, s).start()
    for w in range(n_w):
        own_in(w).wait()
        own_out(w).start()
    for x in range(n_x):
        x_in(x).wait()
        x_out(x).start()

    steps = [(w, k) for w in range(n_w) for k in range(n_hi)]

    def forward(w, k):
        for bit in (1, 2):
            b_copy(w, k, bit).wait_recv()
            c_copy(w, k, bit).start()

    for n, (w, k) in enumerate(steps):
        if k == 0 and w >= 1 and w + 1 < n_w:
            for s in range(1, n_hi):
                a_copy(w + 1, s).start()
        if n > 0:
            if k > 0:
                a_copy(w, k).wait_recv()
            for bit in (1, 2):
                b_copy(w, k, bit).start()
            forward(*steps[n - 1])
    forward(*steps[-1])
    for w, k in steps:
        for bit in (1, 2):
            c_copy(w, k, bit).wait_recv()
    for w in range(n_w):
        own_out(w).wait()
        for s in range(1, n_hi):
            a_copy(w, s).wait_send()
    for w, k in steps:
        for bit in (1, 2):
            b_copy(w, k, bit).wait_send()
            c_copy(w, k, bit).wait_send()
    for x in range(n_x):
        x_out(x).wait()
        for s in range(1, n_hi):
            x_copy(x, s).wait_recv()
            x_copy(x, s).wait_send()


def stream(weights, blocks, collective_id):
    n_hi, n_lo = lax.axis_size("hi"), lax.axis_size("lo")
    n_w, n_x = len(weights), len(blocks)
    dma = pltpu.SemaphoreType.DMA
    out_shape = [
        jax.ShapeDtypeStruct((w.shape[0] * n_hi * n_lo, w.shape[1] // n_hi), w.dtype)
        for w in weights
    ] + [jax.ShapeDtypeStruct((x.shape[0] * n_hi, x.shape[1]), x.dtype) for x in blocks]
    holds = [pltpu.VMEM((w.shape[0], w.shape[1] // n_hi), w.dtype) for w in weights]
    holds += [pltpu.VMEM(x.shape, x.dtype) for x in blocks]
    n_x1 = max(n_x, 1)
    out = pl.pallas_call(
        functools.partial(stream_body, n_w, n_x),
        out_shape=out_shape,
        in_specs=[pl.BlockSpec(memory_space=pl.ANY)] * (n_w + n_x),
        out_specs=[pl.BlockSpec(memory_space=pl.ANY)] * (n_w + n_x),
        scratch_shapes=[
            dma((n_w,)), dma((n_w, n_hi - 1)), dma((n_w, n_hi - 1)),
            dma((n_w, n_hi, 2)), dma((n_w, n_hi, 2)), dma((n_w, n_hi, 2)), dma((n_w, n_hi, 2)),
            dma((n_x1,)), dma((n_x1, n_hi - 1)), dma((n_x1, n_hi - 1)),
        ] + holds,
        compiler_params=pltpu.CompilerParams(
            collective_id=collective_id, has_side_effects=True
        ),
    )(*weights, *blocks)
    return out[:n_w], out[n_w:]


def on_device_columns(
    hidden_in, lengths, norm_attn, q_weight, k_weight, v_weight, out_weight_t, norm_ffn,
    gate_weight, up_weight, down_weight_t, scale_key, scale_value, scale_ffn, out_grad,
    position_bias,
):
    f32, bf16 = jnp.float32, jnp.bfloat16
    n_hi, n_lo = lax.axis_size("hi"), lax.axis_size("lo")
    hi, lo, mp = lax.axis_index("hi"), lax.axis_index("lo"), lax.axis_index("mp")
    d_model = norm_attn.shape[0]
    tokens_local, share = hidden_in.shape
    seq_local = lengths.shape[0]
    seq_len = tokens_local // seq_local
    tokens = n_hi * tokens_local

    def swap_lo(x, bit):
        return lax.ppermute(x, "lo", [(i, i ^ bit) for i in range(n_lo)])

    def swap_hi(x, bit):
        return lax.ppermute(x, "hi", [(i, i ^ bit) for i in range(n_hi)])

    def swap_mp(x):
        return lax.ppermute(x, "mp", [(0, 1), (1, 0)])

    def own_columns(x):
        width = x.shape[-1] // n_hi
        return lax.dynamic_slice_in_dim(x, hi * width, width, x.ndim - 1)

    def times(x, w):
        return jnp.dot(x, w, preferred_element_type=f32)

    def join_features(own):
        other = swap_mp(own)
        lower = jnp.where(mp == 0, own, other)
        upper = jnp.where(mp == 0, other, own)
        return jnp.concatenate([lower, upper], axis=1)

    def gather_tokens(x):
        return join_features(lax.all_gather(x, "hi", axis=0, tiled=True))

    def back_sum(pairs):
        total = None
        for x, w in pairs:
            term = contract_last(x, w)
            total = term if total is None else total + term
        mine = lax.dynamic_slice_in_dim(total, mp * share, share, 1)
        theirs = lax.dynamic_slice_in_dim(total, (1 - mp) * share, share, 1)
        both = (mine + swap_mp(theirs.astype(bf16)).astype(f32)).astype(bf16)
        return lax.psum_scatter(both, "hi", scatter_dimension=0, tiled=True).astype(f32)

    def token_mean(x):
        part = jnp.sum(x, axis=-1, keepdims=True)
        return (part + swap_mp(part)) / d_model

    def own_half(gain):
        return lax.dynamic_slice_in_dim(gain, mp * share, share, 0)[None]

    gain_ffn = own_half(norm_ffn)
    gain_attn_half = own_half(norm_attn)
    gain_attn = norm_attn[None]
    key_scale, value_scale = own_columns(scale_key), own_columns(scale_value)
    ffn_scale = own_columns(scale_ffn)

    inputs_half = hidden_in
    grad_half = lax.dynamic_slice_in_dim(out_grad, mp * share, share, 1)
    all_lengths = lax.all_gather(lengths, "hi", axis=0, tiled=True)

    (q_w, k_w, v_w, o_w, gate_w, up_w, down_w), (inputs_own, grad_own) = stream(
        [q_weight, k_weight, v_weight, out_weight_t, gate_weight, up_weight, down_weight_t],
        [inputs_half, grad_half], 0,
    )
    inputs32 = join_features(inputs_own).astype(f32)
    inv_first = lax.rsqrt(
        jnp.sum(inputs32 * inputs32, axis=-1, keepdims=True) / d_model + EPSILON
    )
    normed_first = (inputs32 * inv_first * gain_attn).astype(bf16)
    queries = times(normed_first, q_w).astype(bf16)
    key_pre = times(normed_first, k_w)
    value_pre = times(normed_first, v_w)
    n_seq = n_hi * seq_local
    heads_local = queries.shape[1] // HEAD_DIM
    shaped = (n_seq, seq_len, heads_local, HEAD_DIM)
    key_rows = (key_pre * key_scale).astype(bf16)
    value_rows = (value_pre * value_scale).astype(bf16)
    q_heads = queries.reshape(shaped)
    k_heads = key_rows.reshape(shaped)
    v_heads = value_rows.reshape(shaped)
    bias = lax.dynamic_slice_in_dim(position_bias, hi * heads_local, heads_local, 0)
    scores = (
        jnp.einsum("bihe,bjhe->bhij", q_heads, k_heads, preferred_element_type=f32)
        + bias[None]
    )
    positions = lax.broadcasted_iota(jnp.int32, (n_seq, seq_len), 1)
    valid_keys = positions < all_lengths[:, None]
    scores = jnp.where(valid_keys[:, None, None, :], scores, NEGATIVE)
    largest = jnp.max(scores, axis=-1, keepdims=True)
    exponent = jnp.exp(scores - largest)
    attn_probs = exponent / jnp.sum(exponent, axis=-1, keepdims=True)
    probs_low = attn_probs.astype(bf16)
    context = (
        jnp.einsum("bhij,bjhe->bihe", probs_low, v_heads, preferred_element_type=f32)
        .reshape(tokens, -1)
        .astype(bf16)
    )
    first_sum = inputs_half.astype(f32) + back_sum([(context, o_w)])
    inv_second = lax.rsqrt(token_mean(first_sum * first_sum) + EPSILON)
    normed_second = gather_tokens((first_sum * inv_second * gain_ffn).astype(bf16))
    grad_all = join_features(grad_own)
    gate_proj = times(normed_second, gate_w)
    upward = times(normed_second, up_w)
    d_hidden = times(grad_all, down_w)
    activated, gelu_back = jax.vjp(gelu_tanh, gate_proj)
    product = activated * upward
    hidden = (product * ffn_scale).astype(bf16)
    grad_ffn_part = jnp.sum(d_hidden * product, axis=0)
    d_product = d_hidden * ffn_scale
    d_gate = gelu_back(d_product * upward)[0].astype(bf16)
    d_up = (d_product * activated).astype(bf16)
    scaled = back_sum([(d_gate, gate_w), (d_up, up_w)]) * gain_ffn
    d_first = (
        grad_half.astype(f32)
        + inv_second * scaled
        - first_sum * inv_second * inv_second * inv_second * token_mean(scaled * first_sum)
    )
    d_context = times(gather_tokens(d_first.astype(bf16)), o_w).astype(bf16)
    dc_heads = d_context.reshape(shaped)
    d_probs = jnp.einsum("bihe,bjhe->bhij", dc_heads, v_heads, preferred_element_type=f32)
    d_scores = (
        attn_probs * (d_probs - jnp.sum(attn_probs * d_probs, axis=-1, keepdims=True))
    ).astype(bf16)
    d_values = jnp.einsum(
        "bhij,bihe->bjhe", probs_low, dc_heads, preferred_element_type=f32
    ).reshape(tokens, -1)
    d_keys = jnp.einsum(
        "bhij,bihe->bjhe", d_scores, q_heads, preferred_element_type=f32
    ).reshape(tokens, -1)
    d_queries = (
        jnp.einsum("bhij,bjhe->bihe", d_scores, k_heads, preferred_element_type=f32)
        .reshape(tokens, -1)
        .astype(bf16)
    )
    grad_key_part = jnp.sum(d_keys * key_pre, axis=0)
    grad_value_part = jnp.sum(d_values * value_pre, axis=0)
    d_key_pre = (d_keys * key_scale).astype(bf16)
    d_value_pre = (d_values * value_scale).astype(bf16)
    scaled_in = (
        back_sum([(d_queries, q_w), (d_key_pre, k_w), (d_value_pre, v_w)]) * gain_attn_half
    )
    mine32 = inputs_half.astype(f32)
    inv_mine = lax.dynamic_slice_in_dim(inv_first, hi * tokens_local, tokens_local, 0)
    mean_dot = token_mean(scaled_in * mine32)
    input_grad = (
        d_first
        + inv_mine * scaled_in
        - mine32 * inv_mine * inv_mine * inv_mine * mean_dot
    ).astype(bf16)
    block_out = (first_sum + back_sum([(hidden, down_w)])).astype(bf16)

    def totals(part):
        part = part[None]
        for bit in (1, 2):
            part = part + swap_lo(part, bit)
        for bit in (1, 2):
            other = swap_hi(part, bit)
            upper = (hi & bit) > 0
            part = jnp.concatenate(
                [jnp.where(upper, other, part), jnp.where(upper, part, other)], axis=0
            )
        return part

    attn_totals = totals(jnp.concatenate([grad_key_part, grad_value_part]))
    width = grad_key_part.shape[0]
    return (
        block_out,
        input_grad,
        attn_totals[:, :width].reshape(-1),
        attn_totals[:, width:].reshape(-1),
        totals(grad_ffn_part).reshape(-1),
    )


def solution(mesh):
    n_dp, n_mp = mesh.shape["dp"], mesh.shape["mp"]
    n_hi = 1
    while n_dp % (n_hi * 2) == 0 and n_hi * n_hi < n_dp:
        n_hi *= 2
    grid = jax.sharding.Mesh(
        mesh.devices.reshape(n_hi, n_dp // n_hi, n_mp), ("hi", "lo", "mp")
    )
    dp = ("hi", "lo")
    weight = P(dp, "mp")
    columns = (n_hi, n_dp // n_hi, n_mp) == (4, 4, 2)
    return jax.shard_map(
        on_device_columns if columns else on_device_general,
        mesh=grid,
        in_specs=(
            P(dp, "mp"), P(dp), P(), weight, weight, weight, weight, P(), weight, weight, weight,
            P("mp"), P("mp"), P("mp"), P(dp, None), P("mp", None, None),
        ),
        out_specs=(P(dp, "mp"), P(dp, "mp"), P("mp"), P("mp"), P("mp")),
        check_vma=False,
    )
```

```python
import functools

import jax
import jax.numpy as jnp
from jax import lax
from jax.experimental import pallas as pl
from jax.experimental.pallas import tpu as pltpu
from jax.sharding import PartitionSpec as P

HEAD_DIM = 64
MESH = pl.DeviceIdType.MESH


EPSILON = 1e-06
NEGATIVE = -1e30


def inverse_rms(values):
    return lax.rsqrt(jnp.mean(values * values, axis=-1, keepdims=True) + EPSILON)


def gelu_tanh(values):
    return jax.nn.gelu(values, approximate=True)


def contract_last(left_side, right_side):
    return lax.dot_general(
        left_side, right_side, (((1,), (1,)), ((), ())), preferred_element_type=jnp.float32
    )


def norm_back(grad_in, values, inverse, gain_vec):
    scaled = grad_in * gain_vec
    correction = (
        values * inverse * inverse * inverse * jnp.mean(scaled * values, axis=-1, keepdims=True)
    )
    return inverse * scaled - correction


WEIGHT_AXIS = "lo"


def on_device_general(
    hidden_in, lengths, norm_attn, q_weight, k_weight, v_weight, out_weight_t, norm_ffn,
    gate_weight, up_weight, down_weight_t, scale_key, scale_value, scale_ffn, out_grad,
    position_bias,
):
    f32, bf16 = jnp.float32, jnp.bfloat16
    wa = WEIGHT_AXIS
    ta = "lo" if wa == "hi" else "hi"
    n_hi, n_lo = lax.axis_size("hi"), lax.axis_size("lo")
    n_t = lax.axis_size(ta)

    def swap(x, bit):
        return lax.ppermute(x, "lo", [(i, i ^ bit) for i in range(n_lo)])

    def own_first(parts):
        if n_lo != 4:
            return parts
        index = lax.axis_index("lo")
        rows, width = parts.shape[0], parts.shape[-1]
        parts = parts.reshape(rows, n_hi, 2, 2, width)
        parts = jnp.where((index & 2) > 0, parts[:, :, ::-1], parts)
        parts = jnp.where((index & 1) > 0, parts[:, :, :, ::-1], parts)
        return parts.reshape(rows, n_hi, n_lo, width)

    def sum_mp(x):
        x = x.astype(bf16)
        if lax.axis_size("mp") != 2:
            return lax.psum(x, "mp").astype(f32)
        return x.astype(f32) + lax.ppermute(x, "mp", [(0, 1), (1, 0)]).astype(f32)

    def split_features(x):
        rows = x.shape[0]
        parts = own_first(x.reshape(rows, n_hi, n_lo, -1))
        order = (1, 0, 2, 3) if ta == "hi" else (2, 0, 1, 3)
        return parts.transpose(order).reshape(n_t, rows, -1)

    def join_features(x):
        rows = x.shape[1]
        if ta == "hi":
            parts = x.transpose(1, 0, 2).reshape(rows, n_hi, n_lo, -1)
            return own_first(parts).reshape(rows, -1)
        return x.reshape(n_lo, rows, n_hi, -1).transpose(1, 2, 0, 3).reshape(rows, -1)

    def exchange(x):
        return lax.all_to_all(x, ta, split_axis=0, concat_axis=0, tiled=True)

    def gather_rows(w):
        if n_lo != 4:
            return lax.all_gather(w, wa, axis=0, tiled=True)
        half = w.shape[0] // 2
        first, second = swap(w, 1), swap(w, 2)
        third = swap(second[:half], 1), swap(first[half:], 2)
        return jnp.concatenate([w, first, second, *third], axis=0)

    def gather_tokens(x):
        return lax.all_gather(x, ta, axis=0, tiled=True)

    def scatter_tokens(x):
        return lax.psum_scatter(x.astype(bf16), ta, scatter_dimension=0, tiled=True)

    def dot(a, b):
        return jnp.dot(a, b, preferred_element_type=f32)

    d_model = norm_attn.shape[0]
    tokens_local = hidden_in.shape[0]
    seq_local = lengths.shape[0]
    seq_len = tokens_local // seq_local
    t_index = lax.axis_index(ta)
    gain_attn = split_features(norm_attn[None])
    gain_attn = lax.dynamic_index_in_dim(gain_attn, t_index, 0, False)
    gain_ffn = split_features(norm_ffn[None])
    gain_ffn = lax.dynamic_index_in_dim(gain_ffn, t_index, 0, False)

    full_inputs = lax.all_gather(hidden_in, "mp", axis=1, tiled=True)
    both = jnp.concatenate([split_features(full_inputs), split_features(out_grad)], axis=2)
    both = exchange(both).reshape(n_t * tokens_local, -1)
    inputs_blk, out_grad_blk = jnp.split(both, 2, axis=1)
    inputs32 = inputs_blk.astype(f32)

    def token_mean(x):
        return lax.psum(jnp.sum(x, axis=-1, keepdims=True), ta) / d_model

    q_full, k_full, v_full = gather_rows(q_weight), gather_rows(k_weight), gather_rows(v_weight)
    o_full = gather_rows(out_weight_t)
    gate_full, up_full = gather_rows(gate_weight), gather_rows(up_weight)
    down_full = gather_rows(down_weight_t)

    inv_first = lax.rsqrt(token_mean(inputs32 * inputs32) + EPSILON)
    normed_first = (inputs32 * inv_first * gain_attn).astype(bf16)
    queries = scatter_tokens(dot(normed_first, q_full))
    key_pre = scatter_tokens(dot(normed_first, k_full)).astype(f32)
    value_pre = scatter_tokens(dot(normed_first, v_full)).astype(f32)
    heads_local = queries.shape[1] // HEAD_DIM
    shaped = (seq_local, seq_len, heads_local, HEAD_DIM)
    key_rows = (key_pre * scale_key).astype(bf16)
    value_rows = (value_pre * scale_value).astype(bf16)
    q_heads = queries.reshape(shaped)
    k_heads = key_rows.reshape(shaped)
    v_heads = value_rows.reshape(shaped)
    scores = (
        jnp.einsum("bihe,bjhe->bhij", q_heads, k_heads, preferred_element_type=f32)
        + position_bias[None]
    )
    positions = lax.broadcasted_iota(jnp.int32, (seq_local, seq_len), 1)
    valid_keys = positions < lengths[:, None]
    scores = jnp.where(valid_keys[:, None, None, :], scores, NEGATIVE)
    largest = jnp.max(scores, axis=-1, keepdims=True)
    exponent = jnp.exp(scores - largest)
    attn_probs = exponent / jnp.sum(exponent, axis=-1, keepdims=True)
    probs_low = attn_probs.astype(bf16)
    context = (
        jnp.einsum("bhij,bjhe->bihe", probs_low, v_heads, preferred_element_type=f32)
        .reshape(tokens_local, -1)
        .astype(bf16)
    )
    first_sum = inputs32 + sum_mp(contract_last(gather_tokens(context), o_full))
    inv_second = lax.rsqrt(token_mean(first_sum * first_sum) + EPSILON)
    normed_second = (first_sum * inv_second * gain_ffn).astype(bf16)
    gate_proj = scatter_tokens(dot(normed_second, gate_full)).astype(f32)
    upward = scatter_tokens(dot(normed_second, up_full)).astype(f32)
    d_hidden = scatter_tokens(dot(out_grad_blk, down_full)).astype(f32)
    activated, gelu_back = jax.vjp(gelu_tanh, gate_proj)
    product = activated * upward
    hidden = (product * scale_ffn).astype(bf16)
    grad_ffn_part = jnp.sum(d_hidden * product, axis=0)
    d_product = d_hidden * scale_ffn
    d_gate = gelu_back(d_product * upward)[0].astype(bf16)
    d_up = (d_product * activated).astype(bf16)
    d_second = sum_mp(
        contract_last(gather_tokens(d_gate), gate_full)
        + contract_last(gather_tokens(d_up), up_full)
    )
    scaled = d_second * gain_ffn
    d_first = (
        out_grad_blk.astype(f32)
        + inv_second * scaled
        - first_sum * inv_second * inv_second * inv_second * token_mean(scaled * first_sum)
    )
    d_context = scatter_tokens(dot(d_first.astype(bf16), o_full))
    dc_heads = d_context.reshape(shaped)
    d_probs = jnp.einsum("bihe,bjhe->bhij", dc_heads, v_heads, preferred_element_type=f32)
    d_scores = (
        attn_probs * (d_probs - jnp.sum(attn_probs * d_probs, axis=-1, keepdims=True))
    ).astype(bf16)
    d_values = jnp.einsum(
        "bhij,bihe->bjhe", probs_low, dc_heads, preferred_element_type=f32
    ).reshape(tokens_local, -1)
    d_keys = jnp.einsum(
        "bhij,bihe->bjhe", d_scores, q_heads, preferred_element_type=f32
    ).reshape(tokens_local, -1)
    d_queries = (
        jnp.einsum("bhij,bjhe->bihe", d_scores, k_heads, preferred_element_type=f32)
        .reshape(tokens_local, -1)
        .astype(bf16)
    )
    grad_key_part = jnp.sum(d_keys * key_pre, axis=0)
    grad_value_part = jnp.sum(d_values * value_pre, axis=0)
    d_key_pre = (d_keys * scale_key).astype(bf16)
    d_value_pre = (d_values * scale_value).astype(bf16)
    d_normed = sum_mp(
        contract_last(gather_tokens(d_queries), q_full)
        + contract_last(gather_tokens(d_key_pre), k_full)
        + contract_last(gather_tokens(d_value_pre), v_full)
    )
    scaled_in = d_normed * gain_attn
    mean_dot = token_mean(scaled_in * inputs32)
    input_grad = (
        d_first
        + inv_first * scaled_in
        - inputs32 * inv_first * inv_first * inv_first * mean_dot
    ).astype(bf16)

    ffn_out = sum_mp(contract_last(gather_tokens(hidden), down_full))
    block_out = (first_sum + ffn_out).astype(bf16)

    share_width = hidden_in.shape[1]
    offset = lax.axis_index("mp") * share_width

    def own_share(x):
        joined = join_features(exchange(x.reshape(n_t, tokens_local, -1)))
        return lax.dynamic_slice_in_dim(joined, offset, share_width, 1)

    parts = jnp.concatenate([grad_key_part, grad_value_part, grad_ffn_part])
    totals = lax.psum(lax.psum(parts, "lo"), "hi")
    width = grad_key_part.shape[0]
    return (
        own_share(block_out),
        own_share(input_grad),
        totals[:width],
        totals[width : 2 * width],
        totals[2 * width :],
    )


class Moves:
    def __init__(self, weights, outs, holds, sems, order):
        self.weights, self.outs, self.holds, self.order = weights, outs, holds, order
        self.own, self.asend, self.arecv, self.bsend, self.brecv, self.csend, self.crecv = sems
        self.n_hi, self.n_lo = lax.axis_size("hi"), lax.axis_size("lo")
        self.hi, self.lo = lax.axis_index("hi"), lax.axis_index("lo")
        self.mp = lax.axis_index("mp")
        self.block = weights[0].shape[0]
        self.next = 0

    def barrier(self):
        barrier = pltpu.get_barrier_semaphore()
        places = [{"hi": lax.rem(self.hi + s, self.n_hi)} for s in range(1, self.n_hi)]
        places += [{"lo": self.lo ^ 1}, {"lo": self.lo ^ 2}, {"mp": 1 - self.mp}]
        for place in places:
            pl.semaphore_signal(barrier, inc=1, device_id=place, device_id_type=MESH)
        pl.semaphore_wait(barrier, len(places))

    def back(self, k):
        return lax.rem(self.hi + self.n_hi - k, self.n_hi)

    def rows(self, w, hi, lo, start=0, size=None):
        first = (hi * self.n_lo + lo) * self.block + start
        return self.outs[w].at[pl.ds(first, size or self.block)]

    def columns(self, w, index):
        width = self.weights[w].shape[1] // self.n_hi
        return self.weights[w].at[:, pl.ds(pl.multiple_of(index * width, 128), width)]

    def a(self, w, s):
        there = lax.rem(self.hi + s, self.n_hi)
        return remote(
            self.columns(w, there), self.rows(w, self.hi, self.lo),
            self.asend.at[w, s - 1], self.arecv.at[w, s - 1], {"hi": there},
        )

    def b(self, w, k, bit):
        dst = self.rows(w, self.back(k), self.lo)
        src = self.columns(w, self.hi) if k == 0 else dst
        return remote(
            src, dst, self.bsend.at[w, k, bit - 1], self.brecv.at[w, k, bit - 1],
            {"lo": self.lo ^ bit},
        )

    def c(self, w, k, bit):
        half = self.block // 2
        part = self.rows(w, self.back(k), self.lo ^ bit, (bit - 1) * half, half)
        return remote(
            part, part, self.csend.at[w, k, bit - 1], self.crecv.at[w, k, bit - 1],
            {"lo": self.lo ^ (3 - bit)},
        )

    def exchange(self, w):
        for s in range(1, self.n_hi):
            self.a(w, s).start()

    def own_in(self, w):
        return pltpu.make_async_copy(self.columns(w, self.hi), self.holds[w], self.own.at[w])

    def own_out(self, w):
        return pltpu.make_async_copy(
            self.holds[w], self.rows(w, self.hi, self.lo), self.own.at[w]
        )

    def start_own(self):
        for w in range(len(self.weights)):
            self.own_in(w).start()

    def place_own(self):
        for w in range(len(self.weights)):
            self.own_in(w).wait()
            self.own_out(w).start()

    def relay(self, n):
        w, k = self.order[n]
        for bit in (1, 2):
            self.b(w, k, bit).wait_recv()
            self.c(w, k, bit).start()

    def advance(self, count=1):
        for _ in range(count):
            n = self.next
            if n < len(self.order):
                w, k = self.order[n]
                if k > 0:
                    self.a(w, k).wait_recv()
                for bit in (1, 2):
                    self.b(w, k, bit).start()
            if n >= 2:
                self.relay(n - 2)
            self.next = n + 1

    def arrived(self, w):
        for k in range(self.n_hi):
            for bit in (1, 2):
                self.c(w, k, bit).wait_recv()
        self.own_out(w).wait()

    def drain(self):
        for w in range(len(self.weights)):
            for s in range(1, self.n_hi):
                self.a(w, s).wait_send()
            for k in range(self.n_hi):
                for bit in (1, 2):
                    self.b(w, k, bit).wait_send()
                    self.c(w, k, bit).wait_send()


class Tokens:
    def __init__(self, moves, src, out, sems):
        self.m, self.src, self.out = moves, src, out
        self.hsend, self.hrecv, self.msend, self.mrecv = sems

    def place(self, origin):
        rows, width = self.src.shape
        return self.out.at[
            pl.ds(origin * rows, rows), pl.ds(pl.multiple_of(self.m.mp * width, 128), width)
        ]

    def far(self, s):
        there = lax.rem(self.m.hi + s, self.m.n_hi)
        return remote(
            self.src, self.place(self.m.hi), self.hsend.at[s - 1], self.hrecv.at[s - 1],
            {"hi": there},
        )

    def near(self, s):
        place = self.place(self.m.back(s))
        return remote(
            self.src if s == 0 else place, place, self.msend.at[s], self.mrecv.at[s],
            {"mp": 1 - self.m.mp},
        )

    def send(self):
        for s in range(1, self.m.n_hi):
            self.far(s).start()
        self.near(0).start()

    def relay(self):
        for s in range(1, self.m.n_hi):
            self.far(s).wait_recv()
            self.near(s).start()

    def finish(self):
        for s in range(self.m.n_hi):
            self.near(s).wait_recv()
        for s in range(self.m.n_hi):
            self.near(s).wait_send()
        for s in range(1, self.m.n_hi):
            self.far(s).wait_send()


def remote(src, dst, send, recv, where):
    return pltpu.make_async_remote_copy(
        src_ref=src, dst_ref=dst, send_sem=send, recv_sem=recv,
        device_id=where, device_id_type=MESH,
    )


def move_scratch(weights):
    n_hi, n_w = lax.axis_size("hi"), len(weights)
    dma = pltpu.SemaphoreType.DMA
    sems = [dma((n_w,)), dma((n_w, n_hi - 1)), dma((n_w, n_hi - 1))]
    sems += [dma((n_w, n_hi, 2)) for _ in range(4)]
    holds = [pltpu.VMEM((w.shape[0], w.shape[1] // n_hi), w.dtype) for w in weights]
    return sems + holds


def token_scratch():
    n_hi = lax.axis_size("hi")
    dma = pltpu.SemaphoreType.DMA
    return [dma((n_hi - 1,)), dma((n_hi - 1,)), dma((n_hi,)), dma((n_hi,))]


def gathered(w):
    n_hi, n_lo = lax.axis_size("hi"), lax.axis_size("lo")
    return jax.ShapeDtypeStruct((w.shape[0] * n_hi * n_lo, w.shape[1] // n_hi), w.dtype)


def first_body(q_w, k_w, v_w, x, mask, q_out, k_out, v_out, x_out, mask_out, *scratch):
    sems, holds, tok = scratch[:7], scratch[7:10], scratch[10:14]
    x_hold, mask_hold, here, m_send, m_recv = scratch[14:]
    order = [(w, 0) for w in range(3)] + [(w, k) for w in range(3) for k in (1, 2, 3)]
    m = Moves((q_w, k_w, v_w), (q_out, k_out, v_out), holds, sems, order)
    rows, mask_rows = x.shape[0], mask.shape[0]
    t = Tokens(m, x, x_out, tok)
    x_in = pltpu.make_async_copy(x, x_hold, here.at[0])
    x_put = pltpu.make_async_copy(x_hold, t.place(m.hi), here.at[0])
    mask_place = mask_out.at[pl.ds(m.hi * mask_rows, mask_rows)]
    mask_in = pltpu.make_async_copy(mask, mask_hold, here.at[1])
    mask_put = pltpu.make_async_copy(mask_hold, mask_place, here.at[1])

    def mask_copy(s):
        there = lax.rem(m.hi + s, m.n_hi)
        return remote(mask, mask_place, m_send.at[s - 1], m_recv.at[s - 1], {"hi": there})

    m.start_own()
    x_in.start()
    mask_in.start()
    m.barrier()
    m.exchange(0)
    m.advance(2)
    m.exchange(1)
    m.advance()
    m.place_own()
    x_in.wait()
    x_put.start()
    mask_in.wait()
    mask_put.start()
    m.exchange(2)
    for s in range(1, m.n_hi):
        mask_copy(s).start()
    t.send()
    m.advance(9)
    t.relay()
    m.advance(2)
    for w in range(3):
        m.arrived(w)
    t.finish()
    m.drain()
    x_put.wait()
    mask_put.wait()
    for s in range(1, m.n_hi):
        mask_copy(s).wait_recv()
        mask_copy(s).wait_send()


def first_kernel(weights, x, mask, collective_id):
    n_hi = lax.axis_size("hi")
    dma = pltpu.SemaphoreType.DMA
    any_spec = pl.BlockSpec(memory_space=pl.ANY)
    out_shape = [gathered(w) for w in weights] + [
        jax.ShapeDtypeStruct((x.shape[0] * n_hi, x.shape[1] * lax.axis_size("mp")), x.dtype),
        jax.ShapeDtypeStruct((mask.shape[0] * n_hi, mask.shape[1]), mask.dtype),
    ]
    return pl.pallas_call(
        first_body,
        out_shape=out_shape,
        in_specs=[any_spec] * 5,
        out_specs=[any_spec] * 5,
        scratch_shapes=move_scratch(weights) + token_scratch() + [
            pltpu.VMEM(x.shape, x.dtype), pltpu.VMEM(mask.shape, mask.dtype),
            dma((2,)), dma((n_hi - 1,)), dma((n_hi - 1,)),
        ],
        compiler_params=pltpu.CompilerParams(
            collective_id=collective_id, has_side_effects=True
        ),
    )(*weights, x, mask)


def second_body(
    o_w, gate_w, up_w, down_w, grad, normed, q_full, k_full, v_full, hidden, gain, bias, mask,
    key_scale, value_scale,
    o_out, gate_out, up_out, down_out, grad_out, second_out, q_out, key_pre, value_pre,
    key_rows, value_rows, probs_out, sum_out, inv_out,
    *scratch,
):
    f32, bf16 = jnp.float32, jnp.bfloat16
    sems, holds, g_tok, n_tok = scratch[:7], scratch[7:11], scratch[11:15], scratch[15:19]
    (o_full, context, theirs, arrived, mine, both, landed, second_own, grad_hold, stat, stat_in,
     here, x_send, x_recv, r_send, r_recv) = scratch[19:]
    order = [
        (0, 0), (1, 0), (0, 1), (0, 2), (0, 3), (2, 0), (1, 1), (1, 2), (1, 3), (3, 0),
        (2, 1), (2, 2), (2, 3), (3, 1), (3, 2), (3, 3),
    ]
    m = Moves((o_w, gate_w, up_w, down_w), (o_out, gate_out, up_out, down_out), holds, sems, order)
    rows, share = hidden.shape
    tokens, d_model = normed.shape
    seq_len = probs_out.shape[-1]
    partner = {"mp": 1 - m.mp}
    grad_half = grad.at[:, pl.ds(pl.multiple_of(m.mp * share, 128), share)]
    g = Tokens(m, grad_half, grad_out, g_tok)
    t = Tokens(m, second_own, second_out, n_tok)
    grad_in = pltpu.make_async_copy(grad_half, grad_hold, here.at[0])
    grad_put = pltpu.make_async_copy(grad_hold, g.place(m.hi), here.at[0])

    def project(w_ref, store):
        tile = 256

        def step(i, carry):
            cols = pl.ds(pl.multiple_of(i * tile, tile), tile)
            store(cols, jnp.dot(normed[...], w_ref[:, cols], preferred_element_type=f32))
            return carry

        lax.fori_loop(0, w_ref.shape[1] // tile, step, 0)

    def store_query(cols, value):
        q_out[:, cols] = value.astype(bf16)

    def store_key(cols, value):
        key_pre[:, cols] = value
        key_rows[:, cols] = (value * key_scale[:, cols]).astype(bf16)

    def store_value(cols, value):
        value_pre[:, cols] = value
        value_rows[:, cols] = (value * value_scale[:, cols]).astype(bf16)

    def attend(seq):
        where = pl.ds(seq * seq_len, seq_len)
        hidden_keys = mask[pl.ds(seq * 8, 8), :][:1] < 0.0
        low = lax.broadcasted_iota(jnp.int32, (seq_len, 2 * HEAD_DIM), 1) < HEAD_DIM
        zero = jnp.zeros((seq_len, 2 * HEAD_DIM), bf16)
        for pair in range(probs_out.shape[1] // 2):
            cols = slice(pair * 2 * HEAD_DIM, (pair + 1) * 2 * HEAD_DIM)
            q2, k2, v2 = q_out[where, cols], key_rows[where, cols], value_rows[where, cols]
            outs = []
            for e in range(2):
                head = 2 * pair + e
                qe = jnp.where(low, q2, zero) if e == 0 else jnp.where(low, zero, q2)
                scores = contract_last(qe, k2) + bias[head]
                scores = jnp.where(hidden_keys, NEGATIVE, scores)
                exponent = jnp.exp(scores - jnp.max(scores, axis=-1, keepdims=True))
                probs = exponent / jnp.sum(exponent, axis=-1, keepdims=True)
                probs_out[seq, head] = probs
                outs.append(jnp.dot(probs.astype(bf16), v2, preferred_element_type=f32))
            context[where, cols] = jnp.where(low, outs[0], outs[1]).astype(bf16)

    def attend_some(first, count):
        def step(i, carry):
            attend(first + i)
            return carry

        lax.fori_loop(0, count, step, 0)

    def out_project(first_row, store):
        tile = 256

        def step(i, carry):
            w_rows = pl.ds(pl.multiple_of(first_row + i * tile, tile), tile)
            cols = pl.ds(pl.multiple_of(i * tile, tile), tile)
            store(cols, contract_last(context[...], o_full[w_rows, :]))
            return carry

        lax.fori_loop(0, share // tile, step, 0)

    def store_theirs(cols, value):
        theirs[:, cols] = value.astype(bf16)

    def store_mine(cols, value):
        mine[:, cols] = value

    def by_rows(count, size, body):
        def step(i, carry):
            body(pl.ds(pl.multiple_of(i * size, size), size))
            return carry

        lax.fori_loop(0, count // size, step, 0)

    halves = remote(theirs, arrived, x_send.at[0], x_recv.at[0], partner)
    stats = remote(stat, stat_in, x_send.at[1], x_recv.at[1], partner)

    def reduce_copy(s):
        there = lax.rem(m.hi + s, m.n_hi)
        return remote(
            both.at[pl.ds(there * rows, rows)], landed.at[s - 1],
            r_send.at[s - 1], r_recv.at[s - 1], {"hi": there},
        )

    m.start_own()
    grad_in.start()
    m.barrier()
    m.exchange(0)
    m.exchange(1)
    m.advance(2)
    m.place_own()
    grad_in.wait()
    grad_put.start()
    project(q_full, store_query)
    m.advance()
    project(k_full, store_key)
    m.advance()
    project(v_full, store_value)
    m.advance()
    m.exchange(2)
    attend_some(0, tokens // seq_len // 2)
    m.advance()
    attend_some(tokens // seq_len // 2, tokens // seq_len // 2)
    m.advance()
    m.arrived(0)
    load = pltpu.make_async_copy(o_out, o_full, here.at[1])
    load.start()
    load.wait()
    out_project((1 - m.mp) * share, store_theirs)
    halves.start()
    out_project(m.mp * share, store_mine)
    m.advance()
    halves.wait_recv()

    def join(at):
        both[at, :] = (mine[at, :] + arrived[at, :].astype(f32)).astype(bf16)

    by_rows(tokens, 32, join)
    for s in range(1, m.n_hi):
        reduce_copy(s).start()
    m.exchange(3)
    m.advance(2)
    for s in range(1, m.n_hi):
        reduce_copy(s).wait_recv()

    def add(at):
        own = pl.ds(pl.multiple_of(m.hi * rows, rows) + at.start, at.size)
        total = hidden[at, :].astype(f32) + mine[own, :] + arrived[own, :].astype(f32)
        for s in range(m.n_hi - 1):
            total = total + landed[s, at, :].astype(f32)
        sum_out[at, :] = total
        square = jnp.sum(total * total, axis=-1, keepdims=True)
        stat[at, :] = jnp.broadcast_to(square, (at.size, stat.shape[1]))

    by_rows(rows, 32, add)
    stats.start()
    stats.wait_recv()

    def normalise(at):
        inverse = lax.rsqrt((stat[at, :] + stat_in[at, :]) / d_model + EPSILON)
        inv_out[at, :] = inverse
        second_own[at, :] = (sum_out[at, :] * inverse[:, :1] * gain[...]).astype(bf16)

    by_rows(rows, 32, normalise)
    t.send()
    second_put = pltpu.make_async_copy(second_own, t.place(m.hi), here.at[2])
    second_put.start()
    m.advance(2)
    g.send()
    m.advance()
    t.relay()
    m.advance(2)
    g.relay()
    m.advance(3)
    for w in (1, 2, 3):
        m.arrived(w)
    t.finish()
    g.finish()
    m.drain()
    second_put.wait()
    grad_put.wait()
    halves.wait_send()
    stats.wait_send()
    for s in range(1, m.n_hi):
        reduce_copy(s).wait_send()


def second_kernel(
    weights, grad, normed, q_full, k_full, v_full, hidden, gain, bias, mask, key_scale,
    value_scale, collective_id,
):
    f32, bf16 = jnp.float32, jnp.bfloat16
    n_hi = lax.axis_size("hi")
    dma = pltpu.SemaphoreType.DMA
    any_spec = pl.BlockSpec(memory_space=pl.ANY)
    vmem = pl.BlockSpec(memory_space=pltpu.VMEM)
    rows, share = hidden.shape
    tokens, d_model = normed.shape
    width = q_full.shape[1]
    heads, seq_len = bias.shape[0], bias.shape[1]
    array = jax.ShapeDtypeStruct
    out_shape = [gathered(w) for w in weights] + [
        array((tokens, d_model), bf16), array((tokens, d_model), bf16),
        array((tokens, width), bf16), array((tokens, width), f32), array((tokens, width), f32),
        array((tokens, width), bf16), array((tokens, width), bf16),
        array((tokens // seq_len, heads, seq_len, seq_len), f32),
        array((rows, share), f32), array((rows, 128), f32),
    ]
    return pl.pallas_call(
        second_body,
        out_shape=out_shape,
        in_specs=[any_spec] * 5 + [vmem] * 10,
        out_specs=[any_spec] * 6 + [vmem] * 8,
        scratch_shapes=move_scratch(weights) + token_scratch() + token_scratch() + [
            pltpu.VMEM((d_model, width), bf16), pltpu.VMEM((tokens, width), bf16),
            pltpu.VMEM((tokens, share), bf16), pltpu.VMEM((tokens, share), bf16),
            pltpu.VMEM((tokens, share), f32), pltpu.VMEM((tokens, share), bf16),
            pltpu.VMEM((n_hi - 1, rows, share), bf16), pltpu.VMEM((rows, share), bf16),
            pltpu.VMEM((rows, share), bf16), pltpu.VMEM((rows, 128), f32),
            pltpu.VMEM((rows, 128), f32),
            dma((3,)), dma((2,)), dma((2,)), dma((n_hi - 1,)), dma((n_hi - 1,)),
        ],
        compiler_params=pltpu.CompilerParams(
            collective_id=collective_id, has_side_effects=True, vmem_limit_bytes=63 * 2**20
        ),
    )(
        *weights, grad, normed, q_full, k_full, v_full, hidden, gain, bias, mask,
        key_scale, value_scale,
    )


def on_device_columns(
    hidden_in, lengths, norm_attn, q_weight, k_weight, v_weight, out_weight_t, norm_ffn,
    gate_weight, up_weight, down_weight_t, scale_key, scale_value, scale_ffn, out_grad,
    position_bias,
):
    f32, bf16 = jnp.float32, jnp.bfloat16
    n_hi, n_lo = lax.axis_size("hi"), lax.axis_size("lo")
    hi, lo, mp = lax.axis_index("hi"), lax.axis_index("lo"), lax.axis_index("mp")
    d_model = norm_attn.shape[0]
    tokens_local, share = hidden_in.shape
    seq_local = lengths.shape[0]
    seq_len = tokens_local // seq_local
    tokens = n_hi * tokens_local

    def swap_lo(x, bit):
        return lax.ppermute(x, "lo", [(i, i ^ bit) for i in range(n_lo)])

    def swap_hi(x, bit):
        return lax.ppermute(x, "hi", [(i, i ^ bit) for i in range(n_hi)])

    def swap_mp(x):
        return lax.ppermute(x, "mp", [(0, 1), (1, 0)])

    def own_columns(x):
        width = x.shape[-1] // n_hi
        return lax.dynamic_slice_in_dim(x, hi * width, width, x.ndim - 1)

    def times(x, w):
        return jnp.dot(x, w, preferred_element_type=f32)

    def join_features(own):
        other = swap_mp(own)
        lower = jnp.where(mp == 0, own, other)
        upper = jnp.where(mp == 0, other, own)
        return jnp.concatenate([lower, upper], axis=1)

    def gather_tokens(x):
        return join_features(lax.all_gather(x, "hi", axis=0, tiled=True))

    def back_sum(pairs):
        total = None
        for x, w in pairs:
            term = contract_last(x, w)
            total = term if total is None else total + term
        mine = lax.dynamic_slice_in_dim(total, mp * share, share, 1)
        theirs = lax.dynamic_slice_in_dim(total, (1 - mp) * share, share, 1)
        both = (mine + swap_mp(theirs.astype(bf16)).astype(f32)).astype(bf16)
        return lax.psum_scatter(both, "hi", scatter_dimension=0, tiled=True).astype(f32)

    def token_mean(x):
        part = jnp.sum(x, axis=-1, keepdims=True)
        return (part + swap_mp(part)) / d_model

    def own_half(gain):
        return lax.dynamic_slice_in_dim(gain, mp * share, share, 0)[None]

    gain_ffn = own_half(norm_ffn)
    gain_attn_half = own_half(norm_attn)
    gain_attn = norm_attn[None]
    key_scale, value_scale = own_columns(scale_key), own_columns(scale_value)
    ffn_scale = own_columns(scale_ffn)

    inputs_half = hidden_in
    grad_half = lax.dynamic_slice_in_dim(out_grad, mp * share, share, 1)
    keep = lax.broadcasted_iota(jnp.int32, (8 * seq_local, seq_len), 1) < lengths[0]
    mask = jnp.where(keep, 0.0, NEGATIVE)
    q_w, k_w, v_w, inputs_all, masks = first_kernel(
        (q_weight, k_weight, v_weight), hidden_in, mask, 0
    )
    inputs32 = inputs_all.astype(f32)
    inv_first = lax.rsqrt(
        jnp.sum(inputs32 * inputs32, axis=-1, keepdims=True) / d_model + EPSILON
    )
    normed_first = (inputs32 * inv_first * gain_attn).astype(bf16)
    heads_local = q_w.shape[1] // HEAD_DIM
    bias = lax.dynamic_slice_in_dim(position_bias, hi * heads_local, heads_local, 0)
    (
        o_w, gate_w, up_w, down_w, grad_all, normed_second, queries, key_pre, value_pre,
        key_rows, value_rows, attn_probs, first_sum, inv_second,
    ) = second_kernel(
        (out_weight_t, gate_weight, up_weight, down_weight_t), out_grad, normed_first,
        q_w, k_w, v_w, hidden_in, gain_ffn, bias, masks, key_scale[None], value_scale[None], 1,
    )
    inv_second = inv_second[:, :1]
    n_seq = n_hi * seq_local
    shaped = (n_seq, seq_len, heads_local, HEAD_DIM)
    q_heads = queries.reshape(shaped)
    k_heads = key_rows.reshape(shaped)
    v_heads = value_rows.reshape(shaped)
    probs_low = attn_probs.astype(bf16)
    gate_proj = times(normed_second, gate_w)
    upward = times(normed_second, up_w)
    d_hidden = times(grad_all, down_w)
    activated, gelu_back = jax.vjp(gelu_tanh, gate_proj)
    product = activated * upward
    hidden = (product * ffn_scale).astype(bf16)
    grad_ffn_part = jnp.sum(d_hidden * product, axis=0)
    d_product = d_hidden * ffn_scale
    d_gate = gelu_back(d_product * upward)[0].astype(bf16)
    d_up = (d_product * activated).astype(bf16)
    scaled = back_sum([(d_gate, gate_w), (d_up, up_w)]) * gain_ffn
    d_first = (
        grad_half.astype(f32)
        + inv_second * scaled
        - first_sum * inv_second * inv_second * inv_second * token_mean(scaled * first_sum)
    )
    d_context = times(gather_tokens(d_first.astype(bf16)), o_w).astype(bf16)
    dc_heads = d_context.reshape(shaped)
    d_probs = jnp.einsum("bihe,bjhe->bhij", dc_heads, v_heads, preferred_element_type=f32)
    d_scores = (
        attn_probs * (d_probs - jnp.sum(attn_probs * d_probs, axis=-1, keepdims=True))
    ).astype(bf16)
    d_values = jnp.einsum(
        "bhij,bihe->bjhe", probs_low, dc_heads, preferred_element_type=f32
    ).reshape(tokens, -1)
    d_keys = jnp.einsum(
        "bhij,bihe->bjhe", d_scores, q_heads, preferred_element_type=f32
    ).reshape(tokens, -1)
    d_queries = (
        jnp.einsum("bhij,bjhe->bihe", d_scores, k_heads, preferred_element_type=f32)
        .reshape(tokens, -1)
        .astype(bf16)
    )
    grad_key_part = jnp.sum(d_keys * key_pre, axis=0)
    grad_value_part = jnp.sum(d_values * value_pre, axis=0)
    d_key_pre = (d_keys * key_scale).astype(bf16)
    d_value_pre = (d_values * value_scale).astype(bf16)
    scaled_in = (
        back_sum([(d_queries, q_w), (d_key_pre, k_w), (d_value_pre, v_w)]) * gain_attn_half
    )
    mine32 = inputs_half.astype(f32)
    inv_mine = lax.dynamic_slice_in_dim(inv_first, hi * tokens_local, tokens_local, 0)
    mean_dot = token_mean(scaled_in * mine32)
    input_grad = (
        d_first
        + inv_mine * scaled_in
        - mine32 * inv_mine * inv_mine * inv_mine * mean_dot
    ).astype(bf16)
    block_out = (first_sum + back_sum([(hidden, down_w)])).astype(bf16)

    def totals(part):
        part = part[None]
        for bit in (1, 2):
            part = part + swap_lo(part, bit)
        for bit in (1, 2):
            other = swap_hi(part, bit)
            upper = (hi & bit) > 0
            part = jnp.concatenate(
                [jnp.where(upper, other, part), jnp.where(upper, part, other)], axis=0
            )
        return part

    attn_totals = totals(jnp.concatenate([grad_key_part, grad_value_part]))
    width = grad_key_part.shape[0]
    return (
        block_out,
        input_grad,
        attn_totals[:, :width].reshape(-1),
        attn_totals[:, width:].reshape(-1),
        totals(grad_ffn_part).reshape(-1),
    )


def solution(mesh):
    n_dp, n_mp = mesh.shape["dp"], mesh.shape["mp"]
    n_hi = 1
    while n_dp % (n_hi * 2) == 0 and n_hi * n_hi < n_dp:
        n_hi *= 2
    grid = jax.sharding.Mesh(
        mesh.devices.reshape(n_hi, n_dp // n_hi, n_mp), ("hi", "lo", "mp")
    )
    dp = ("hi", "lo")
    weight = P(dp, "mp")
    columns = (n_hi, n_dp // n_hi, n_mp) == (4, 4, 2)
    return jax.shard_map(
        on_device_columns if columns else on_device_general,
        mesh=grid,
        in_specs=(
            P(dp, "mp"), P(dp), P(), weight, weight, weight, weight, P(), weight, weight, weight,
            P("mp"), P("mp"), P("mp"), P(dp, None), P("mp", None, None),
        ),
        out_specs=(P(dp, "mp"), P(dp, "mp"), P("mp"), P("mp"), P("mp")),
        check_vma=False,
    )
```

```python
import functools

import jax
import jax.numpy as jnp
from jax import lax
from jax.experimental import pallas as pl
from jax.experimental.pallas import tpu as pltpu
from jax.sharding import PartitionSpec as P

HEAD_DIM = 64
MESH = pl.DeviceIdType.MESH


EPSILON = 1e-06
NEGATIVE = -1e30


def inverse_rms(values):
    return lax.rsqrt(jnp.mean(values * values, axis=-1, keepdims=True) + EPSILON)


def gelu_tanh(values):
    return jax.nn.gelu(values, approximate=True)


def contract_last(left_side, right_side):
    return lax.dot_general(
        left_side, right_side, (((1,), (1,)), ((), ())), preferred_element_type=jnp.float32
    )


def norm_back(grad_in, values, inverse, gain_vec):
    scaled = grad_in * gain_vec
    correction = (
        values * inverse * inverse * inverse * jnp.mean(scaled * values, axis=-1, keepdims=True)
    )
    return inverse * scaled - correction


WEIGHT_AXIS = "lo"


def on_device_general(
    hidden_in, lengths, norm_attn, q_weight, k_weight, v_weight, out_weight_t, norm_ffn,
    gate_weight, up_weight, down_weight_t, scale_key, scale_value, scale_ffn, out_grad,
    position_bias,
):
    f32, bf16 = jnp.float32, jnp.bfloat16
    wa = WEIGHT_AXIS
    ta = "lo" if wa == "hi" else "hi"
    n_hi, n_lo = lax.axis_size("hi"), lax.axis_size("lo")
    n_t = lax.axis_size(ta)

    def swap(x, bit):
        return lax.ppermute(x, "lo", [(i, i ^ bit) for i in range(n_lo)])

    def own_first(parts):
        if n_lo != 4:
            return parts
        index = lax.axis_index("lo")
        rows, width = parts.shape[0], parts.shape[-1]
        parts = parts.reshape(rows, n_hi, 2, 2, width)
        parts = jnp.where((index & 2) > 0, parts[:, :, ::-1], parts)
        parts = jnp.where((index & 1) > 0, parts[:, :, :, ::-1], parts)
        return parts.reshape(rows, n_hi, n_lo, width)

    def sum_mp(x):
        x = x.astype(bf16)
        if lax.axis_size("mp") != 2:
            return lax.psum(x, "mp").astype(f32)
        return x.astype(f32) + lax.ppermute(x, "mp", [(0, 1), (1, 0)]).astype(f32)

    def split_features(x):
        rows = x.shape[0]
        parts = own_first(x.reshape(rows, n_hi, n_lo, -1))
        order = (1, 0, 2, 3) if ta == "hi" else (2, 0, 1, 3)
        return parts.transpose(order).reshape(n_t, rows, -1)

    def join_features(x):
        rows = x.shape[1]
        if ta == "hi":
            parts = x.transpose(1, 0, 2).reshape(rows, n_hi, n_lo, -1)
            return own_first(parts).reshape(rows, -1)
        return x.reshape(n_lo, rows, n_hi, -1).transpose(1, 2, 0, 3).reshape(rows, -1)

    def exchange(x):
        return lax.all_to_all(x, ta, split_axis=0, concat_axis=0, tiled=True)

    def gather_rows(w):
        if n_lo != 4:
            return lax.all_gather(w, wa, axis=0, tiled=True)
        half = w.shape[0] // 2
        first, second = swap(w, 1), swap(w, 2)
        third = swap(second[:half], 1), swap(first[half:], 2)
        return jnp.concatenate([w, first, second, *third], axis=0)

    def gather_tokens(x):
        return lax.all_gather(x, ta, axis=0, tiled=True)

    def scatter_tokens(x):
        return lax.psum_scatter(x.astype(bf16), ta, scatter_dimension=0, tiled=True)

    def dot(a, b):
        return jnp.dot(a, b, preferred_element_type=f32)

    d_model = norm_attn.shape[0]
    tokens_local = hidden_in.shape[0]
    seq_local = lengths.shape[0]
    seq_len = tokens_local // seq_local
    t_index = lax.axis_index(ta)
    gain_attn = split_features(norm_attn[None])
    gain_attn = lax.dynamic_index_in_dim(gain_attn, t_index, 0, False)
    gain_ffn = split_features(norm_ffn[None])
    gain_ffn = lax.dynamic_index_in_dim(gain_ffn, t_index, 0, False)

    full_inputs = lax.all_gather(hidden_in, "mp", axis=1, tiled=True)
    both = jnp.concatenate([split_features(full_inputs), split_features(out_grad)], axis=2)
    both = exchange(both).reshape(n_t * tokens_local, -1)
    inputs_blk, out_grad_blk = jnp.split(both, 2, axis=1)
    inputs32 = inputs_blk.astype(f32)

    def token_mean(x):
        return lax.psum(jnp.sum(x, axis=-1, keepdims=True), ta) / d_model

    q_full, k_full, v_full = gather_rows(q_weight), gather_rows(k_weight), gather_rows(v_weight)
    o_full = gather_rows(out_weight_t)
    gate_full, up_full = gather_rows(gate_weight), gather_rows(up_weight)
    down_full = gather_rows(down_weight_t)

    inv_first = lax.rsqrt(token_mean(inputs32 * inputs32) + EPSILON)
    normed_first = (inputs32 * inv_first * gain_attn).astype(bf16)
    queries = scatter_tokens(dot(normed_first, q_full))
    key_pre = scatter_tokens(dot(normed_first, k_full)).astype(f32)
    value_pre = scatter_tokens(dot(normed_first, v_full)).astype(f32)
    heads_local = queries.shape[1] // HEAD_DIM
    shaped = (seq_local, seq_len, heads_local, HEAD_DIM)
    key_rows = (key_pre * scale_key).astype(bf16)
    value_rows = (value_pre * scale_value).astype(bf16)
    q_heads = queries.reshape(shaped)
    k_heads = key_rows.reshape(shaped)
    v_heads = value_rows.reshape(shaped)
    scores = (
        jnp.einsum("bihe,bjhe->bhij", q_heads, k_heads, preferred_element_type=f32)
        + position_bias[None]
    )
    positions = lax.broadcasted_iota(jnp.int32, (seq_local, seq_len), 1)
    valid_keys = positions < lengths[:, None]
    scores = jnp.where(valid_keys[:, None, None, :], scores, NEGATIVE)
    largest = jnp.max(scores, axis=-1, keepdims=True)
    exponent = jnp.exp(scores - largest)
    attn_probs = exponent / jnp.sum(exponent, axis=-1, keepdims=True)
    probs_low = attn_probs.astype(bf16)
    context = (
        jnp.einsum("bhij,bjhe->bihe", probs_low, v_heads, preferred_element_type=f32)
        .reshape(tokens_local, -1)
        .astype(bf16)
    )
    first_sum = inputs32 + sum_mp(contract_last(gather_tokens(context), o_full))
    inv_second = lax.rsqrt(token_mean(first_sum * first_sum) + EPSILON)
    normed_second = (first_sum * inv_second * gain_ffn).astype(bf16)
    gate_proj = scatter_tokens(dot(normed_second, gate_full)).astype(f32)
    upward = scatter_tokens(dot(normed_second, up_full)).astype(f32)
    d_hidden = scatter_tokens(dot(out_grad_blk, down_full)).astype(f32)
    activated, gelu_back = jax.vjp(gelu_tanh, gate_proj)
    product = activated * upward
    hidden = (product * scale_ffn).astype(bf16)
    grad_ffn_part = jnp.sum(d_hidden * product, axis=0)
    d_product = d_hidden * scale_ffn
    d_gate = gelu_back(d_product * upward)[0].astype(bf16)
    d_up = (d_product * activated).astype(bf16)
    d_second = sum_mp(
        contract_last(gather_tokens(d_gate), gate_full)
        + contract_last(gather_tokens(d_up), up_full)
    )
    scaled = d_second * gain_ffn
    d_first = (
        out_grad_blk.astype(f32)
        + inv_second * scaled
        - first_sum * inv_second * inv_second * inv_second * token_mean(scaled * first_sum)
    )
    d_context = scatter_tokens(dot(d_first.astype(bf16), o_full))
    dc_heads = d_context.reshape(shaped)
    d_probs = jnp.einsum("bihe,bjhe->bhij", dc_heads, v_heads, preferred_element_type=f32)
    d_scores = (
        attn_probs * (d_probs - jnp.sum(attn_probs * d_probs, axis=-1, keepdims=True))
    ).astype(bf16)
    d_values = jnp.einsum(
        "bhij,bihe->bjhe", probs_low, dc_heads, preferred_element_type=f32
    ).reshape(tokens_local, -1)
    d_keys = jnp.einsum(
        "bhij,bihe->bjhe", d_scores, q_heads, preferred_element_type=f32
    ).reshape(tokens_local, -1)
    d_queries = (
        jnp.einsum("bhij,bjhe->bihe", d_scores, k_heads, preferred_element_type=f32)
        .reshape(tokens_local, -1)
        .astype(bf16)
    )
    grad_key_part = jnp.sum(d_keys * key_pre, axis=0)
    grad_value_part = jnp.sum(d_values * value_pre, axis=0)
    d_key_pre = (d_keys * scale_key).astype(bf16)
    d_value_pre = (d_values * scale_value).astype(bf16)
    d_normed = sum_mp(
        contract_last(gather_tokens(d_queries), q_full)
        + contract_last(gather_tokens(d_key_pre), k_full)
        + contract_last(gather_tokens(d_value_pre), v_full)
    )
    scaled_in = d_normed * gain_attn
    mean_dot = token_mean(scaled_in * inputs32)
    input_grad = (
        d_first
        + inv_first * scaled_in
        - inputs32 * inv_first * inv_first * inv_first * mean_dot
    ).astype(bf16)

    ffn_out = sum_mp(contract_last(gather_tokens(hidden), down_full))
    block_out = (first_sum + ffn_out).astype(bf16)

    share_width = hidden_in.shape[1]
    offset = lax.axis_index("mp") * share_width

    def own_share(x):
        joined = join_features(exchange(x.reshape(n_t, tokens_local, -1)))
        return lax.dynamic_slice_in_dim(joined, offset, share_width, 1)

    parts = jnp.concatenate([grad_key_part, grad_value_part, grad_ffn_part])
    totals = lax.psum(lax.psum(parts, "lo"), "hi")
    width = grad_key_part.shape[0]
    return (
        own_share(block_out),
        own_share(input_grad),
        totals[:width],
        totals[width : 2 * width],
        totals[2 * width :],
    )


class Moves:
    def __init__(self, weights, outs, holds, sems, order):
        self.weights, self.outs, self.holds, self.order = weights, outs, holds, order
        self.own, self.asend, self.arecv, self.bsend, self.brecv, self.csend, self.crecv = sems
        self.n_hi, self.n_lo = lax.axis_size("hi"), lax.axis_size("lo")
        self.hi, self.lo = lax.axis_index("hi"), lax.axis_index("lo")
        self.mp = lax.axis_index("mp")
        self.block = weights[0].shape[0]
        self.next = 0

    def barrier(self):
        barrier = pltpu.get_barrier_semaphore()
        places = [{"hi": lax.rem(self.hi + s, self.n_hi)} for s in range(1, self.n_hi)]
        places += [{"lo": self.lo ^ 1}, {"lo": self.lo ^ 2}, {"mp": 1 - self.mp}]
        for place in places:
            pl.semaphore_signal(barrier, inc=1, device_id=place, device_id_type=MESH)
        pl.semaphore_wait(barrier, len(places))

    def back(self, k):
        return lax.rem(self.hi + self.n_hi - k, self.n_hi)

    def rows(self, w, hi, lo, start=0, size=None):
        first = (hi * self.n_lo + lo) * self.block + start
        return self.outs[w].at[pl.ds(first, size or self.block)]

    def columns(self, w, index):
        width = self.weights[w].shape[1] // self.n_hi
        return self.weights[w].at[:, pl.ds(pl.multiple_of(index * width, 128), width)]

    def a(self, w, s):
        there = lax.rem(self.hi + s, self.n_hi)
        return remote(
            self.columns(w, there), self.rows(w, self.hi, self.lo),
            self.asend.at[w, s - 1], self.arecv.at[w, s - 1], {"hi": there},
        )

    def b(self, w, k, bit):
        dst = self.rows(w, self.back(k), self.lo)
        src = self.columns(w, self.hi) if k == 0 else dst
        return remote(
            src, dst, self.bsend.at[w, k, bit - 1], self.brecv.at[w, k, bit - 1],
            {"lo": self.lo ^ bit},
        )

    def c(self, w, k, bit):
        half = self.block // 2
        part = self.rows(w, self.back(k), self.lo ^ bit, (bit - 1) * half, half)
        return remote(
            part, part, self.csend.at[w, k, bit - 1], self.crecv.at[w, k, bit - 1],
            {"lo": self.lo ^ (3 - bit)},
        )

    def exchange(self, w, first=1, last=None):
        for s in range(first, last or self.n_hi):
            self.a(w, s).start()

    def own_in(self, w):
        return pltpu.make_async_copy(self.columns(w, self.hi), self.holds[w], self.own.at[w])

    def own_out(self, w):
        return pltpu.make_async_copy(
            self.holds[w], self.rows(w, self.hi, self.lo), self.own.at[w]
        )

    def start_own(self):
        for w in range(len(self.weights)):
            self.own_in(w).start()

    def place_own(self):
        for w in range(len(self.weights)):
            self.own_in(w).wait()
            self.own_out(w).start()

    def relay(self, n):
        w, k = self.order[n]
        for bit in (1, 2):
            self.b(w, k, bit).wait_recv()
            self.c(w, k, bit).start()

    def advance(self, count=1):
        for _ in range(count):
            n = self.next
            if n < len(self.order):
                w, k = self.order[n]
                if k > 0:
                    self.a(w, k).wait_recv()
                for bit in (1, 2):
                    self.b(w, k, bit).start()
            if n >= 2:
                self.relay(n - 2)
            self.next = n + 1

    def arrived(self, w):
        for k in range(self.n_hi):
            for bit in (1, 2):
                self.c(w, k, bit).wait_recv()
        self.own_out(w).wait()

    def drain(self):
        for w in range(len(self.weights)):
            for s in range(1, self.n_hi):
                self.a(w, s).wait_send()
            for k in range(self.n_hi):
                for bit in (1, 2):
                    self.b(w, k, bit).wait_send()
                    self.c(w, k, bit).wait_send()


class Tokens:
    def __init__(self, moves, src, out, sems):
        self.m, self.src, self.out = moves, src, out
        self.usend, self.urecv, self.dsend, self.drecv, self.msend, self.mrecv = sems

    def place(self, origin):
        rows, width = self.src.shape
        return self.out.at[
            pl.ds(origin * rows, rows), pl.ds(pl.multiple_of(self.m.mp * width, 128), width)
        ]

    def up(self, d):
        place = self.place(self.m.hi - d)
        return remote(
            self.src if d == 0 else place, place, self.usend.at[d], self.urecv.at[d],
            {"hi": lax.rem(self.m.hi + 1, self.m.n_hi)},
        )

    def down(self, d):
        place = self.place(self.m.hi + d)
        return remote(
            self.src if d == 0 else place, place, self.dsend.at[d], self.drecv.at[d],
            {"hi": lax.rem(self.m.hi + self.m.n_hi - 1, self.m.n_hi)},
        )

    def landed(self, origin, sem):
        place = self.place(origin)
        return remote(
            place, place, sem, sem, {"hi": lax.rem(self.m.hi + 1, self.m.n_hi)}
        )

    def near(self, s):
        place = self.place(self.m.back(s))
        return remote(
            self.src if s == 0 else place, place, self.msend.at[s], self.mrecv.at[s],
            {"mp": 1 - self.m.mp},
        )

    def goes_up(self, d):
        return (self.m.hi >= d) & (self.m.hi + 1 < self.m.n_hi)

    def goes_down(self, d):
        return (self.m.hi + d < self.m.n_hi) & (self.m.hi > 0)

    def send(self):
        pl.when(self.goes_up(0))(lambda: self.up(0).start())
        pl.when(self.goes_down(0))(lambda: self.down(0).start())
        self.near(0).start()

    def relay(self, r):
        hi, n_hi = self.m.hi, self.m.n_hi

        def from_below():
            self.landed(hi - r, self.urecv.at[r - 1]).wait_recv()
            if r < n_hi - 1:
                pl.when(hi + 1 < n_hi)(lambda: self.up(r).start())
            self.near(r).start()

        def from_above():
            self.landed(hi + r, self.drecv.at[r - 1]).wait_recv()
            if r < n_hi - 1:
                pl.when(hi > 0)(lambda: self.down(r).start())
            self.near(n_hi - r).start()

        pl.when(hi >= r)(from_below)
        pl.when(hi + r < n_hi)(from_above)

    def finish(self):
        for s in range(self.m.n_hi):
            self.near(s).wait_recv()
        for s in range(self.m.n_hi):
            self.near(s).wait_send()
        for d in range(self.m.n_hi - 1):
            pl.when(self.goes_up(d))(lambda d=d: self.up(d).wait_send())
            pl.when(self.goes_down(d))(lambda d=d: self.down(d).wait_send())


def remote(src, dst, send, recv, where):
    return pltpu.make_async_remote_copy(
        src_ref=src, dst_ref=dst, send_sem=send, recv_sem=recv,
        device_id=where, device_id_type=MESH,
    )


def move_scratch(weights):
    n_hi, n_w = lax.axis_size("hi"), len(weights)
    dma = pltpu.SemaphoreType.DMA
    sems = [dma((n_w,)), dma((n_w, n_hi - 1)), dma((n_w, n_hi - 1))]
    sems += [dma((n_w, n_hi, 2)) for _ in range(4)]
    holds = [pltpu.VMEM((w.shape[0], w.shape[1] // n_hi), w.dtype) for w in weights]
    return sems + holds


def token_scratch():
    n_hi = lax.axis_size("hi")
    dma = pltpu.SemaphoreType.DMA
    return [dma((n_hi - 1,)) for _ in range(4)] + [dma((n_hi,)), dma((n_hi,))]


def gathered(w):
    n_hi, n_lo = lax.axis_size("hi"), lax.axis_size("lo")
    return jax.ShapeDtypeStruct((w.shape[0] * n_hi * n_lo, w.shape[1] // n_hi), w.dtype)


def forward_body(
    q_w, k_w, v_w, o_w, gate_w, up_w, down_w, grad, x, mask, hidden, gain_first, gain, bias,
    key_scale, value_scale,
    q_all, k_all, v_all, o_out, gate_out, up_out, down_out, grad_out, x_out, mask_out,
    second_out, q_out, key_pre, value_pre, key_rows, value_rows, probs_out, sum_out, inv_out,
    gate_proj, upward,
    *scratch,
):
    f32, bf16 = jnp.float32, jnp.bfloat16
    sems, holds = scratch[:7], scratch[7:14]
    g_tok, n_tok, x_tok = scratch[14:20], scratch[20:26], scratch[26:32]
    (q_full, k_full, v_full, normed, context, theirs, arrived, mine, both, landed, second_own,
     grad_hold, x_hold, mask_hold, mask_full, stat, stat_in, tiles, here, tile_sem, x_send,
     x_recv, r_send, r_recv, m_send, m_recv) = scratch[32:]
    o_full, second_full = q_full, normed
    order = [
        (0, 0), (1, 0), (2, 0), (4, 0), (0, 1), (0, 2), (0, 3), (3, 0), (1, 1), (1, 2), (1, 3),
        (5, 0), (2, 1), (2, 2), (2, 3), (3, 1), (3, 2), (3, 3), (4, 1), (4, 2), (4, 3), (6, 0),
        (5, 1), (5, 2), (5, 3), (6, 1), (6, 2), (6, 3),
    ]
    m = Moves(
        (q_w, k_w, v_w, o_w, gate_w, up_w, down_w),
        (q_all, k_all, v_all, o_out, gate_out, up_out, down_out), holds, sems, order,
    )
    rows, share = hidden.shape
    tokens, d_model = normed.shape
    seq_len = probs_out.shape[-1]
    partner = {"mp": 1 - m.mp}
    grad_half = grad.at[:, pl.ds(pl.multiple_of(m.mp * share, 128), share)]
    g = Tokens(m, grad_half, grad_out, g_tok)
    t = Tokens(m, second_own, second_out, n_tok)
    xt = Tokens(m, x, x_out, x_tok)
    x_in = pltpu.make_async_copy(x, x_hold, here.at[3])
    x_put = pltpu.make_async_copy(x_hold, xt.place(m.hi), here.at[3])
    mask_rows = mask.shape[0]
    mask_place = mask_out.at[pl.ds(m.hi * mask_rows, mask_rows)]
    mask_in = pltpu.make_async_copy(mask, mask_hold, here.at[4])
    mask_put = pltpu.make_async_copy(mask_hold, mask_place, here.at[4])
    grad_in = pltpu.make_async_copy(grad_half, grad_hold, here.at[0])
    grad_put = pltpu.make_async_copy(grad_hold, g.place(m.hi), here.at[0])

    def project(w_ref, store):
        tile = 256

        def step(i, carry):
            cols = pl.ds(pl.multiple_of(i * tile, tile), tile)
            store(cols, jnp.dot(normed[...], w_ref[:, cols], preferred_element_type=f32))
            return carry

        lax.fori_loop(0, w_ref.shape[1] // tile, step, 0)

    def store_query(cols, value):
        q_out[:, cols] = value.astype(bf16)

    def store_key(cols, value):
        key_pre[:, cols] = value
        key_rows[:, cols] = (value * key_scale[:, cols]).astype(bf16)

    def store_value(cols, value):
        value_pre[:, cols] = value
        value_rows[:, cols] = (value * value_scale[:, cols]).astype(bf16)

    def attend(seq):
        where = pl.ds(seq * seq_len, seq_len)
        hidden_keys = mask_full[pl.ds(seq * 8, 8), :][:1] < 0.0
        low = lax.broadcasted_iota(jnp.int32, (seq_len, 2 * HEAD_DIM), 1) < HEAD_DIM
        zero = jnp.zeros((seq_len, 2 * HEAD_DIM), bf16)
        for pair in range(probs_out.shape[1] // 2):
            cols = slice(pair * 2 * HEAD_DIM, (pair + 1) * 2 * HEAD_DIM)
            q2, k2, v2 = q_out[where, cols], key_rows[where, cols], value_rows[where, cols]
            outs = []
            for e in range(2):
                head = 2 * pair + e
                qe = jnp.where(low, q2, zero) if e == 0 else jnp.where(low, zero, q2)
                scores = contract_last(qe, k2) + bias[head]
                scores = jnp.where(hidden_keys, NEGATIVE, scores)
                exponent = jnp.exp(scores - jnp.max(scores, axis=-1, keepdims=True))
                probs = exponent / jnp.sum(exponent, axis=-1, keepdims=True)
                probs_out[seq, head] = probs
                outs.append(jnp.dot(probs.astype(bf16), v2, preferred_element_type=f32))
            context[where, cols] = jnp.where(low, outs[0], outs[1]).astype(bf16)

    def attend_some(first, count):
        def step(i, carry):
            attend(first + i)
            return carry

        lax.fori_loop(0, count, step, 0)

    def out_project(first_row, store):
        tile = 256

        def step(i, carry):
            w_rows = pl.ds(pl.multiple_of(first_row + i * tile, tile), tile)
            cols = pl.ds(pl.multiple_of(i * tile, tile), tile)
            store(cols, contract_last(context[...], o_full[w_rows, :]))
            return carry

        lax.fori_loop(0, share // tile, step, 0)

    def widen(w_ref, out_ref):
        tile = tiles.shape[2]
        count = w_ref.shape[1] // tile

        def bring(i):
            slot = lax.rem(i, 2)
            cols = pl.ds(pl.multiple_of(i * tile, tile), tile)
            return pltpu.make_async_copy(w_ref.at[:, cols], tiles.at[slot], tile_sem.at[slot])

        bring(0).start()

        def step(i, carry):
            pl.when(i + 1 < count)(lambda: bring(i + 1).start())
            bring(i).wait()
            cols = pl.ds(pl.multiple_of(i * tile, tile), tile)
            out_ref[:, cols] = jnp.dot(
                second_full[...], tiles[lax.rem(i, 2)], preferred_element_type=f32
            )
            return carry

        lax.fori_loop(0, count, step, 0)

    def store_theirs(cols, value):
        theirs[:, cols] = value.astype(bf16)

    def store_mine(cols, value):
        mine[:, cols] = value

    def by_rows(count, size, body):
        def step(i, carry):
            body(pl.ds(pl.multiple_of(i * size, size), size))
            return carry

        lax.fori_loop(0, count // size, step, 0)

    halves = remote(theirs, arrived, x_send.at[0], x_recv.at[0], partner)
    stats = remote(stat, stat_in, x_send.at[1], x_recv.at[1], partner)

    def mask_copy(s):
        there = lax.rem(m.hi + s, m.n_hi)
        return remote(mask, mask_place, m_send.at[s - 1], m_recv.at[s - 1], {"hi": there})

    def reduce_copy(s):
        there = lax.rem(m.hi + s, m.n_hi)
        return remote(
            both.at[pl.ds(there * rows, rows)], landed.at[s - 1],
            r_send.at[s - 1], r_recv.at[s - 1], {"hi": there},
        )

    def load(pairs):
        copies = [
            pltpu.make_async_copy(src, dst, here.at[5 + i]) for i, (src, dst) in enumerate(pairs)
        ]
        for copy in copies:
            copy.start()
        for copy in copies:
            copy.wait()

    def normalise_first(at):
        value = normed[at, :].astype(f32)
        square = jnp.sum(value * value, axis=-1, keepdims=True)
        inverse = lax.rsqrt(square / d_model + EPSILON)
        normed[at, :] = (value * inverse * gain_first[...]).astype(bf16)

    m.start_own()
    x_in.start()
    mask_in.start()
    grad_in.start()
    m.barrier()
    m.exchange(0)
    m.advance()
    m.exchange(1)
    m.advance(2)
    m.place_own()
    for copy, put in ((x_in, x_put), (mask_in, mask_put), (grad_in, grad_put)):
        copy.wait()
        put.start()
    xt.send()
    for s in range(1, m.n_hi):
        mask_copy(s).start()
    m.exchange(2)
    m.advance(4)
    xt.relay(1)
    m.exchange(3)
    m.advance(5)
    xt.relay(2)
    m.exchange(4)
    m.advance(3)
    xt.relay(3)
    m.exchange(5, 1, 3)
    xt.finish()
    x_put.wait()
    mask_put.wait()
    for s in range(1, m.n_hi):
        mask_copy(s).wait_recv()
    m.arrived(0)
    m.arrived(1)
    load([(x_out, normed), (q_all, q_full), (k_all, k_full), (mask_out, mask_full)])
    by_rows(tokens, 32, normalise_first)
    project(q_full, store_query)
    m.advance()
    project(k_full, store_key)
    m.advance()
    m.arrived(2)
    load([(v_all, v_full)])
    project(v_full, store_value)
    m.advance()
    attend_some(0, tokens // seq_len // 2)
    m.advance()
    attend_some(tokens // seq_len // 2, tokens // seq_len // 2)
    m.advance()
    m.arrived(3)
    load([(o_out, o_full)])
    out_project((1 - m.mp) * share, store_theirs)
    halves.start()
    out_project(m.mp * share, store_mine)
    m.advance()
    halves.wait_recv()

    def join(at):
        both[at, :] = (mine[at, :] + arrived[at, :].astype(f32)).astype(bf16)

    by_rows(tokens, 32, join)
    for s in range(1, m.n_hi):
        reduce_copy(s).start()
    m.exchange(5, 3)
    m.exchange(6)
    m.advance(3)
    for s in range(1, m.n_hi):
        reduce_copy(s).wait_recv()

    def add(at):
        own = pl.ds(pl.multiple_of(m.hi * rows, rows) + at.start, at.size)
        total = hidden[at, :].astype(f32) + mine[own, :] + arrived[own, :].astype(f32)
        for s in range(m.n_hi - 1):
            total = total + landed[s, at, :].astype(f32)
        sum_out[at, :] = total
        square = jnp.sum(total * total, axis=-1, keepdims=True)
        stat[at, :] = jnp.broadcast_to(square, (at.size, stat.shape[1]))

    by_rows(rows, 32, add)
    stats.start()
    stats.wait_recv()

    def normalise(at):
        inverse = lax.rsqrt((stat[at, :] + stat_in[at, :]) / d_model + EPSILON)
        inv_out[at, :] = inverse
        second_own[at, :] = (sum_out[at, :] * inverse[:, :1] * gain[...]).astype(bf16)

    by_rows(rows, 32, normalise)
    t.send()
    second_put = pltpu.make_async_copy(second_own, t.place(m.hi), here.at[2])
    second_put.start()
    g.send()
    m.advance(4)
    t.relay(1)
    g.relay(1)
    m.advance()
    t.relay(2)
    g.relay(2)
    m.advance()
    t.relay(3)
    t.finish()
    second_put.wait()
    m.arrived(4)
    m.arrived(5)
    load([(second_out, second_full)])
    widen(gate_out, gate_proj)
    g.relay(3)
    widen(up_out, upward)
    m.arrived(6)
    g.finish()
    m.drain()
    grad_put.wait()
    halves.wait_send()
    stats.wait_send()
    for s in range(1, m.n_hi):
        reduce_copy(s).wait_send()
        mask_copy(s).wait_send()


def forward_kernel(
    weights, grad, x, mask, gain_first, gain, bias, key_scale, value_scale, collective_id
):
    f32, bf16 = jnp.float32, jnp.bfloat16
    n_hi = lax.axis_size("hi")
    dma = pltpu.SemaphoreType.DMA
    any_spec = pl.BlockSpec(memory_space=pl.ANY)
    vmem = pl.BlockSpec(memory_space=pltpu.VMEM)
    rows, share = x.shape
    tokens, d_model = rows * n_hi, gain_first.shape[1]
    width, wide = key_scale.shape[1], weights[4].shape[1] // n_hi
    heads, seq_len = bias.shape[0], bias.shape[1]
    array = jax.ShapeDtypeStruct
    out_shape = [gathered(w) for w in weights] + [
        array((tokens, d_model), bf16), array((tokens, d_model), bf16),
        array((mask.shape[0] * n_hi, mask.shape[1]), f32), array((tokens, d_model), bf16),
        array((tokens, width), bf16), array((tokens, width), f32), array((tokens, width), f32),
        array((tokens, width), bf16), array((tokens, width), bf16),
        array((tokens // seq_len, heads, seq_len, seq_len), f32),
        array((rows, share), f32), array((rows, 128), f32),
        array((tokens, wide), f32), array((tokens, wide), f32),
    ]
    return pl.pallas_call(
        forward_body,
        out_shape=out_shape,
        in_specs=[any_spec] * 10 + [vmem] * 6,
        out_specs=[any_spec] * 11 + [vmem] * 10,
        scratch_shapes=move_scratch(weights) + token_scratch() * 3 + [
            pltpu.VMEM((d_model, width), bf16), pltpu.VMEM((d_model, width), bf16),
            pltpu.VMEM((d_model, width), bf16), pltpu.VMEM((tokens, d_model), bf16),
            pltpu.VMEM((tokens, width), bf16),
            pltpu.VMEM((tokens, share), bf16), pltpu.VMEM((tokens, share), bf16),
            pltpu.VMEM((tokens, share), f32), pltpu.VMEM((tokens, share), bf16),
            pltpu.VMEM((n_hi - 1, rows, share), bf16), pltpu.VMEM((rows, share), bf16),
            pltpu.VMEM((rows, share), bf16), pltpu.VMEM((rows, share), bf16),
            pltpu.VMEM(mask.shape, f32), pltpu.VMEM((mask.shape[0] * n_hi, seq_len), f32),
            pltpu.VMEM((rows, 128), f32), pltpu.VMEM((rows, 128), f32),
            pltpu.VMEM((2, d_model, 256), bf16),
            dma((9,)), dma((2,)), dma((2,)), dma((2,)), dma((n_hi - 1,)), dma((n_hi - 1,)),
            dma((n_hi - 1,)), dma((n_hi - 1,)),
        ],
        compiler_params=pltpu.CompilerParams(
            collective_id=collective_id, has_side_effects=True, vmem_limit_bytes=63 * 2**20
        ),
    )(*weights, grad, x, mask, x, gain_first, gain, bias, key_scale, value_scale)


def on_device_columns(
    hidden_in, lengths, norm_attn, q_weight, k_weight, v_weight, out_weight_t, norm_ffn,
    gate_weight, up_weight, down_weight_t, scale_key, scale_value, scale_ffn, out_grad,
    position_bias,
):
    f32, bf16 = jnp.float32, jnp.bfloat16
    n_hi, n_lo = lax.axis_size("hi"), lax.axis_size("lo")
    hi, lo, mp = lax.axis_index("hi"), lax.axis_index("lo"), lax.axis_index("mp")
    d_model = norm_attn.shape[0]
    tokens_local, share = hidden_in.shape
    seq_local = lengths.shape[0]
    seq_len = tokens_local // seq_local
    tokens = n_hi * tokens_local

    def swap_lo(x, bit):
        return lax.ppermute(x, "lo", [(i, i ^ bit) for i in range(n_lo)])

    def swap_hi(x, bit):
        return lax.ppermute(x, "hi", [(i, i ^ bit) for i in range(n_hi)])

    def swap_mp(x):
        return lax.ppermute(x, "mp", [(0, 1), (1, 0)])

    def own_columns(x):
        width = x.shape[-1] // n_hi
        return lax.dynamic_slice_in_dim(x, hi * width, width, x.ndim - 1)

    def times(x, w):
        return jnp.dot(x, w, preferred_element_type=f32)

    def join_features(own):
        other = swap_mp(own)
        lower = jnp.where(mp == 0, own, other)
        upper = jnp.where(mp == 0, other, own)
        return jnp.concatenate([lower, upper], axis=1)

    def gather_tokens(x):
        return join_features(lax.all_gather(x, "hi", axis=0, tiled=True))

    def back_sum(pairs):
        total = None
        for x, w in pairs:
            term = contract_last(x, w)
            total = term if total is None else total + term
        mine = lax.dynamic_slice_in_dim(total, mp * share, share, 1)
        theirs = lax.dynamic_slice_in_dim(total, (1 - mp) * share, share, 1)
        return (mine + swap_mp(theirs.astype(bf16)).astype(f32)).astype(bf16)

    def scatter(x):
        return lax.psum_scatter(x, "hi", scatter_dimension=0, tiled=True).astype(f32)

    def token_mean(x):
        part = jnp.sum(x, axis=-1, keepdims=True)
        return (part + swap_mp(part)) / d_model

    def own_half(gain):
        return lax.dynamic_slice_in_dim(gain, mp * share, share, 0)[None]

    gain_ffn = own_half(norm_ffn)
    gain_attn_half = own_half(norm_attn)
    gain_attn = norm_attn[None]
    key_scale, value_scale = own_columns(scale_key), own_columns(scale_value)
    ffn_scale = own_columns(scale_ffn)

    inputs_half = hidden_in
    grad_half = lax.dynamic_slice_in_dim(out_grad, mp * share, share, 1)
    keep = lax.broadcasted_iota(jnp.int32, (8 * seq_local, seq_len), 1) < lengths[0]
    mask = jnp.where(keep, 0.0, NEGATIVE)
    heads_local = q_weight.shape[1] // n_hi // HEAD_DIM
    bias = lax.dynamic_slice_in_dim(position_bias, hi * heads_local, heads_local, 0)
    (
        q_w, k_w, v_w, o_w, gate_w, up_w, down_w, grad_all, inputs_all, _, _, queries, key_pre,
        value_pre, key_rows, value_rows, attn_probs, first_sum, inv_second, gate_proj, upward,
    ) = forward_kernel(
        (q_weight, k_weight, v_weight, out_weight_t, gate_weight, up_weight, down_weight_t),
        out_grad, hidden_in, mask, gain_attn, gain_ffn, bias, key_scale[None],
        value_scale[None], 0,
    )
    inputs32 = lax.dynamic_slice_in_dim(
        inputs_all, hi * tokens_local, tokens_local, 0
    ).astype(f32)
    inv_mine = lax.rsqrt(
        jnp.sum(inputs32 * inputs32, axis=-1, keepdims=True) / d_model + EPSILON
    )
    inv_second = inv_second[:, :1]
    n_seq = n_hi * seq_local
    shaped = (n_seq, seq_len, heads_local, HEAD_DIM)
    q_heads = queries.reshape(shaped)
    k_heads = key_rows.reshape(shaped)
    v_heads = value_rows.reshape(shaped)
    probs_low = attn_probs.astype(bf16)
    d_hidden = times(grad_all, down_w)
    activated, gelu_back = jax.vjp(gelu_tanh, gate_proj)
    product = activated * upward
    hidden = (product * ffn_scale).astype(bf16)
    grad_ffn_part = jnp.sum(d_hidden * product, axis=0)
    d_product = d_hidden * ffn_scale
    d_gate = gelu_back(d_product * upward)[0].astype(bf16)
    d_up = (d_product * activated).astype(bf16)
    scaled = scatter(back_sum([(d_gate, gate_w), (d_up, up_w)])) * gain_ffn
    d_first = (
        grad_half.astype(f32)
        + inv_second * scaled
        - first_sum * inv_second * inv_second * inv_second * token_mean(scaled * first_sum)
    )
    d_first_all, ffn_part = lax.optimization_barrier(
        (gather_tokens(d_first.astype(bf16)), back_sum([(hidden, down_w)]))
    )
    ffn_out = scatter(ffn_part)
    d_context = times(d_first_all, o_w).astype(bf16)
    dc_heads = d_context.reshape(shaped)
    d_probs = jnp.einsum("bihe,bjhe->bhij", dc_heads, v_heads, preferred_element_type=f32)
    d_scores = (
        attn_probs * (d_probs - jnp.sum(attn_probs * d_probs, axis=-1, keepdims=True))
    ).astype(bf16)
    d_values = jnp.einsum(
        "bhij,bihe->bjhe", probs_low, dc_heads, preferred_element_type=f32
    ).reshape(tokens, -1)
    d_keys = jnp.einsum(
        "bhij,bihe->bjhe", d_scores, q_heads, preferred_element_type=f32
    ).reshape(tokens, -1)
    d_queries = (
        jnp.einsum("bhij,bjhe->bihe", d_scores, k_heads, preferred_element_type=f32)
        .reshape(tokens, -1)
        .astype(bf16)
    )
    grad_key_part = jnp.sum(d_keys * key_pre, axis=0)
    grad_value_part = jnp.sum(d_values * value_pre, axis=0)
    d_key_pre = (d_keys * key_scale).astype(bf16)
    d_value_pre = (d_values * value_scale).astype(bf16)
    ffn_out, d_queries = lax.optimization_barrier((ffn_out, d_queries))
    scaled_in = (
        scatter(back_sum([(d_queries, q_w), (d_key_pre, k_w), (d_value_pre, v_w)]))
        * gain_attn_half
    )
    mine32 = inputs_half.astype(f32)
    mean_dot = token_mean(scaled_in * mine32)
    input_grad = (
        d_first
        + inv_mine * scaled_in
        - mine32 * inv_mine * inv_mine * inv_mine * mean_dot
    ).astype(bf16)
    block_out = (first_sum + ffn_out).astype(bf16)

    def totals(part):
        part = part[None]
        for bit in (1, 2):
            part = part + swap_lo(part, bit)
        for bit in (1, 2):
            other = swap_hi(part, bit)
            upper = (hi & bit) > 0
            part = jnp.concatenate(
                [jnp.where(upper, other, part), jnp.where(upper, part, other)], axis=0
            )
        return part

    attn_totals = totals(jnp.concatenate([grad_key_part, grad_value_part]))
    width = grad_key_part.shape[0]
    return (
        block_out,
        input_grad,
        attn_totals[:, :width].reshape(-1),
        attn_totals[:, width:].reshape(-1),
        totals(grad_ffn_part).reshape(-1),
    )


def solution(mesh):
    n_dp, n_mp = mesh.shape["dp"], mesh.shape["mp"]
    n_hi = 1
    while n_dp % (n_hi * 2) == 0 and n_hi * n_hi < n_dp:
        n_hi *= 2
    grid = jax.sharding.Mesh(
        mesh.devices.reshape(n_hi, n_dp // n_hi, n_mp), ("hi", "lo", "mp")
    )
    dp = ("hi", "lo")
    weight = P(dp, "mp")
    columns = (n_hi, n_dp // n_hi, n_mp) == (4, 4, 2)
    return jax.shard_map(
        on_device_columns if columns else on_device_general,
        mesh=grid,
        in_specs=(
            P(dp, "mp"), P(dp), P(), weight, weight, weight, weight, P(), weight, weight, weight,
            P("mp"), P("mp"), P("mp"), P(dp, None), P("mp", None, None),
        ),
        out_specs=(P(dp, "mp"), P(dp, "mp"), P("mp"), P("mp"), P("mp")),
        check_vma=False,
    )
```

```python
import functools

import jax
import jax.numpy as jnp
from jax import lax
from jax.experimental import pallas as pl
from jax.experimental.pallas import tpu as pltpu
from jax.sharding import PartitionSpec as P

HEAD_DIM = 64
MESH = pl.DeviceIdType.MESH


EPSILON = 1e-06
NEGATIVE = -1e30


def inverse_rms(values):
    return lax.rsqrt(jnp.mean(values * values, axis=-1, keepdims=True) + EPSILON)


def gelu_tanh(values):
    return jax.nn.gelu(values, approximate=True)


def contract_last(left_side, right_side):
    return lax.dot_general(
        left_side, right_side, (((1,), (1,)), ((), ())), preferred_element_type=jnp.float32
    )


def norm_back(grad_in, values, inverse, gain_vec):
    scaled = grad_in * gain_vec
    correction = (
        values * inverse * inverse * inverse * jnp.mean(scaled * values, axis=-1, keepdims=True)
    )
    return inverse * scaled - correction


WEIGHT_AXIS = "lo"


def on_device_general(
    hidden_in, lengths, norm_attn, q_weight, k_weight, v_weight, out_weight_t, norm_ffn,
    gate_weight, up_weight, down_weight_t, scale_key, scale_value, scale_ffn, out_grad,
    position_bias,
):
    f32, bf16 = jnp.float32, jnp.bfloat16
    wa = WEIGHT_AXIS
    ta = "lo" if wa == "hi" else "hi"
    n_hi, n_lo = lax.axis_size("hi"), lax.axis_size("lo")
    n_t = lax.axis_size(ta)

    def swap(x, bit):
        return lax.ppermute(x, "lo", [(i, i ^ bit) for i in range(n_lo)])

    def own_first(parts):
        if n_lo != 4:
            return parts
        index = lax.axis_index("lo")
        rows, width = parts.shape[0], parts.shape[-1]
        parts = parts.reshape(rows, n_hi, 2, 2, width)
        parts = jnp.where((index & 2) > 0, parts[:, :, ::-1], parts)
        parts = jnp.where((index & 1) > 0, parts[:, :, :, ::-1], parts)
        return parts.reshape(rows, n_hi, n_lo, width)

    def sum_mp(x):
        x = x.astype(bf16)
        if lax.axis_size("mp") != 2:
            return lax.psum(x, "mp").astype(f32)
        return x.astype(f32) + lax.ppermute(x, "mp", [(0, 1), (1, 0)]).astype(f32)

    def split_features(x):
        rows = x.shape[0]
        parts = own_first(x.reshape(rows, n_hi, n_lo, -1))
        order = (1, 0, 2, 3) if ta == "hi" else (2, 0, 1, 3)
        return parts.transpose(order).reshape(n_t, rows, -1)

    def join_features(x):
        rows = x.shape[1]
        if ta == "hi":
            parts = x.transpose(1, 0, 2).reshape(rows, n_hi, n_lo, -1)
            return own_first(parts).reshape(rows, -1)
        return x.reshape(n_lo, rows, n_hi, -1).transpose(1, 2, 0, 3).reshape(rows, -1)

    def exchange(x):
        return lax.all_to_all(x, ta, split_axis=0, concat_axis=0, tiled=True)

    def gather_rows(w):
        if n_lo != 4:
            return lax.all_gather(w, wa, axis=0, tiled=True)
        half = w.shape[0] // 2
        first, second = swap(w, 1), swap(w, 2)
        third = swap(second[:half], 1), swap(first[half:], 2)
        return jnp.concatenate([w, first, second, *third], axis=0)

    def gather_tokens(x):
        return lax.all_gather(x, ta, axis=0, tiled=True)

    def scatter_tokens(x):
        return lax.psum_scatter(x.astype(bf16), ta, scatter_dimension=0, tiled=True)

    def dot(a, b):
        return jnp.dot(a, b, preferred_element_type=f32)

    d_model = norm_attn.shape[0]
    tokens_local = hidden_in.shape[0]
    seq_local = lengths.shape[0]
    seq_len = tokens_local // seq_local
    t_index = lax.axis_index(ta)
    gain_attn = split_features(norm_attn[None])
    gain_attn = lax.dynamic_index_in_dim(gain_attn, t_index, 0, False)
    gain_ffn = split_features(norm_ffn[None])
    gain_ffn = lax.dynamic_index_in_dim(gain_ffn, t_index, 0, False)

    full_inputs = lax.all_gather(hidden_in, "mp", axis=1, tiled=True)
    both = jnp.concatenate([split_features(full_inputs), split_features(out_grad)], axis=2)
    both = exchange(both).reshape(n_t * tokens_local, -1)
    inputs_blk, out_grad_blk = jnp.split(both, 2, axis=1)
    inputs32 = inputs_blk.astype(f32)

    def token_mean(x):
        return lax.psum(jnp.sum(x, axis=-1, keepdims=True), ta) / d_model

    q_full, k_full, v_full = gather_rows(q_weight), gather_rows(k_weight), gather_rows(v_weight)
    o_full = gather_rows(out_weight_t)
    gate_full, up_full = gather_rows(gate_weight), gather_rows(up_weight)
    down_full = gather_rows(down_weight_t)

    inv_first = lax.rsqrt(token_mean(inputs32 * inputs32) + EPSILON)
    normed_first = (inputs32 * inv_first * gain_attn).astype(bf16)
    queries = scatter_tokens(dot(normed_first, q_full))
    key_pre = scatter_tokens(dot(normed_first, k_full)).astype(f32)
    value_pre = scatter_tokens(dot(normed_first, v_full)).astype(f32)
    heads_local = queries.shape[1] // HEAD_DIM
    shaped = (seq_local, seq_len, heads_local, HEAD_DIM)
    key_rows = (key_pre * scale_key).astype(bf16)
    value_rows = (value_pre * scale_value).astype(bf16)
    q_heads = queries.reshape(shaped)
    k_heads = key_rows.reshape(shaped)
    v_heads = value_rows.reshape(shaped)
    scores = (
        jnp.einsum("bihe,bjhe->bhij", q_heads, k_heads, preferred_element_type=f32)
        + position_bias[None]
    )
    positions = lax.broadcasted_iota(jnp.int32, (seq_local, seq_len), 1)
    valid_keys = positions < lengths[:, None]
    scores = jnp.where(valid_keys[:, None, None, :], scores, NEGATIVE)
    largest = jnp.max(scores, axis=-1, keepdims=True)
    exponent = jnp.exp(scores - largest)
    attn_probs = exponent / jnp.sum(exponent, axis=-1, keepdims=True)
    probs_low = attn_probs.astype(bf16)
    context = (
        jnp.einsum("bhij,bjhe->bihe", probs_low, v_heads, preferred_element_type=f32)
        .reshape(tokens_local, -1)
        .astype(bf16)
    )
    first_sum = inputs32 + sum_mp(contract_last(gather_tokens(context), o_full))
    inv_second = lax.rsqrt(token_mean(first_sum * first_sum) + EPSILON)
    normed_second = (first_sum * inv_second * gain_ffn).astype(bf16)
    gate_proj = scatter_tokens(dot(normed_second, gate_full)).astype(f32)
    upward = scatter_tokens(dot(normed_second, up_full)).astype(f32)
    d_hidden = scatter_tokens(dot(out_grad_blk, down_full)).astype(f32)
    activated, gelu_back = jax.vjp(gelu_tanh, gate_proj)
    product = activated * upward
    hidden = (product * scale_ffn).astype(bf16)
    grad_ffn_part = jnp.sum(d_hidden * product, axis=0)
    d_product = d_hidden * scale_ffn
    d_gate = gelu_back(d_product * upward)[0].astype(bf16)
    d_up = (d_product * activated).astype(bf16)
    d_second = sum_mp(
        contract_last(gather_tokens(d_gate), gate_full)
        + contract_last(gather_tokens(d_up), up_full)
    )
    scaled = d_second * gain_ffn
    d_first = (
        out_grad_blk.astype(f32)
        + inv_second * scaled
        - first_sum * inv_second * inv_second * inv_second * token_mean(scaled * first_sum)
    )
    d_context = scatter_tokens(dot(d_first.astype(bf16), o_full))
    dc_heads = d_context.reshape(shaped)
    d_probs = jnp.einsum("bihe,bjhe->bhij", dc_heads, v_heads, preferred_element_type=f32)
    d_scores = (
        attn_probs * (d_probs - jnp.sum(attn_probs * d_probs, axis=-1, keepdims=True))
    ).astype(bf16)
    d_values = jnp.einsum(
        "bhij,bihe->bjhe", probs_low, dc_heads, preferred_element_type=f32
    ).reshape(tokens_local, -1)
    d_keys = jnp.einsum(
        "bhij,bihe->bjhe", d_scores, q_heads, preferred_element_type=f32
    ).reshape(tokens_local, -1)
    d_queries = (
        jnp.einsum("bhij,bjhe->bihe", d_scores, k_heads, preferred_element_type=f32)
        .reshape(tokens_local, -1)
        .astype(bf16)
    )
    grad_key_part = jnp.sum(d_keys * key_pre, axis=0)
    grad_value_part = jnp.sum(d_values * value_pre, axis=0)
    d_key_pre = (d_keys * scale_key).astype(bf16)
    d_value_pre = (d_values * scale_value).astype(bf16)
    d_normed = sum_mp(
        contract_last(gather_tokens(d_queries), q_full)
        + contract_last(gather_tokens(d_key_pre), k_full)
        + contract_last(gather_tokens(d_value_pre), v_full)
    )
    scaled_in = d_normed * gain_attn
    mean_dot = token_mean(scaled_in * inputs32)
    input_grad = (
        d_first
        + inv_first * scaled_in
        - inputs32 * inv_first * inv_first * inv_first * mean_dot
    ).astype(bf16)

    ffn_out = sum_mp(contract_last(gather_tokens(hidden), down_full))
    block_out = (first_sum + ffn_out).astype(bf16)

    share_width = hidden_in.shape[1]
    offset = lax.axis_index("mp") * share_width

    def own_share(x):
        joined = join_features(exchange(x.reshape(n_t, tokens_local, -1)))
        return lax.dynamic_slice_in_dim(joined, offset, share_width, 1)

    parts = jnp.concatenate([grad_key_part, grad_value_part, grad_ffn_part])
    totals = lax.psum(lax.psum(parts, "lo"), "hi")
    width = grad_key_part.shape[0]
    return (
        own_share(block_out),
        own_share(input_grad),
        totals[:width],
        totals[width : 2 * width],
        totals[2 * width :],
    )


class Moves:
    def __init__(self, weights, outs, holds, sems, order):
        self.weights, self.outs, self.holds, self.order = weights, outs, holds, order
        self.own, self.asend, self.arecv, self.bsend, self.brecv, self.csend, self.crecv = sems
        self.n_hi, self.n_lo = lax.axis_size("hi"), lax.axis_size("lo")
        self.hi, self.lo = lax.axis_index("hi"), lax.axis_index("lo")
        self.mp = lax.axis_index("mp")
        self.block = weights[0].shape[0]
        self.next = 0

    def barrier(self):
        barrier = pltpu.get_barrier_semaphore()
        places = [{"hi": lax.rem(self.hi + s, self.n_hi)} for s in range(1, self.n_hi)]
        places += [{"lo": self.lo ^ 1}, {"lo": self.lo ^ 2}, {"mp": 1 - self.mp}]
        for place in places:
            pl.semaphore_signal(barrier, inc=1, device_id=place, device_id_type=MESH)
        pl.semaphore_wait(barrier, len(places))

    def back(self, k):
        return lax.rem(self.hi + self.n_hi - k, self.n_hi)

    def rows(self, w, hi, lo, start=0, size=None):
        first = (hi * self.n_lo + lo) * self.block + start
        return self.outs[w].at[pl.ds(first, size or self.block)]

    def columns(self, w, index):
        width = self.weights[w].shape[1] // self.n_hi
        return self.weights[w].at[:, pl.ds(pl.multiple_of(index * width, 128), width)]

    def a(self, w, s):
        there = lax.rem(self.hi + s, self.n_hi)
        return remote(
            self.columns(w, there), self.rows(w, self.hi, self.lo),
            self.asend.at[w, s - 1], self.arecv.at[w, s - 1], {"hi": there},
        )

    def b(self, w, k, bit):
        dst = self.rows(w, self.back(k), self.lo)
        src = self.columns(w, self.hi) if k == 0 else dst
        return remote(
            src, dst, self.bsend.at[w, k, bit - 1], self.brecv.at[w, k, bit - 1],
            {"lo": self.lo ^ bit},
        )

    def c(self, w, k, bit):
        half = self.block // 2
        part = self.rows(w, self.back(k), self.lo ^ bit, (bit - 1) * half, half)
        return remote(
            part, part, self.csend.at[w, k, bit - 1], self.crecv.at[w, k, bit - 1],
            {"lo": self.lo ^ (3 - bit)},
        )

    def exchange(self, w, first=1, last=None):
        for s in range(first, last or self.n_hi):
            self.a(w, s).start()

    def own_in(self, w):
        return pltpu.make_async_copy(self.columns(w, self.hi), self.holds[w], self.own.at[w])

    def own_out(self, w):
        return pltpu.make_async_copy(
            self.holds[w], self.rows(w, self.hi, self.lo), self.own.at[w]
        )

    def start_own(self):
        for w in range(len(self.weights)):
            self.own_in(w).start()

    def place_own(self):
        for w in range(len(self.weights)):
            self.own_in(w).wait()
            self.own_out(w).start()

    def relay(self, n):
        w, k = self.order[n]
        for bit in (1, 2):
            self.b(w, k, bit).wait_recv()
            self.c(w, k, bit).start()

    def advance(self, count=1):
        for _ in range(count):
            n = self.next
            if n < len(self.order):
                w, k = self.order[n]
                if k > 0:
                    self.a(w, k).wait_recv()
                for bit in (1, 2):
                    self.b(w, k, bit).start()
            if n >= 2:
                self.relay(n - 2)
            self.next = n + 1

    def arrived(self, w):
        for k in range(self.n_hi):
            for bit in (1, 2):
                self.c(w, k, bit).wait_recv()
        self.own_out(w).wait()

    def drain(self):
        for w in range(len(self.weights)):
            for s in range(1, self.n_hi):
                self.a(w, s).wait_send()
            for k in range(self.n_hi):
                for bit in (1, 2):
                    self.b(w, k, bit).wait_send()
                    self.c(w, k, bit).wait_send()


class Tokens:
    def __init__(self, moves, src, out, sems):
        self.m, self.src, self.out = moves, src, out
        self.usend, self.urecv, self.dsend, self.drecv, self.msend, self.mrecv = sems

    def place(self, origin):
        rows, width = self.src.shape
        return self.out.at[
            pl.ds(origin * rows, rows), pl.ds(pl.multiple_of(self.m.mp * width, 128), width)
        ]

    def up(self, d):
        place = self.place(self.m.hi - d)
        return remote(
            self.src if d == 0 else place, place, self.usend.at[d], self.urecv.at[d],
            {"hi": lax.rem(self.m.hi + 1, self.m.n_hi)},
        )

    def down(self, d):
        place = self.place(self.m.hi + d)
        return remote(
            self.src if d == 0 else place, place, self.dsend.at[d], self.drecv.at[d],
            {"hi": lax.rem(self.m.hi + self.m.n_hi - 1, self.m.n_hi)},
        )

    def landed(self, origin, sem):
        place = self.place(origin)
        return remote(
            place, place, sem, sem, {"hi": lax.rem(self.m.hi + 1, self.m.n_hi)}
        )

    def near(self, s):
        place = self.place(self.m.back(s))
        return remote(
            self.src if s == 0 else place, place, self.msend.at[s], self.mrecv.at[s],
            {"mp": 1 - self.m.mp},
        )

    def goes_up(self, d):
        return (self.m.hi >= d) & (self.m.hi + 1 < self.m.n_hi)

    def goes_down(self, d):
        return (self.m.hi + d < self.m.n_hi) & (self.m.hi > 0)

    def send(self):
        pl.when(self.goes_up(0))(lambda: self.up(0).start())
        pl.when(self.goes_down(0))(lambda: self.down(0).start())
        self.near(0).start()

    def relay(self, r):
        hi, n_hi = self.m.hi, self.m.n_hi

        def from_below():
            self.landed(hi - r, self.urecv.at[r - 1]).wait_recv()
            if r < n_hi - 1:
                pl.when(hi + 1 < n_hi)(lambda: self.up(r).start())
            self.near(r).start()

        def from_above():
            self.landed(hi + r, self.drecv.at[r - 1]).wait_recv()
            if r < n_hi - 1:
                pl.when(hi > 0)(lambda: self.down(r).start())
            self.near(n_hi - r).start()

        pl.when(hi >= r)(from_below)
        pl.when(hi + r < n_hi)(from_above)

    def finish(self):
        for s in range(self.m.n_hi):
            self.near(s).wait_recv()
        for s in range(self.m.n_hi):
            self.near(s).wait_send()
        for d in range(self.m.n_hi - 1):
            pl.when(self.goes_up(d))(lambda d=d: self.up(d).wait_send())
            pl.when(self.goes_down(d))(lambda d=d: self.down(d).wait_send())


def remote(src, dst, send, recv, where):
    return pltpu.make_async_remote_copy(
        src_ref=src, dst_ref=dst, send_sem=send, recv_sem=recv,
        device_id=where, device_id_type=MESH,
    )


def move_scratch(weights):
    n_hi, n_w = lax.axis_size("hi"), len(weights)
    dma = pltpu.SemaphoreType.DMA
    sems = [dma((n_w,)), dma((n_w, n_hi - 1)), dma((n_w, n_hi - 1))]
    sems += [dma((n_w, n_hi, 2)) for _ in range(4)]
    holds = [pltpu.VMEM((w.shape[0], w.shape[1] // n_hi), w.dtype) for w in weights]
    return sems + holds


def token_scratch():
    n_hi = lax.axis_size("hi")
    dma = pltpu.SemaphoreType.DMA
    return [dma((n_hi - 1,)) for _ in range(4)] + [dma((n_hi,)), dma((n_hi,))]


def gathered(w):
    n_hi, n_lo = lax.axis_size("hi"), lax.axis_size("lo")
    return jax.ShapeDtypeStruct((w.shape[0] * n_hi * n_lo, w.shape[1] // n_hi), w.dtype)


def forward_body(
    q_w, k_w, v_w, o_w, gate_w, up_w, down_w, grad, x, mask, hidden, gain_first, gain, bias,
    key_scale, value_scale,
    q_all, k_all, v_all, o_out, gate_out, up_out, down_out, grad_out, x_out, mask_out,
    second_out, q_out, key_pre, value_pre, key_rows, value_rows, probs_out, sum_out, inv_out,
    gate_proj, upward,
    *scratch,
):
    f32, bf16 = jnp.float32, jnp.bfloat16
    sems, holds = scratch[:7], scratch[7:14]
    g_tok, n_tok, x_tok = scratch[14:20], scratch[20:26], scratch[26:32]
    (q_full, k_full, v_full, normed, context, theirs, arrived, mine, both, landed, second_own,
     grad_hold, x_hold, mask_hold, mask_full, stat, stat_in, tiles, here, tile_sem, x_send,
     x_recv, r_send, r_recv, m_send, m_recv) = scratch[32:]
    o_full, second_full = q_full, normed
    order = [
        (0, 0), (1, 0), (2, 0), (4, 0), (0, 1), (0, 2), (0, 3), (3, 0), (1, 1), (1, 2), (1, 3),
        (5, 0), (2, 1), (2, 2), (2, 3), (3, 1), (3, 2), (3, 3), (4, 1), (4, 2), (4, 3), (6, 0),
        (5, 1), (5, 2), (5, 3), (6, 1), (6, 2), (6, 3),
    ]
    m = Moves(
        (q_w, k_w, v_w, o_w, gate_w, up_w, down_w),
        (q_all, k_all, v_all, o_out, gate_out, up_out, down_out), holds, sems, order,
    )
    rows, share = hidden.shape
    tokens, d_model = normed.shape
    seq_len = probs_out.shape[-1]
    partner = {"mp": 1 - m.mp}
    grad_half = grad.at[:, pl.ds(pl.multiple_of(m.mp * share, 128), share)]
    g = Tokens(m, grad_half, grad_out, g_tok)
    t = Tokens(m, second_own, second_out, n_tok)
    xt = Tokens(m, x, x_out, x_tok)
    x_in = pltpu.make_async_copy(x, x_hold, here.at[3])
    x_put = pltpu.make_async_copy(x_hold, xt.place(m.hi), here.at[3])
    mask_rows = mask.shape[0]
    mask_place = mask_out.at[pl.ds(m.hi * mask_rows, mask_rows)]
    mask_in = pltpu.make_async_copy(mask, mask_hold, here.at[4])
    mask_put = pltpu.make_async_copy(mask_hold, mask_place, here.at[4])
    grad_in = pltpu.make_async_copy(grad_half, grad_hold, here.at[0])
    grad_put = pltpu.make_async_copy(grad_hold, g.place(m.hi), here.at[0])

    def project(w_ref, store):
        tile = 256

        def step(i, carry):
            cols = pl.ds(pl.multiple_of(i * tile, tile), tile)
            store(cols, jnp.dot(normed[...], w_ref[:, cols], preferred_element_type=f32))
            return carry

        lax.fori_loop(0, w_ref.shape[1] // tile, step, 0)

    def store_query(cols, value):
        q_out[:, cols] = value.astype(bf16)

    def store_key(cols, value):
        key_pre[:, cols] = value
        key_rows[:, cols] = (value * key_scale[:, cols]).astype(bf16)

    def store_value(cols, value):
        value_pre[:, cols] = value
        value_rows[:, cols] = (value * value_scale[:, cols]).astype(bf16)

    def attend(seq):
        where = pl.ds(seq * seq_len, seq_len)
        hidden_keys = mask_full[pl.ds(seq * 8, 8), :][:1] < 0.0
        low = lax.broadcasted_iota(jnp.int32, (seq_len, 2 * HEAD_DIM), 1) < HEAD_DIM
        zero = jnp.zeros((seq_len, 2 * HEAD_DIM), bf16)
        for pair in range(probs_out.shape[1] // 2):
            cols = slice(pair * 2 * HEAD_DIM, (pair + 1) * 2 * HEAD_DIM)
            q2, k2, v2 = q_out[where, cols], key_rows[where, cols], value_rows[where, cols]
            outs = []
            for e in range(2):
                head = 2 * pair + e
                qe = jnp.where(low, q2, zero) if e == 0 else jnp.where(low, zero, q2)
                scores = contract_last(qe, k2) + bias[head]
                scores = jnp.where(hidden_keys, NEGATIVE, scores)
                exponent = jnp.exp(scores - jnp.max(scores, axis=-1, keepdims=True))
                probs = exponent / jnp.sum(exponent, axis=-1, keepdims=True)
                probs_out[seq, head] = probs
                outs.append(jnp.dot(probs.astype(bf16), v2, preferred_element_type=f32))
            context[where, cols] = jnp.where(low, outs[0], outs[1]).astype(bf16)

    def attend_some(first, count):
        def step(i, carry):
            attend(first + i)
            return carry

        lax.fori_loop(0, count, step, 0)

    def out_project(first_row, store):
        tile = 256

        def step(i, carry):
            w_rows = pl.ds(pl.multiple_of(first_row + i * tile, tile), tile)
            cols = pl.ds(pl.multiple_of(i * tile, tile), tile)
            store(cols, contract_last(context[...], o_full[w_rows, :]))
            return carry

        lax.fori_loop(0, share // tile, step, 0)

    def widen(w_ref, out_ref):
        tile = tiles.shape[2]
        count = w_ref.shape[1] // tile

        def bring(i):
            slot = lax.rem(i, 2)
            cols = pl.ds(pl.multiple_of(i * tile, tile), tile)
            return pltpu.make_async_copy(w_ref.at[:, cols], tiles.at[slot], tile_sem.at[slot])

        bring(0).start()

        def step(i, carry):
            pl.when(i + 1 < count)(lambda: bring(i + 1).start())
            bring(i).wait()
            cols = pl.ds(pl.multiple_of(i * tile, tile), tile)
            out_ref[:, cols] = jnp.dot(
                second_full[...], tiles[lax.rem(i, 2)], preferred_element_type=f32
            )
            return carry

        lax.fori_loop(0, count, step, 0)

    def store_theirs(cols, value):
        theirs[:, cols] = value.astype(bf16)

    def store_mine(cols, value):
        mine[:, cols] = value

    def by_rows(count, size, body):
        def step(i, carry):
            body(pl.ds(pl.multiple_of(i * size, size), size))
            return carry

        lax.fori_loop(0, count // size, step, 0)

    halves = remote(theirs, arrived, x_send.at[0], x_recv.at[0], partner)
    stats = remote(stat, stat_in, x_send.at[1], x_recv.at[1], partner)

    def mask_copy(s):
        there = lax.rem(m.hi + s, m.n_hi)
        return remote(mask, mask_place, m_send.at[s - 1], m_recv.at[s - 1], {"hi": there})

    def reduce_copy(s):
        there = lax.rem(m.hi + s, m.n_hi)
        return remote(
            both.at[pl.ds(there * rows, rows)], landed.at[s - 1],
            r_send.at[s - 1], r_recv.at[s - 1], {"hi": there},
        )

    def load(pairs):
        copies = [
            pltpu.make_async_copy(src, dst, here.at[5 + i]) for i, (src, dst) in enumerate(pairs)
        ]
        for copy in copies:
            copy.start()
        for copy in copies:
            copy.wait()

    def normalise_first(at):
        value = normed[at, :].astype(f32)
        square = jnp.sum(value * value, axis=-1, keepdims=True)
        inverse = lax.rsqrt(square / d_model + EPSILON)
        normed[at, :] = (value * inverse * gain_first[...]).astype(bf16)

    m.start_own()
    x_in.start()
    mask_in.start()
    grad_in.start()
    m.barrier()
    m.exchange(0)
    m.advance()
    m.exchange(1)
    m.advance(2)
    m.place_own()
    for copy, put in ((x_in, x_put), (mask_in, mask_put), (grad_in, grad_put)):
        copy.wait()
        put.start()
    xt.send()
    for s in range(1, m.n_hi):
        mask_copy(s).start()
    m.exchange(2)
    m.advance(4)
    xt.relay(1)
    m.exchange(3)
    m.advance(5)
    xt.relay(2)
    m.exchange(4)
    m.advance(3)
    xt.relay(3)
    m.exchange(5, 1, 3)
    xt.finish()
    x_put.wait()
    mask_put.wait()
    for s in range(1, m.n_hi):
        mask_copy(s).wait_recv()
    m.arrived(0)
    m.arrived(1)
    load([(x_out, normed), (q_all, q_full), (k_all, k_full), (mask_out, mask_full)])
    by_rows(tokens, 32, normalise_first)
    project(q_full, store_query)
    m.advance()
    project(k_full, store_key)
    m.advance()
    m.arrived(2)
    load([(v_all, v_full)])
    project(v_full, store_value)
    m.advance()
    attend_some(0, tokens // seq_len // 2)
    m.advance()
    attend_some(tokens // seq_len // 2, tokens // seq_len // 2)
    m.advance()
    m.arrived(3)
    load([(o_out, o_full)])
    out_project((1 - m.mp) * share, store_theirs)
    halves.start()
    out_project(m.mp * share, store_mine)
    m.advance()
    halves.wait_recv()

    def join(at):
        both[at, :] = (mine[at, :] + arrived[at, :].astype(f32)).astype(bf16)

    by_rows(tokens, 32, join)
    for s in range(1, m.n_hi):
        reduce_copy(s).start()
    m.exchange(5, 3)
    m.exchange(6)
    m.advance(3)
    for s in range(1, m.n_hi):
        reduce_copy(s).wait_recv()

    def add(at):
        own = pl.ds(pl.multiple_of(m.hi * rows, rows) + at.start, at.size)
        total = hidden[at, :].astype(f32) + mine[own, :] + arrived[own, :].astype(f32)
        for s in range(m.n_hi - 1):
            total = total + landed[s, at, :].astype(f32)
        sum_out[at, :] = total
        square = jnp.sum(total * total, axis=-1, keepdims=True)
        stat[at, :] = jnp.broadcast_to(square, (at.size, stat.shape[1]))

    by_rows(rows, 32, add)
    stats.start()
    stats.wait_recv()

    def normalise(at):
        inverse = lax.rsqrt((stat[at, :] + stat_in[at, :]) / d_model + EPSILON)
        inv_out[at, :] = inverse
        second_own[at, :] = (sum_out[at, :] * inverse[:, :1] * gain[...]).astype(bf16)

    by_rows(rows, 32, normalise)
    t.send()
    second_put = pltpu.make_async_copy(second_own, t.place(m.hi), here.at[2])
    second_put.start()
    g.send()
    m.advance(4)
    t.relay(1)
    g.relay(1)
    m.advance()
    t.relay(2)
    g.relay(2)
    m.advance()
    t.relay(3)
    t.finish()
    second_put.wait()
    m.arrived(4)
    m.arrived(5)
    load([(second_out, second_full)])
    widen(gate_out, gate_proj)
    g.relay(3)
    widen(up_out, upward)
    m.arrived(6)
    g.finish()
    m.drain()
    grad_put.wait()
    halves.wait_send()
    stats.wait_send()
    for s in range(1, m.n_hi):
        reduce_copy(s).wait_send()
        mask_copy(s).wait_send()


def forward_kernel(
    weights, grad, x, mask, gain_first, gain, bias, key_scale, value_scale, collective_id
):
    f32, bf16 = jnp.float32, jnp.bfloat16
    n_hi = lax.axis_size("hi")
    dma = pltpu.SemaphoreType.DMA
    any_spec = pl.BlockSpec(memory_space=pl.ANY)
    vmem = pl.BlockSpec(memory_space=pltpu.VMEM)
    rows, share = x.shape
    tokens, d_model = rows * n_hi, gain_first.shape[1]
    width, wide = key_scale.shape[1], weights[4].shape[1] // n_hi
    heads, seq_len = bias.shape[0], bias.shape[1]
    array = jax.ShapeDtypeStruct
    out_shape = [gathered(w) for w in weights] + [
        array((tokens, d_model), bf16), array((tokens, d_model), bf16),
        array((mask.shape[0] * n_hi, mask.shape[1]), f32), array((tokens, d_model), bf16),
        array((tokens, width), bf16), array((tokens, width), f32), array((tokens, width), f32),
        array((tokens, width), bf16), array((tokens, width), bf16),
        array((tokens // seq_len, heads, seq_len, seq_len), f32),
        array((rows, share), f32), array((rows, 128), f32),
        array((tokens, wide), f32), array((tokens, wide), f32),
    ]
    return pl.pallas_call(
        forward_body,
        out_shape=out_shape,
        in_specs=[any_spec] * 10 + [vmem] * 6,
        out_specs=[any_spec] * 11 + [vmem] * 10,
        scratch_shapes=move_scratch(weights) + token_scratch() * 3 + [
            pltpu.VMEM((d_model, width), bf16), pltpu.VMEM((d_model, width), bf16),
            pltpu.VMEM((d_model, width), bf16), pltpu.VMEM((tokens, d_model), bf16),
            pltpu.VMEM((tokens, width), bf16),
            pltpu.VMEM((tokens, share), bf16), pltpu.VMEM((tokens, share), bf16),
            pltpu.VMEM((tokens, share), f32), pltpu.VMEM((tokens, share), bf16),
            pltpu.VMEM((n_hi - 1, rows, share), bf16), pltpu.VMEM((rows, share), bf16),
            pltpu.VMEM((rows, share), bf16), pltpu.VMEM((rows, share), bf16),
            pltpu.VMEM(mask.shape, f32), pltpu.VMEM((mask.shape[0] * n_hi, seq_len), f32),
            pltpu.VMEM((rows, 128), f32), pltpu.VMEM((rows, 128), f32),
            pltpu.VMEM((2, d_model, 256), bf16),
            dma((9,)), dma((2,)), dma((2,)), dma((2,)), dma((n_hi - 1,)), dma((n_hi - 1,)),
            dma((n_hi - 1,)), dma((n_hi - 1,)),
        ],
        compiler_params=pltpu.CompilerParams(
            collective_id=collective_id, has_side_effects=True, vmem_limit_bytes=63 * 2**20
        ),
    )(*weights, grad, x, mask, x, gain_first, gain, bias, key_scale, value_scale)


class Spot:
    def __init__(self):
        self.n_hi, self.hi, self.mp = lax.axis_size("hi"), lax.axis_index("hi"), lax.axis_index("mp")

    def back(self, k):
        return lax.rem(self.hi + self.n_hi - k, self.n_hi)


def back_body(
    gate_w, up_w, down_w, d_gate, d_up, hidden, first_sum, inv, gain, grad,
    first_all, ffn_part, d_first,
    theirs, arrived, mine, theirs_ffn, arrived_ffn, mine_ffn, both, landed, own, stat, stat_in,
    tile_a, tile_b, sem_a, sem_b, here, x_send, x_recv, r_send, r_recv, *tok,
):
    f32, bf16 = jnp.float32, jnp.bfloat16
    m = Spot()
    rows, share = grad.shape
    tokens, d_model = first_all.shape
    t = Tokens(m, own, first_all, tok)
    partner = {"mp": 1 - m.mp}
    barrier = pltpu.get_barrier_semaphore()
    places = [{"hi": lax.rem(m.hi + s, m.n_hi)} for s in range(1, m.n_hi)] + [partner]
    for place in places:
        pl.semaphore_signal(barrier, inc=1, device_id=place, device_id_type=MESH)
    pl.semaphore_wait(barrier, len(places))
    tile = tile_a.shape[1]
    per_half = share // tile

    def product(pairs, far, close, copy):
        def bring(i):
            side = jnp.where(i < per_half, 1 - m.mp, m.mp)
            first = side * share + lax.rem(i, per_half) * tile
            slot = lax.rem(i, 2)
            return [
                pltpu.make_async_copy(
                    w.at[pl.ds(pl.multiple_of(first, tile), tile)], buf.at[slot], sem.at[slot]
                )
                for _, w, buf, sem in pairs
            ]

        def start(i):
            for one in bring(i):
                one.start()

        start(0)

        def step(i, store):
            pl.when(i + 1 < 2 * per_half)(lambda: start(i + 1))
            for one in bring(i):
                one.wait()
            slot = lax.rem(i, 2)
            total = None
            for left, _, buf, _ in pairs:
                term = contract_last(left[...], buf[slot])
                total = term if total is None else total + term
            store(pl.ds(pl.multiple_of(lax.rem(i, per_half) * tile, tile), tile), total)

        def far_step(i, carry):
            def store(cols, value):
                far[:, cols] = value.astype(bf16)

            step(i, store)
            return carry

        def close_step(i, carry):
            def store(cols, value):
                close[:, cols] = value

            step(i + per_half, store)
            return carry

        lax.fori_loop(0, per_half, far_step, 0)
        copy.start()
        lax.fori_loop(0, per_half, close_step, 0)

    def by_rows(count, size, body):
        def step(i, carry):
            body(pl.ds(pl.multiple_of(i * size, size), size))
            return carry

        lax.fori_loop(0, count // size, step, 0)

    halves = remote(theirs, arrived, x_send.at[0], x_recv.at[0], partner)
    stats = remote(stat, stat_in, x_send.at[1], x_recv.at[1], partner)
    halves_ffn = remote(theirs_ffn, arrived_ffn, x_send.at[2], x_recv.at[2], partner)

    def reduce_copy(s):
        there = lax.rem(m.hi + s, m.n_hi)
        return remote(
            both.at[pl.ds(there * rows, rows)], landed.at[s - 1],
            r_send.at[s - 1], r_recv.at[s - 1], {"hi": there},
        )

    product(
        [(d_gate, gate_w, tile_a, sem_a), (d_up, up_w, tile_b, sem_b)], theirs, mine, halves
    )
    halves.wait_recv()

    def join(at):
        both[at, :] = (mine[at, :] + arrived[at, :].astype(f32)).astype(bf16)

    by_rows(tokens, 32, join)
    for s in range(1, m.n_hi):
        reduce_copy(s).start()
    product([(hidden, down_w, tile_a, sem_a)], theirs_ffn, mine_ffn, halves_ffn)
    halves_ffn.wait_recv()

    def join_ffn(at):
        ffn_part[at, :] = (mine_ffn[at, :] + arrived_ffn[at, :].astype(f32)).astype(bf16)

    by_rows(tokens, 32, join_ffn)
    for s in range(1, m.n_hi):
        reduce_copy(s).wait_recv()

    def add(at):
        at_own = pl.ds(pl.multiple_of(m.hi * rows, rows) + at.start, at.size)
        total = mine[at_own, :] + arrived[at_own, :].astype(f32)
        for s in range(m.n_hi - 1):
            total = total + landed[s, at, :].astype(f32)
        total = total * gain[...]
        d_first[at, :] = total
        dots = jnp.sum(total * first_sum[at, :], axis=-1, keepdims=True)
        stat[at, :] = jnp.broadcast_to(dots, (at.size, stat.shape[1]))

    by_rows(rows, 32, add)
    stats.start()
    stats.wait_recv()

    def finish(at):
        inverse = inv[at, :][:, :1]
        mean = (stat[at, :] + stat_in[at, :])[:, :1] / d_model
        total = (
            grad[at, :].astype(f32)
            + inverse * d_first[at, :]
            - first_sum[at, :] * (inverse * inverse * inverse * mean)
        )
        d_first[at, :] = total
        own[at, :] = total.astype(bf16)

    by_rows(rows, 32, finish)
    t.send()
    put = pltpu.make_async_copy(own, t.place(m.hi), here.at[0])
    put.start()
    for r in range(1, m.n_hi):
        t.relay(r)
    t.finish()
    put.wait()
    halves.wait_send()
    halves_ffn.wait_send()
    stats.wait_send()
    for s in range(1, m.n_hi):
        reduce_copy(s).wait_send()


def back_kernel(
    gate_w, up_w, down_w, d_gate, d_up, hidden, first_sum, inv, gain, grad, collective_id
):
    f32, bf16 = jnp.float32, jnp.bfloat16
    n_hi = lax.axis_size("hi")
    dma = pltpu.SemaphoreType.DMA
    any_spec = pl.BlockSpec(memory_space=pl.ANY)
    vmem = pl.BlockSpec(memory_space=pltpu.VMEM)
    rows, share = grad.shape
    tokens, wide = d_gate.shape
    array = jax.ShapeDtypeStruct
    return pl.pallas_call(
        back_body,
        out_shape=[
            array((tokens, gate_w.shape[0]), bf16), array((tokens, share), bf16),
            array((rows, share), f32),
        ],
        in_specs=[any_spec] * 3 + [vmem] * 7,
        out_specs=[any_spec, vmem, vmem],
        scratch_shapes=[
            pltpu.VMEM((tokens, share), bf16), pltpu.VMEM((tokens, share), bf16),
            pltpu.VMEM((tokens, share), f32),
            pltpu.VMEM((tokens, share), bf16), pltpu.VMEM((tokens, share), bf16),
            pltpu.VMEM((tokens, share), f32), pltpu.VMEM((tokens, share), bf16),
            pltpu.VMEM((n_hi - 1, rows, share), bf16), pltpu.VMEM((rows, share), bf16),
            pltpu.VMEM((rows, 128), f32), pltpu.VMEM((rows, 128), f32),
            pltpu.VMEM((2, 256, wide), bf16), pltpu.VMEM((2, 256, wide), bf16),
            dma((2,)), dma((2,)), dma((1,)), dma((3,)), dma((3,)),
            dma((n_hi - 1,)), dma((n_hi - 1,)),
        ] + token_scratch(),
        compiler_params=pltpu.CompilerParams(
            collective_id=collective_id, has_side_effects=True, vmem_limit_bytes=60 * 2**20
        ),
    )(gate_w, up_w, down_w, d_gate, d_up, hidden, first_sum, inv, gain, grad)


def on_device_columns(
    hidden_in, lengths, norm_attn, q_weight, k_weight, v_weight, out_weight_t, norm_ffn,
    gate_weight, up_weight, down_weight_t, scale_key, scale_value, scale_ffn, out_grad,
    position_bias,
):
    f32, bf16 = jnp.float32, jnp.bfloat16
    n_hi, n_lo = lax.axis_size("hi"), lax.axis_size("lo")
    hi, lo, mp = lax.axis_index("hi"), lax.axis_index("lo"), lax.axis_index("mp")
    d_model = norm_attn.shape[0]
    tokens_local, share = hidden_in.shape
    seq_local = lengths.shape[0]
    seq_len = tokens_local // seq_local
    tokens = n_hi * tokens_local

    def swap_lo(x, bit):
        return lax.ppermute(x, "lo", [(i, i ^ bit) for i in range(n_lo)])

    def swap_hi(x, bit):
        return lax.ppermute(x, "hi", [(i, i ^ bit) for i in range(n_hi)])

    def swap_mp(x):
        return lax.ppermute(x, "mp", [(0, 1), (1, 0)])

    def own_columns(x):
        width = x.shape[-1] // n_hi
        return lax.dynamic_slice_in_dim(x, hi * width, width, x.ndim - 1)

    def times(x, w):
        return jnp.dot(x, w, preferred_element_type=f32)

    def join_features(own):
        other = swap_mp(own)
        lower = jnp.where(mp == 0, own, other)
        upper = jnp.where(mp == 0, other, own)
        return jnp.concatenate([lower, upper], axis=1)

    def back_sum(pairs):
        total = None
        for x, w in pairs:
            term = contract_last(x, w)
            total = term if total is None else total + term
        mine = lax.dynamic_slice_in_dim(total, mp * share, share, 1)
        theirs = lax.dynamic_slice_in_dim(total, (1 - mp) * share, share, 1)
        return (mine + swap_mp(theirs.astype(bf16)).astype(f32)).astype(bf16)

    def scatter(x):
        return lax.psum_scatter(x, "hi", scatter_dimension=0, tiled=True).astype(f32)

    def token_mean(x):
        part = jnp.sum(x, axis=-1, keepdims=True)
        return (part + swap_mp(part)) / d_model

    def own_half(gain):
        return lax.dynamic_slice_in_dim(gain, mp * share, share, 0)[None]

    gain_ffn = own_half(norm_ffn)
    gain_attn_half = own_half(norm_attn)
    gain_attn = norm_attn[None]
    key_scale, value_scale = own_columns(scale_key), own_columns(scale_value)
    ffn_scale = own_columns(scale_ffn)

    inputs_half = hidden_in
    grad_half = lax.dynamic_slice_in_dim(out_grad, mp * share, share, 1)
    keep = lax.broadcasted_iota(jnp.int32, (8 * seq_local, seq_len), 1) < lengths[0]
    mask = jnp.where(keep, 0.0, NEGATIVE)
    heads_local = q_weight.shape[1] // n_hi // HEAD_DIM
    bias = lax.dynamic_slice_in_dim(position_bias, hi * heads_local, heads_local, 0)
    (
        q_w, k_w, v_w, o_w, gate_w, up_w, down_w, grad_all, inputs_all, _, _, queries, key_pre,
        value_pre, key_rows, value_rows, attn_probs, first_sum, inv_second, gate_proj, upward,
    ) = forward_kernel(
        (q_weight, k_weight, v_weight, out_weight_t, gate_weight, up_weight, down_weight_t),
        out_grad, hidden_in, mask, gain_attn, gain_ffn, bias, key_scale[None],
        value_scale[None], 0,
    )
    inputs32 = lax.dynamic_slice_in_dim(
        inputs_all, hi * tokens_local, tokens_local, 0
    ).astype(f32)
    inv_mine = lax.rsqrt(
        jnp.sum(inputs32 * inputs32, axis=-1, keepdims=True) / d_model + EPSILON
    )
    n_seq = n_hi * seq_local
    shaped = (n_seq, seq_len, heads_local, HEAD_DIM)
    q_heads = queries.reshape(shaped)
    k_heads = key_rows.reshape(shaped)
    v_heads = value_rows.reshape(shaped)
    probs_low = attn_probs.astype(bf16)
    d_hidden = times(grad_all, down_w)
    activated, gelu_back = jax.vjp(gelu_tanh, gate_proj)
    product = activated * upward
    hidden = (product * ffn_scale).astype(bf16)
    grad_ffn_part = jnp.sum(d_hidden * product, axis=0)
    d_product = d_hidden * ffn_scale
    d_gate = gelu_back(d_product * upward)[0].astype(bf16)
    d_up = (d_product * activated).astype(bf16)
    d_first_all, ffn_part, d_first = back_kernel(
        gate_w, up_w, down_w, d_gate, d_up, hidden, first_sum, inv_second, gain_ffn,
        grad_half, 1,
    )
    ffn_out = scatter(ffn_part)
    d_context = times(d_first_all, o_w).astype(bf16)
    dc_heads = d_context.reshape(shaped)
    d_probs = jnp.einsum("bihe,bjhe->bhij", dc_heads, v_heads, preferred_element_type=f32)
    d_scores = (
        attn_probs * (d_probs - jnp.sum(attn_probs * d_probs, axis=-1, keepdims=True))
    ).astype(bf16)
    d_values = jnp.einsum(
        "bhij,bihe->bjhe", probs_low, dc_heads, preferred_element_type=f32
    ).reshape(tokens, -1)
    d_keys = jnp.einsum(
        "bhij,bihe->bjhe", d_scores, q_heads, preferred_element_type=f32
    ).reshape(tokens, -1)
    d_queries = (
        jnp.einsum("bhij,bjhe->bihe", d_scores, k_heads, preferred_element_type=f32)
        .reshape(tokens, -1)
        .astype(bf16)
    )
    grad_key_part = jnp.sum(d_keys * key_pre, axis=0)
    grad_value_part = jnp.sum(d_values * value_pre, axis=0)
    d_key_pre = (d_keys * key_scale).astype(bf16)
    d_value_pre = (d_values * value_scale).astype(bf16)
    ffn_out, d_queries = lax.optimization_barrier((ffn_out, d_queries))
    scaled_in = (
        scatter(back_sum([(d_queries, q_w), (d_key_pre, k_w), (d_value_pre, v_w)]))
        * gain_attn_half
    )
    mine32 = inputs_half.astype(f32)
    mean_dot = token_mean(scaled_in * mine32)
    input_grad = (
        d_first
        + inv_mine * scaled_in
        - mine32 * inv_mine * inv_mine * inv_mine * mean_dot
    ).astype(bf16)
    block_out = (first_sum + ffn_out).astype(bf16)

    def totals(part):
        part = part[None]
        for bit in (1, 2):
            part = part + swap_lo(part, bit)
        for bit in (1, 2):
            other = swap_hi(part, bit)
            upper = (hi & bit) > 0
            part = jnp.concatenate(
                [jnp.where(upper, other, part), jnp.where(upper, part, other)], axis=0
            )
        return part

    attn_totals = totals(jnp.concatenate([grad_key_part, grad_value_part]))
    width = grad_key_part.shape[0]
    return (
        block_out,
        input_grad,
        attn_totals[:, :width].reshape(-1),
        attn_totals[:, width:].reshape(-1),
        totals(grad_ffn_part).reshape(-1),
    )


def solution(mesh):
    n_dp, n_mp = mesh.shape["dp"], mesh.shape["mp"]
    n_hi = 1
    while n_dp % (n_hi * 2) == 0 and n_hi * n_hi < n_dp:
        n_hi *= 2
    grid = jax.sharding.Mesh(
        mesh.devices.reshape(n_hi, n_dp // n_hi, n_mp), ("hi", "lo", "mp")
    )
    dp = ("hi", "lo")
    weight = P(dp, "mp")
    columns = (n_hi, n_dp // n_hi, n_mp) == (4, 4, 2)
    return jax.shard_map(
        on_device_columns if columns else on_device_general,
        mesh=grid,
        in_specs=(
            P(dp, "mp"), P(dp), P(), weight, weight, weight, weight, P(), weight, weight, weight,
            P("mp"), P("mp"), P("mp"), P(dp, None), P("mp", None, None),
        ),
        out_specs=(P(dp, "mp"), P(dp, "mp"), P("mp"), P("mp"), P("mp")),
        check_vma=False,
    )
```

```python
import functools

import jax
import jax.numpy as jnp
from jax import lax
from jax.experimental import pallas as pl
from jax.experimental.pallas import tpu as pltpu
from jax.sharding import PartitionSpec as P

HEAD_DIM = 64
MESH = pl.DeviceIdType.MESH


EPSILON = 1e-06
NEGATIVE = -1e30


def inverse_rms(values):
    return lax.rsqrt(jnp.mean(values * values, axis=-1, keepdims=True) + EPSILON)


def gelu_tanh(values):
    return jax.nn.gelu(values, approximate=True)


def contract_last(left_side, right_side):
    return lax.dot_general(
        left_side, right_side, (((1,), (1,)), ((), ())), preferred_element_type=jnp.float32
    )


def norm_back(grad_in, values, inverse, gain_vec):
    scaled = grad_in * gain_vec
    correction = (
        values * inverse * inverse * inverse * jnp.mean(scaled * values, axis=-1, keepdims=True)
    )
    return inverse * scaled - correction


WEIGHT_AXIS = "lo"


def on_device_general(
    hidden_in, lengths, norm_attn, q_weight, k_weight, v_weight, out_weight_t, norm_ffn,
    gate_weight, up_weight, down_weight_t, scale_key, scale_value, scale_ffn, out_grad,
    position_bias,
):
    f32, bf16 = jnp.float32, jnp.bfloat16
    wa = WEIGHT_AXIS
    ta = "lo" if wa == "hi" else "hi"
    n_hi, n_lo = lax.axis_size("hi"), lax.axis_size("lo")
    n_t = lax.axis_size(ta)

    def swap(x, bit):
        return lax.ppermute(x, "lo", [(i, i ^ bit) for i in range(n_lo)])

    def own_first(parts):
        if n_lo != 4:
            return parts
        index = lax.axis_index("lo")
        rows, width = parts.shape[0], parts.shape[-1]
        parts = parts.reshape(rows, n_hi, 2, 2, width)
        parts = jnp.where((index & 2) > 0, parts[:, :, ::-1], parts)
        parts = jnp.where((index & 1) > 0, parts[:, :, :, ::-1], parts)
        return parts.reshape(rows, n_hi, n_lo, width)

    def sum_mp(x):
        x = x.astype(bf16)
        if lax.axis_size("mp") != 2:
            return lax.psum(x, "mp").astype(f32)
        return x.astype(f32) + lax.ppermute(x, "mp", [(0, 1), (1, 0)]).astype(f32)

    def split_features(x):
        rows = x.shape[0]
        parts = own_first(x.reshape(rows, n_hi, n_lo, -1))
        order = (1, 0, 2, 3) if ta == "hi" else (2, 0, 1, 3)
        return parts.transpose(order).reshape(n_t, rows, -1)

    def join_features(x):
        rows = x.shape[1]
        if ta == "hi":
            parts = x.transpose(1, 0, 2).reshape(rows, n_hi, n_lo, -1)
            return own_first(parts).reshape(rows, -1)
        return x.reshape(n_lo, rows, n_hi, -1).transpose(1, 2, 0, 3).reshape(rows, -1)

    def exchange(x):
        return lax.all_to_all(x, ta, split_axis=0, concat_axis=0, tiled=True)

    def gather_rows(w):
        if n_lo != 4:
            return lax.all_gather(w, wa, axis=0, tiled=True)
        half = w.shape[0] // 2
        first, second = swap(w, 1), swap(w, 2)
        third = swap(second[:half], 1), swap(first[half:], 2)
        return jnp.concatenate([w, first, second, *third], axis=0)

    def gather_tokens(x):
        return lax.all_gather(x, ta, axis=0, tiled=True)

    def scatter_tokens(x):
        return lax.psum_scatter(x.astype(bf16), ta, scatter_dimension=0, tiled=True)

    def dot(a, b):
        return jnp.dot(a, b, preferred_element_type=f32)

    d_model = norm_attn.shape[0]
    tokens_local = hidden_in.shape[0]
    seq_local = lengths.shape[0]
    seq_len = tokens_local // seq_local
    t_index = lax.axis_index(ta)
    gain_attn = split_features(norm_attn[None])
    gain_attn = lax.dynamic_index_in_dim(gain_attn, t_index, 0, False)
    gain_ffn = split_features(norm_ffn[None])
    gain_ffn = lax.dynamic_index_in_dim(gain_ffn, t_index, 0, False)

    full_inputs = lax.all_gather(hidden_in, "mp", axis=1, tiled=True)
    both = jnp.concatenate([split_features(full_inputs), split_features(out_grad)], axis=2)
    both = exchange(both).reshape(n_t * tokens_local, -1)
    inputs_blk, out_grad_blk = jnp.split(both, 2, axis=1)
    inputs32 = inputs_blk.astype(f32)

    def token_mean(x):
        return lax.psum(jnp.sum(x, axis=-1, keepdims=True), ta) / d_model

    q_full, k_full, v_full = gather_rows(q_weight), gather_rows(k_weight), gather_rows(v_weight)
    o_full = gather_rows(out_weight_t)
    gate_full, up_full = gather_rows(gate_weight), gather_rows(up_weight)
    down_full = gather_rows(down_weight_t)

    inv_first = lax.rsqrt(token_mean(inputs32 * inputs32) + EPSILON)
    normed_first = (inputs32 * inv_first * gain_attn).astype(bf16)
    queries = scatter_tokens(dot(normed_first, q_full))
    key_pre = scatter_tokens(dot(normed_first, k_full)).astype(f32)
    value_pre = scatter_tokens(dot(normed_first, v_full)).astype(f32)
    heads_local = queries.shape[1] // HEAD_DIM
    shaped = (seq_local, seq_len, heads_local, HEAD_DIM)
    key_rows = (key_pre * scale_key).astype(bf16)
    value_rows = (value_pre * scale_value).astype(bf16)
    q_heads = queries.reshape(shaped)
    k_heads = key_rows.reshape(shaped)
    v_heads = value_rows.reshape(shaped)
    scores = (
        jnp.einsum("bihe,bjhe->bhij", q_heads, k_heads, preferred_element_type=f32)
        + position_bias[None]
    )
    positions = lax.broadcasted_iota(jnp.int32, (seq_local, seq_len), 1)
    valid_keys = positions < lengths[:, None]
    scores = jnp.where(valid_keys[:, None, None, :], scores, NEGATIVE)
    largest = jnp.max(scores, axis=-1, keepdims=True)
    exponent = jnp.exp(scores - largest)
    attn_probs = exponent / jnp.sum(exponent, axis=-1, keepdims=True)
    probs_low = attn_probs.astype(bf16)
    context = (
        jnp.einsum("bhij,bjhe->bihe", probs_low, v_heads, preferred_element_type=f32)
        .reshape(tokens_local, -1)
        .astype(bf16)
    )
    first_sum = inputs32 + sum_mp(contract_last(gather_tokens(context), o_full))
    inv_second = lax.rsqrt(token_mean(first_sum * first_sum) + EPSILON)
    normed_second = (first_sum * inv_second * gain_ffn).astype(bf16)
    gate_proj = scatter_tokens(dot(normed_second, gate_full)).astype(f32)
    upward = scatter_tokens(dot(normed_second, up_full)).astype(f32)
    d_hidden = scatter_tokens(dot(out_grad_blk, down_full)).astype(f32)
    activated, gelu_back = jax.vjp(gelu_tanh, gate_proj)
    product = activated * upward
    hidden = (product * scale_ffn).astype(bf16)
    grad_ffn_part = jnp.sum(d_hidden * product, axis=0)
    d_product = d_hidden * scale_ffn
    d_gate = gelu_back(d_product * upward)[0].astype(bf16)
    d_up = (d_product * activated).astype(bf16)
    d_second = sum_mp(
        contract_last(gather_tokens(d_gate), gate_full)
        + contract_last(gather_tokens(d_up), up_full)
    )
    scaled = d_second * gain_ffn
    d_first = (
        out_grad_blk.astype(f32)
        + inv_second * scaled
        - first_sum * inv_second * inv_second * inv_second * token_mean(scaled * first_sum)
    )
    d_context = scatter_tokens(dot(d_first.astype(bf16), o_full))
    dc_heads = d_context.reshape(shaped)
    d_probs = jnp.einsum("bihe,bjhe->bhij", dc_heads, v_heads, preferred_element_type=f32)
    d_scores = (
        attn_probs * (d_probs - jnp.sum(attn_probs * d_probs, axis=-1, keepdims=True))
    ).astype(bf16)
    d_values = jnp.einsum(
        "bhij,bihe->bjhe", probs_low, dc_heads, preferred_element_type=f32
    ).reshape(tokens_local, -1)
    d_keys = jnp.einsum(
        "bhij,bihe->bjhe", d_scores, q_heads, preferred_element_type=f32
    ).reshape(tokens_local, -1)
    d_queries = (
        jnp.einsum("bhij,bjhe->bihe", d_scores, k_heads, preferred_element_type=f32)
        .reshape(tokens_local, -1)
        .astype(bf16)
    )
    grad_key_part = jnp.sum(d_keys * key_pre, axis=0)
    grad_value_part = jnp.sum(d_values * value_pre, axis=0)
    d_key_pre = (d_keys * scale_key).astype(bf16)
    d_value_pre = (d_values * scale_value).astype(bf16)
    d_normed = sum_mp(
        contract_last(gather_tokens(d_queries), q_full)
        + contract_last(gather_tokens(d_key_pre), k_full)
        + contract_last(gather_tokens(d_value_pre), v_full)
    )
    scaled_in = d_normed * gain_attn
    mean_dot = token_mean(scaled_in * inputs32)
    input_grad = (
        d_first
        + inv_first * scaled_in
        - inputs32 * inv_first * inv_first * inv_first * mean_dot
    ).astype(bf16)

    ffn_out = sum_mp(contract_last(gather_tokens(hidden), down_full))
    block_out = (first_sum + ffn_out).astype(bf16)

    share_width = hidden_in.shape[1]
    offset = lax.axis_index("mp") * share_width

    def own_share(x):
        joined = join_features(exchange(x.reshape(n_t, tokens_local, -1)))
        return lax.dynamic_slice_in_dim(joined, offset, share_width, 1)

    parts = jnp.concatenate([grad_key_part, grad_value_part, grad_ffn_part])
    totals = lax.psum(lax.psum(parts, "lo"), "hi")
    width = grad_key_part.shape[0]
    return (
        own_share(block_out),
        own_share(input_grad),
        totals[:width],
        totals[width : 2 * width],
        totals[2 * width :],
    )


class Moves:
    def __init__(self, weights, outs, holds, sems, order):
        self.weights, self.outs, self.holds, self.order = weights, outs, holds, order
        self.own, self.asend, self.arecv, self.bsend, self.brecv, self.csend, self.crecv = sems
        self.n_hi, self.n_lo = lax.axis_size("hi"), lax.axis_size("lo")
        self.hi, self.lo = lax.axis_index("hi"), lax.axis_index("lo")
        self.mp = lax.axis_index("mp")
        self.block = weights[0].shape[0]
        self.next = 0

    def barrier(self):
        barrier = pltpu.get_barrier_semaphore()
        places = [{"hi": lax.rem(self.hi + s, self.n_hi)} for s in range(1, self.n_hi)]
        places += [{"lo": self.lo ^ 1}, {"lo": self.lo ^ 2}, {"mp": 1 - self.mp}]
        for place in places:
            pl.semaphore_signal(barrier, inc=1, device_id=place, device_id_type=MESH)
        pl.semaphore_wait(barrier, len(places))

    def back(self, k):
        return lax.rem(self.hi + self.n_hi - k, self.n_hi)

    def rows(self, w, hi, lo, start=0, size=None):
        first = (hi * self.n_lo + lo) * self.block + start
        return self.outs[w].at[pl.ds(first, size or self.block)]

    def columns(self, w, index):
        width = self.weights[w].shape[1] // self.n_hi
        return self.weights[w].at[:, pl.ds(pl.multiple_of(index * width, 128), width)]

    def a(self, w, s):
        there = lax.rem(self.hi + s, self.n_hi)
        return remote(
            self.columns(w, there), self.rows(w, self.hi, self.lo),
            self.asend.at[w, s - 1], self.arecv.at[w, s - 1], {"hi": there},
        )

    def b(self, w, k, bit):
        dst = self.rows(w, self.back(k), self.lo)
        src = self.columns(w, self.hi) if k == 0 else dst
        return remote(
            src, dst, self.bsend.at[w, k, bit - 1], self.brecv.at[w, k, bit - 1],
            {"lo": self.lo ^ bit},
        )

    def c(self, w, k, bit):
        half = self.block // 2
        part = self.rows(w, self.back(k), self.lo ^ bit, (bit - 1) * half, half)
        return remote(
            part, part, self.csend.at[w, k, bit - 1], self.crecv.at[w, k, bit - 1],
            {"lo": self.lo ^ (3 - bit)},
        )

    def exchange(self, w, first=1, last=None):
        for s in range(first, last or self.n_hi):
            self.a(w, s).start()

    def own_in(self, w):
        return pltpu.make_async_copy(self.columns(w, self.hi), self.holds[w], self.own.at[w])

    def own_out(self, w):
        return pltpu.make_async_copy(
            self.holds[w], self.rows(w, self.hi, self.lo), self.own.at[w]
        )

    def start_own(self):
        for w in range(len(self.weights)):
            self.own_in(w).start()

    def place_own(self):
        for w in range(len(self.weights)):
            self.own_in(w).wait()
            self.own_out(w).start()

    def relay(self, n):
        w, k = self.order[n]
        for bit in (1, 2):
            self.b(w, k, bit).wait_recv()
            self.c(w, k, bit).start()

    def advance(self, count=1):
        for _ in range(count):
            n = self.next
            if n < len(self.order):
                w, k = self.order[n]
                if k > 0:
                    self.a(w, k).wait_recv()
                for bit in (1, 2):
                    self.b(w, k, bit).start()
            if n >= 2:
                self.relay(n - 2)
            self.next = n + 1

    def arrived(self, w):
        for k in range(self.n_hi):
            for bit in (1, 2):
                self.c(w, k, bit).wait_recv()
        self.own_out(w).wait()

    def drain(self):
        for w in range(len(self.weights)):
            for s in range(1, self.n_hi):
                self.a(w, s).wait_send()
            for k in range(self.n_hi):
                for bit in (1, 2):
                    self.b(w, k, bit).wait_send()
                    self.c(w, k, bit).wait_send()


class Tokens:
    def __init__(self, moves, src, out, sems):
        self.m, self.src, self.out = moves, src, out
        self.usend, self.urecv, self.dsend, self.drecv, self.msend, self.mrecv = sems

    def place(self, origin):
        rows, width = self.src.shape
        return self.out.at[
            pl.ds(origin * rows, rows), pl.ds(pl.multiple_of(self.m.mp * width, 128), width)
        ]

    def up(self, d):
        place = self.place(self.m.hi - d)
        return remote(
            self.src if d == 0 else place, place, self.usend.at[d], self.urecv.at[d],
            {"hi": lax.rem(self.m.hi + 1, self.m.n_hi)},
        )

    def down(self, d):
        place = self.place(self.m.hi + d)
        return remote(
            self.src if d == 0 else place, place, self.dsend.at[d], self.drecv.at[d],
            {"hi": lax.rem(self.m.hi + self.m.n_hi - 1, self.m.n_hi)},
        )

    def landed(self, origin, sem):
        place = self.place(origin)
        return remote(
            place, place, sem, sem, {"hi": lax.rem(self.m.hi + 1, self.m.n_hi)}
        )

    def near(self, s):
        place = self.place(self.m.back(s))
        return remote(
            self.src if s == 0 else place, place, self.msend.at[s], self.mrecv.at[s],
            {"mp": 1 - self.m.mp},
        )

    def goes_up(self, d):
        return (self.m.hi >= d) & (self.m.hi + 1 < self.m.n_hi)

    def goes_down(self, d):
        return (self.m.hi + d < self.m.n_hi) & (self.m.hi > 0)

    def send(self):
        pl.when(self.goes_up(0))(lambda: self.up(0).start())
        pl.when(self.goes_down(0))(lambda: self.down(0).start())
        self.near(0).start()

    def relay(self, r):
        hi, n_hi = self.m.hi, self.m.n_hi

        def from_below():
            self.landed(hi - r, self.urecv.at[r - 1]).wait_recv()
            if r < n_hi - 1:
                pl.when(hi + 1 < n_hi)(lambda: self.up(r).start())
            self.near(r).start()

        def from_above():
            self.landed(hi + r, self.drecv.at[r - 1]).wait_recv()
            if r < n_hi - 1:
                pl.when(hi > 0)(lambda: self.down(r).start())
            self.near(n_hi - r).start()

        pl.when(hi >= r)(from_below)
        pl.when(hi + r < n_hi)(from_above)

    def finish(self):
        for s in range(self.m.n_hi):
            self.near(s).wait_recv()
        for s in range(self.m.n_hi):
            self.near(s).wait_send()
        for d in range(self.m.n_hi - 1):
            pl.when(self.goes_up(d))(lambda d=d: self.up(d).wait_send())
            pl.when(self.goes_down(d))(lambda d=d: self.down(d).wait_send())


def remote(src, dst, send, recv, where):
    return pltpu.make_async_remote_copy(
        src_ref=src, dst_ref=dst, send_sem=send, recv_sem=recv,
        device_id=where, device_id_type=MESH,
    )


def move_scratch(weights):
    n_hi, n_w = lax.axis_size("hi"), len(weights)
    dma = pltpu.SemaphoreType.DMA
    sems = [dma((n_w,)), dma((n_w, n_hi - 1)), dma((n_w, n_hi - 1))]
    sems += [dma((n_w, n_hi, 2)) for _ in range(4)]
    holds = [pltpu.VMEM((w.shape[0], w.shape[1] // n_hi), w.dtype) for w in weights]
    return sems + holds


def token_scratch():
    n_hi = lax.axis_size("hi")
    dma = pltpu.SemaphoreType.DMA
    return [dma((n_hi - 1,)) for _ in range(4)] + [dma((n_hi,)), dma((n_hi,))]


def gathered(w):
    n_hi, n_lo = lax.axis_size("hi"), lax.axis_size("lo")
    return jax.ShapeDtypeStruct((w.shape[0] * n_hi * n_lo, w.shape[1] // n_hi), w.dtype)


def forward_body(
    q_w, k_w, v_w, o_w, gate_w, up_w, down_w, grad, x, mask, hidden, gain_first, gain, bias,
    key_scale, value_scale,
    q_all, k_all, v_all, o_out, gate_out, up_out, down_out, grad_out, x_out, mask_out,
    second_out, q_out, key_pre, value_pre, key_rows, value_rows, probs_out, sum_out, inv_out,
    gate_proj, upward,
    *scratch,
):
    f32, bf16 = jnp.float32, jnp.bfloat16
    sems, holds = scratch[:7], scratch[7:14]
    g_tok, n_tok, x_tok = scratch[14:20], scratch[20:26], scratch[26:32]
    (q_full, k_full, v_full, normed, context, theirs, arrived, mine, both, landed, second_own,
     grad_hold, x_hold, mask_hold, mask_full, stat, stat_in, tiles, here, tile_sem, x_send,
     x_recv, r_send, r_recv, m_send, m_recv) = scratch[32:]
    o_full, second_full = q_full, normed
    order = [
        (0, 0), (1, 0), (2, 0), (4, 0), (0, 1), (0, 2), (0, 3), (3, 0), (1, 1), (1, 2), (1, 3),
        (5, 0), (2, 1), (2, 2), (2, 3), (3, 1), (3, 2), (3, 3), (4, 1), (4, 2), (4, 3), (6, 0),
        (5, 1), (5, 2), (5, 3), (6, 1), (6, 2), (6, 3),
    ]
    m = Moves(
        (q_w, k_w, v_w, o_w, gate_w, up_w, down_w),
        (q_all, k_all, v_all, o_out, gate_out, up_out, down_out), holds, sems, order,
    )
    rows, share = hidden.shape
    tokens, d_model = normed.shape
    seq_len = probs_out.shape[-1]
    partner = {"mp": 1 - m.mp}
    grad_half = grad.at[:, pl.ds(pl.multiple_of(m.mp * share, 128), share)]
    g = Tokens(m, grad_half, grad_out, g_tok)
    t = Tokens(m, second_own, second_out, n_tok)
    xt = Tokens(m, x, x_out, x_tok)
    x_in = pltpu.make_async_copy(x, x_hold, here.at[3])
    x_put = pltpu.make_async_copy(x_hold, xt.place(m.hi), here.at[3])
    mask_rows = mask.shape[0]
    mask_place = mask_out.at[pl.ds(m.hi * mask_rows, mask_rows)]
    mask_in = pltpu.make_async_copy(mask, mask_hold, here.at[4])
    mask_put = pltpu.make_async_copy(mask_hold, mask_place, here.at[4])
    grad_in = pltpu.make_async_copy(grad_half, grad_hold, here.at[0])
    grad_put = pltpu.make_async_copy(grad_hold, g.place(m.hi), here.at[0])

    def project(w_ref, store):
        tile = 256

        def step(i, carry):
            cols = pl.ds(pl.multiple_of(i * tile, tile), tile)
            store(cols, jnp.dot(normed[...], w_ref[:, cols], preferred_element_type=f32))
            return carry

        lax.fori_loop(0, w_ref.shape[1] // tile, step, 0)

    def store_query(cols, value):
        q_out[:, cols] = value.astype(bf16)

    def store_key(cols, value):
        key_pre[:, cols] = value
        key_rows[:, cols] = (value * key_scale[:, cols]).astype(bf16)

    def store_value(cols, value):
        value_pre[:, cols] = value
        value_rows[:, cols] = (value * value_scale[:, cols]).astype(bf16)

    def attend(seq):
        where = pl.ds(seq * seq_len, seq_len)
        hidden_keys = mask_full[pl.ds(seq * 8, 8), :][:1] < 0.0
        low = lax.broadcasted_iota(jnp.int32, (seq_len, 2 * HEAD_DIM), 1) < HEAD_DIM
        zero = jnp.zeros((seq_len, 2 * HEAD_DIM), bf16)
        for pair in range(probs_out.shape[1] // 2):
            cols = slice(pair * 2 * HEAD_DIM, (pair + 1) * 2 * HEAD_DIM)
            q2, k2, v2 = q_out[where, cols], key_rows[where, cols], value_rows[where, cols]
            outs = []
            for e in range(2):
                head = 2 * pair + e
                qe = jnp.where(low, q2, zero) if e == 0 else jnp.where(low, zero, q2)
                scores = contract_last(qe, k2) + bias[head]
                scores = jnp.where(hidden_keys, NEGATIVE, scores)
                exponent = jnp.exp(scores - jnp.max(scores, axis=-1, keepdims=True))
                probs = exponent / jnp.sum(exponent, axis=-1, keepdims=True)
                probs_out[seq, head] = probs
                outs.append(jnp.dot(probs.astype(bf16), v2, preferred_element_type=f32))
            context[where, cols] = jnp.where(low, outs[0], outs[1]).astype(bf16)

    def attend_some(first, count):
        def step(i, carry):
            attend(first + i)
            return carry

        lax.fori_loop(0, count, step, 0)

    def out_project(first_row, store):
        tile = 256

        def step(i, carry):
            w_rows = pl.ds(pl.multiple_of(first_row + i * tile, tile), tile)
            cols = pl.ds(pl.multiple_of(i * tile, tile), tile)
            store(cols, contract_last(context[...], o_full[w_rows, :]))
            return carry

        lax.fori_loop(0, share // tile, step, 0)

    def widen(w_ref, out_ref):
        tile = tiles.shape[2]
        count = w_ref.shape[1] // tile

        def bring(i):
            slot = lax.rem(i, 2)
            cols = pl.ds(pl.multiple_of(i * tile, tile), tile)
            return pltpu.make_async_copy(w_ref.at[:, cols], tiles.at[slot], tile_sem.at[slot])

        bring(0).start()

        def step(i, carry):
            pl.when(i + 1 < count)(lambda: bring(i + 1).start())
            bring(i).wait()
            cols = pl.ds(pl.multiple_of(i * tile, tile), tile)
            out_ref[:, cols] = jnp.dot(
                second_full[...], tiles[lax.rem(i, 2)], preferred_element_type=f32
            )
            return carry

        lax.fori_loop(0, count, step, 0)

    def store_theirs(cols, value):
        theirs[:, cols] = value.astype(bf16)

    def store_mine(cols, value):
        mine[:, cols] = value

    def by_rows(count, size, body):
        def step(i, carry):
            body(pl.ds(pl.multiple_of(i * size, size), size))
            return carry

        lax.fori_loop(0, count // size, step, 0)

    halves = remote(theirs, arrived, x_send.at[0], x_recv.at[0], partner)
    stats = remote(stat, stat_in, x_send.at[1], x_recv.at[1], partner)

    def mask_copy(s):
        there = lax.rem(m.hi + s, m.n_hi)
        return remote(mask, mask_place, m_send.at[s - 1], m_recv.at[s - 1], {"hi": there})

    def reduce_copy(s):
        there = lax.rem(m.hi + s, m.n_hi)
        return remote(
            both.at[pl.ds(there * rows, rows)], landed.at[s - 1],
            r_send.at[s - 1], r_recv.at[s - 1], {"hi": there},
        )

    def load(pairs):
        copies = [
            pltpu.make_async_copy(src, dst, here.at[5 + i]) for i, (src, dst) in enumerate(pairs)
        ]
        for copy in copies:
            copy.start()
        for copy in copies:
            copy.wait()

    def normalise_first(at):
        value = normed[at, :].astype(f32)
        square = jnp.sum(value * value, axis=-1, keepdims=True)
        inverse = lax.rsqrt(square / d_model + EPSILON)
        normed[at, :] = (value * inverse * gain_first[...]).astype(bf16)

    m.start_own()
    x_in.start()
    mask_in.start()
    grad_in.start()
    m.barrier()
    m.exchange(0)
    m.advance()
    m.exchange(1)
    m.advance(2)
    m.place_own()
    for copy, put in ((x_in, x_put), (mask_in, mask_put), (grad_in, grad_put)):
        copy.wait()
        put.start()
    xt.send()
    for s in range(1, m.n_hi):
        mask_copy(s).start()
    m.exchange(2)
    m.advance(4)
    xt.relay(1)
    m.exchange(3)
    m.advance(5)
    xt.relay(2)
    m.exchange(4)
    m.advance(3)
    xt.relay(3)
    m.exchange(5, 1, 3)
    xt.finish()
    x_put.wait()
    mask_put.wait()
    for s in range(1, m.n_hi):
        mask_copy(s).wait_recv()
    m.arrived(0)
    m.arrived(1)
    load([(x_out, normed), (q_all, q_full), (k_all, k_full), (mask_out, mask_full)])
    by_rows(tokens, 32, normalise_first)
    project(q_full, store_query)
    m.advance()
    project(k_full, store_key)
    m.advance()
    m.arrived(2)
    load([(v_all, v_full)])
    project(v_full, store_value)
    m.advance()
    attend_some(0, tokens // seq_len // 2)
    m.advance()
    attend_some(tokens // seq_len // 2, tokens // seq_len // 2)
    m.advance()
    m.arrived(3)
    load([(o_out, o_full)])
    out_project((1 - m.mp) * share, store_theirs)
    halves.start()
    out_project(m.mp * share, store_mine)
    m.advance()
    halves.wait_recv()

    def join(at):
        both[at, :] = (mine[at, :] + arrived[at, :].astype(f32)).astype(bf16)

    by_rows(tokens, 32, join)
    for s in range(1, m.n_hi):
        reduce_copy(s).start()
    m.exchange(5, 3)
    m.exchange(6)
    m.advance(3)
    for s in range(1, m.n_hi):
        reduce_copy(s).wait_recv()

    def add(at):
        own = pl.ds(pl.multiple_of(m.hi * rows, rows) + at.start, at.size)
        total = hidden[at, :].astype(f32) + mine[own, :] + arrived[own, :].astype(f32)
        for s in range(m.n_hi - 1):
            total = total + landed[s, at, :].astype(f32)
        sum_out[at, :] = total
        square = jnp.sum(total * total, axis=-1, keepdims=True)
        stat[at, :] = jnp.broadcast_to(square, (at.size, stat.shape[1]))

    by_rows(rows, 32, add)
    stats.start()
    stats.wait_recv()

    def normalise(at):
        inverse = lax.rsqrt((stat[at, :] + stat_in[at, :]) / d_model + EPSILON)
        inv_out[at, :] = inverse
        second_own[at, :] = (sum_out[at, :] * inverse[:, :1] * gain[...]).astype(bf16)

    by_rows(rows, 32, normalise)
    t.send()
    second_put = pltpu.make_async_copy(second_own, t.place(m.hi), here.at[2])
    second_put.start()
    g.send()
    m.advance(4)
    t.relay(1)
    g.relay(1)
    m.advance()
    t.relay(2)
    g.relay(2)
    m.advance()
    t.relay(3)
    t.finish()
    second_put.wait()
    m.arrived(4)
    m.arrived(5)
    load([(second_out, second_full)])
    widen(gate_out, gate_proj)
    g.relay(3)
    widen(up_out, upward)
    m.arrived(6)
    g.finish()
    m.drain()
    grad_put.wait()
    halves.wait_send()
    stats.wait_send()
    for s in range(1, m.n_hi):
        reduce_copy(s).wait_send()
        mask_copy(s).wait_send()


def forward_kernel(
    weights, grad, x, mask, gain_first, gain, bias, key_scale, value_scale, collective_id
):
    f32, bf16 = jnp.float32, jnp.bfloat16
    n_hi = lax.axis_size("hi")
    dma = pltpu.SemaphoreType.DMA
    any_spec = pl.BlockSpec(memory_space=pl.ANY)
    vmem = pl.BlockSpec(memory_space=pltpu.VMEM)
    rows, share = x.shape
    tokens, d_model = rows * n_hi, gain_first.shape[1]
    width, wide = key_scale.shape[1], weights[4].shape[1] // n_hi
    heads, seq_len = bias.shape[0], bias.shape[1]
    array = jax.ShapeDtypeStruct
    out_shape = [gathered(w) for w in weights] + [
        array((tokens, d_model), bf16), array((tokens, d_model), bf16),
        array((mask.shape[0] * n_hi, mask.shape[1]), f32), array((tokens, d_model), bf16),
        array((tokens, width), bf16), array((tokens, width), f32), array((tokens, width), f32),
        array((tokens, width), bf16), array((tokens, width), bf16),
        array((tokens // seq_len, heads, seq_len, seq_len), f32),
        array((rows, share), f32), array((rows, 128), f32),
        array((tokens, wide), f32), array((tokens, wide), f32),
    ]
    return pl.pallas_call(
        forward_body,
        out_shape=out_shape,
        in_specs=[any_spec] * 10 + [vmem] * 6,
        out_specs=[any_spec] * 11 + [vmem] * 10,
        scratch_shapes=move_scratch(weights) + token_scratch() * 3 + [
            pltpu.VMEM((d_model, width), bf16), pltpu.VMEM((d_model, width), bf16),
            pltpu.VMEM((d_model, width), bf16), pltpu.VMEM((tokens, d_model), bf16),
            pltpu.VMEM((tokens, width), bf16),
            pltpu.VMEM((tokens, share), bf16), pltpu.VMEM((tokens, share), bf16),
            pltpu.VMEM((tokens, share), f32), pltpu.VMEM((tokens, share), bf16),
            pltpu.VMEM((n_hi - 1, rows, share), bf16), pltpu.VMEM((rows, share), bf16),
            pltpu.VMEM((rows, share), bf16), pltpu.VMEM((rows, share), bf16),
            pltpu.VMEM(mask.shape, f32), pltpu.VMEM((mask.shape[0] * n_hi, seq_len), f32),
            pltpu.VMEM((rows, 128), f32), pltpu.VMEM((rows, 128), f32),
            pltpu.VMEM((2, d_model, 256), bf16),
            dma((9,)), dma((2,)), dma((2,)), dma((2,)), dma((n_hi - 1,)), dma((n_hi - 1,)),
            dma((n_hi - 1,)), dma((n_hi - 1,)),
        ],
        compiler_params=pltpu.CompilerParams(
            collective_id=collective_id, has_side_effects=True, vmem_limit_bytes=63 * 2**20
        ),
    )(*weights, grad, x, mask, x, gain_first, gain, bias, key_scale, value_scale)


class Spot:
    def __init__(self):
        self.n_hi, self.hi, self.mp = lax.axis_size("hi"), lax.axis_index("hi"), lax.axis_index("mp")

    def back(self, k):
        return lax.rem(self.hi + self.n_hi - k, self.n_hi)


def back_body(
    gate_w, up_w, down_w, d_gate, d_up, hidden, first_sum, inv, gain, grad,
    first_all, ffn_part, d_first,
    theirs, arrived, mine, theirs_ffn, arrived_ffn, mine_ffn, both, landed, own, stat, stat_in,
    tile_a, tile_b, sem_a, sem_b, here, x_send, x_recv, r_send, r_recv, *tok,
):
    f32, bf16 = jnp.float32, jnp.bfloat16
    m = Spot()
    rows, share = grad.shape
    tokens, d_model = first_all.shape
    t = Tokens(m, own, first_all, tok)
    partner = {"mp": 1 - m.mp}
    barrier = pltpu.get_barrier_semaphore()
    places = [{"hi": lax.rem(m.hi + s, m.n_hi)} for s in range(1, m.n_hi)] + [partner]
    for place in places:
        pl.semaphore_signal(barrier, inc=1, device_id=place, device_id_type=MESH)
    pl.semaphore_wait(barrier, len(places))
    tile = tile_a.shape[1]
    per_half = share // tile

    def product(pairs, far, close, copy):
        def bring(i):
            side = jnp.where(i < per_half, 1 - m.mp, m.mp)
            first = side * share + lax.rem(i, per_half) * tile
            slot = lax.rem(i, 2)
            return [
                pltpu.make_async_copy(
                    w.at[pl.ds(pl.multiple_of(first, tile), tile)], buf.at[slot], sem.at[slot]
                )
                for _, w, buf, sem in pairs
            ]

        def start(i):
            for one in bring(i):
                one.start()

        start(0)

        def step(i, store):
            pl.when(i + 1 < 2 * per_half)(lambda: start(i + 1))
            for one in bring(i):
                one.wait()
            slot = lax.rem(i, 2)
            total = None
            for left, _, buf, _ in pairs:
                term = contract_last(left[...], buf[slot])
                total = term if total is None else total + term
            store(pl.ds(pl.multiple_of(lax.rem(i, per_half) * tile, tile), tile), total)

        def far_step(i, carry):
            def store(cols, value):
                far[:, cols] = value.astype(bf16)

            step(i, store)
            return carry

        def close_step(i, carry):
            def store(cols, value):
                close[:, cols] = value

            step(i + per_half, store)
            return carry

        lax.fori_loop(0, per_half, far_step, 0)
        copy.start()
        lax.fori_loop(0, per_half, close_step, 0)

    def by_rows(count, size, body):
        def step(i, carry):
            body(pl.ds(pl.multiple_of(i * size, size), size))
            return carry

        lax.fori_loop(0, count // size, step, 0)

    halves = remote(theirs, arrived, x_send.at[0], x_recv.at[0], partner)
    stats = remote(stat, stat_in, x_send.at[1], x_recv.at[1], partner)
    halves_ffn = remote(theirs_ffn, arrived_ffn, x_send.at[2], x_recv.at[2], partner)

    def reduce_copy(s):
        there = lax.rem(m.hi + s, m.n_hi)
        return remote(
            both.at[pl.ds(there * rows, rows)], landed.at[s - 1],
            r_send.at[s - 1], r_recv.at[s - 1], {"hi": there},
        )

    product(
        [(d_gate, gate_w, tile_a, sem_a), (d_up, up_w, tile_b, sem_b)], theirs, mine, halves
    )
    halves.wait_recv()

    def join(at):
        both[at, :] = (mine[at, :] + arrived[at, :].astype(f32)).astype(bf16)

    by_rows(tokens, 32, join)
    for s in range(1, m.n_hi):
        reduce_copy(s).start()
    product([(hidden, down_w, tile_a, sem_a)], theirs_ffn, mine_ffn, halves_ffn)
    halves_ffn.wait_recv()

    def join_ffn(at):
        ffn_part[at, :] = (mine_ffn[at, :] + arrived_ffn[at, :].astype(f32)).astype(bf16)

    by_rows(tokens, 32, join_ffn)
    for s in range(1, m.n_hi):
        reduce_copy(s).wait_recv()

    def add(at):
        at_own = pl.ds(pl.multiple_of(m.hi * rows, rows) + at.start, at.size)
        total = mine[at_own, :] + arrived[at_own, :].astype(f32)
        for s in range(m.n_hi - 1):
            total = total + landed[s, at, :].astype(f32)
        total = total * gain[...]
        d_first[at, :] = total
        dots = jnp.sum(total * first_sum[at, :], axis=-1, keepdims=True)
        stat[at, :] = jnp.broadcast_to(dots, (at.size, stat.shape[1]))

    by_rows(rows, 32, add)
    stats.start()
    stats.wait_recv()

    def finish(at):
        inverse = inv[at, :][:, :1]
        mean = (stat[at, :] + stat_in[at, :])[:, :1] / d_model
        total = (
            grad[at, :].astype(f32)
            + inverse * d_first[at, :]
            - first_sum[at, :] * (inverse * inverse * inverse * mean)
        )
        d_first[at, :] = total
        own[at, :] = total.astype(bf16)

    by_rows(rows, 32, finish)
    t.send()
    put = pltpu.make_async_copy(own, t.place(m.hi), here.at[0])
    put.start()
    for r in range(1, m.n_hi):
        t.relay(r)
    t.finish()
    put.wait()
    halves.wait_send()
    halves_ffn.wait_send()
    stats.wait_send()
    for s in range(1, m.n_hi):
        reduce_copy(s).wait_send()


def back_kernel(
    gate_w, up_w, down_w, d_gate, d_up, hidden, first_sum, inv, gain, grad, collective_id
):
    f32, bf16 = jnp.float32, jnp.bfloat16
    n_hi = lax.axis_size("hi")
    dma = pltpu.SemaphoreType.DMA
    any_spec = pl.BlockSpec(memory_space=pl.ANY)
    vmem = pl.BlockSpec(memory_space=pltpu.VMEM)
    rows, share = grad.shape
    tokens, wide = d_gate.shape
    array = jax.ShapeDtypeStruct
    return pl.pallas_call(
        back_body,
        out_shape=[
            array((tokens, gate_w.shape[0]), bf16), array((tokens, share), bf16),
            array((rows, share), f32),
        ],
        in_specs=[any_spec] * 3 + [vmem] * 7,
        out_specs=[any_spec, vmem, vmem],
        scratch_shapes=[
            pltpu.VMEM((tokens, share), bf16), pltpu.VMEM((tokens, share), bf16),
            pltpu.VMEM((tokens, share), f32),
            pltpu.VMEM((tokens, share), bf16), pltpu.VMEM((tokens, share), bf16),
            pltpu.VMEM((tokens, share), f32), pltpu.VMEM((tokens, share), bf16),
            pltpu.VMEM((n_hi - 1, rows, share), bf16), pltpu.VMEM((rows, share), bf16),
            pltpu.VMEM((rows, 128), f32), pltpu.VMEM((rows, 128), f32),
            pltpu.VMEM((2, 256, wide), bf16), pltpu.VMEM((2, 256, wide), bf16),
            dma((2,)), dma((2,)), dma((1,)), dma((3,)), dma((3,)),
            dma((n_hi - 1,)), dma((n_hi - 1,)),
        ] + token_scratch(),
        compiler_params=pltpu.CompilerParams(
            collective_id=collective_id, has_side_effects=True, vmem_limit_bytes=60 * 2**20
        ),
    )(gate_w, up_w, down_w, d_gate, d_up, hidden, first_sum, inv, gain, grad)


def on_device_columns(
    hidden_in, lengths, norm_attn, q_weight, k_weight, v_weight, out_weight_t, norm_ffn,
    gate_weight, up_weight, down_weight_t, scale_key, scale_value, scale_ffn, out_grad,
    position_bias,
):
    f32, bf16 = jnp.float32, jnp.bfloat16
    n_hi, n_lo = lax.axis_size("hi"), lax.axis_size("lo")
    hi, lo, mp = lax.axis_index("hi"), lax.axis_index("lo"), lax.axis_index("mp")
    d_model = norm_attn.shape[0]
    tokens_local, share = hidden_in.shape
    seq_local = lengths.shape[0]
    seq_len = tokens_local // seq_local
    tokens = n_hi * tokens_local

    def swap_lo(x, bit):
        return lax.ppermute(x, "lo", [(i, i ^ bit) for i in range(n_lo)])

    def swap_hi(x, bit):
        return lax.ppermute(x, "hi", [(i, i ^ bit) for i in range(n_hi)])

    def swap_mp(x):
        return lax.ppermute(x, "mp", [(0, 1), (1, 0)])

    def own_columns(x):
        width = x.shape[-1] // n_hi
        return lax.dynamic_slice_in_dim(x, hi * width, width, x.ndim - 1)

    def times(x, w):
        return jnp.dot(x, w, preferred_element_type=f32)

    def join_features(own):
        other = swap_mp(own)
        lower = jnp.where(mp == 0, own, other)
        upper = jnp.where(mp == 0, other, own)
        return jnp.concatenate([lower, upper], axis=1)

    def back_sum(pairs):
        total = None
        for x, w in pairs:
            term = contract_last(x, w)
            total = term if total is None else total + term
        mine = lax.dynamic_slice_in_dim(total, mp * share, share, 1)
        theirs = lax.dynamic_slice_in_dim(total, (1 - mp) * share, share, 1)
        return (mine + swap_mp(theirs.astype(bf16)).astype(f32)).astype(bf16)

    def scatter(x):
        return lax.psum_scatter(x, "hi", scatter_dimension=0, tiled=True).astype(f32)

    def token_mean(x):
        part = jnp.sum(x, axis=-1, keepdims=True)
        return (part + swap_mp(part)) / d_model

    def own_half(gain):
        return lax.dynamic_slice_in_dim(gain, mp * share, share, 0)[None]

    gain_ffn = own_half(norm_ffn)
    gain_attn_half = own_half(norm_attn)
    gain_attn = norm_attn[None]
    key_scale, value_scale = own_columns(scale_key), own_columns(scale_value)
    ffn_scale = own_columns(scale_ffn)

    inputs_half = hidden_in
    grad_half = lax.dynamic_slice_in_dim(out_grad, mp * share, share, 1)
    keep = lax.broadcasted_iota(jnp.int32, (8 * seq_local, seq_len), 1) < lengths[0]
    mask = jnp.where(keep, 0.0, NEGATIVE)
    heads_local = q_weight.shape[1] // n_hi // HEAD_DIM
    bias = lax.dynamic_slice_in_dim(position_bias, hi * heads_local, heads_local, 0)
    (
        q_w, k_w, v_w, o_w, gate_w, up_w, down_w, grad_all, inputs_all, _, _, queries, key_pre,
        value_pre, key_rows, value_rows, attn_probs, first_sum, inv_second, gate_proj, upward,
    ) = forward_kernel(
        (q_weight, k_weight, v_weight, out_weight_t, gate_weight, up_weight, down_weight_t),
        out_grad, hidden_in, mask, gain_attn, gain_ffn, bias, key_scale[None],
        value_scale[None], 0,
    )
    inputs32 = lax.dynamic_slice_in_dim(
        inputs_all, hi * tokens_local, tokens_local, 0
    ).astype(f32)
    inv_mine = lax.rsqrt(
        jnp.sum(inputs32 * inputs32, axis=-1, keepdims=True) / d_model + EPSILON
    )
    n_seq = n_hi * seq_local
    shaped = (n_seq, seq_len, heads_local, HEAD_DIM)
    q_heads = queries.reshape(shaped)
    k_heads = key_rows.reshape(shaped)
    v_heads = value_rows.reshape(shaped)
    probs_low = attn_probs.astype(bf16)
    d_hidden = times(grad_all, down_w)
    activated, gelu_back = jax.vjp(gelu_tanh, gate_proj)
    product = activated * upward
    hidden = (product * ffn_scale).astype(bf16)
    grad_ffn_part = jnp.sum(d_hidden * product, axis=0)
    d_product = d_hidden * ffn_scale
    d_gate = gelu_back(d_product * upward)[0].astype(bf16)
    d_up = (d_product * activated).astype(bf16)
    d_first_all, ffn_part, d_first = back_kernel(
        gate_w, up_w, down_w, d_gate, d_up, hidden, first_sum, inv_second, gain_ffn,
        grad_half, 1,
    )
    ffn_out = scatter(ffn_part)
    d_context = times(d_first_all, o_w).astype(bf16)
    dc_heads = d_context.reshape(shaped)
    d_probs = jnp.einsum("bihe,bjhe->bhij", dc_heads, v_heads, preferred_element_type=f32)
    d_scores = (
        attn_probs * (d_probs - jnp.sum(attn_probs * d_probs, axis=-1, keepdims=True))
    ).astype(bf16)
    d_values = jnp.einsum(
        "bhij,bihe->bjhe", probs_low, dc_heads, preferred_element_type=f32
    ).reshape(tokens, -1)
    d_keys = jnp.einsum(
        "bhij,bihe->bjhe", d_scores, q_heads, preferred_element_type=f32
    ).reshape(tokens, -1)
    d_queries = (
        jnp.einsum("bhij,bjhe->bihe", d_scores, k_heads, preferred_element_type=f32)
        .reshape(tokens, -1)
        .astype(bf16)
    )
    grad_key_part = jnp.sum(d_keys * key_pre, axis=0)
    grad_value_part = jnp.sum(d_values * value_pre, axis=0)
    d_key_pre = (d_keys * key_scale).astype(bf16)
    d_value_pre = (d_values * value_scale).astype(bf16)
    input_part = back_sum([(d_queries, q_w), (d_key_pre, k_w), (d_value_pre, v_w)])
    ffn_out, input_part = lax.optimization_barrier((ffn_out, input_part))
    scaled_in = scatter(input_part) * gain_attn_half
    mine32 = inputs_half.astype(f32)
    mean_dot = token_mean(scaled_in * mine32)
    input_grad = (
        d_first
        + inv_mine * scaled_in
        - mine32 * inv_mine * inv_mine * inv_mine * mean_dot
    ).astype(bf16)
    block_out = (first_sum + ffn_out).astype(bf16)

    def totals(part):
        part = part[None]
        for bit in (1, 2):
            part = part + swap_lo(part, bit)
        for bit in (1, 2):
            other = swap_hi(part, bit)
            upper = (hi & bit) > 0
            part = jnp.concatenate(
                [jnp.where(upper, other, part), jnp.where(upper, part, other)], axis=0
            )
        return part

    attn_totals = totals(jnp.concatenate([grad_key_part, grad_value_part]))
    width = grad_key_part.shape[0]
    return (
        block_out,
        input_grad,
        attn_totals[:, :width].reshape(-1),
        attn_totals[:, width:].reshape(-1),
        totals(grad_ffn_part).reshape(-1),
    )


def solution(mesh):
    n_dp, n_mp = mesh.shape["dp"], mesh.shape["mp"]
    n_hi = 1
    while n_dp % (n_hi * 2) == 0 and n_hi * n_hi < n_dp:
        n_hi *= 2
    grid = jax.sharding.Mesh(
        mesh.devices.reshape(n_hi, n_dp // n_hi, n_mp), ("hi", "lo", "mp")
    )
    dp = ("hi", "lo")
    weight = P(dp, "mp")
    columns = (n_hi, n_dp // n_hi, n_mp) == (4, 4, 2)
    return jax.shard_map(
        on_device_columns if columns else on_device_general,
        mesh=grid,
        in_specs=(
            P(dp, "mp"), P(dp), P(), weight, weight, weight, weight, P(), weight, weight, weight,
            P("mp"), P("mp"), P("mp"), P(dp, None), P("mp", None, None),
        ),
        out_specs=(P(dp, "mp"), P(dp, "mp"), P("mp"), P("mp"), P("mp")),
        check_vma=False,
    )
```
